512 devices in a mesh: gx: 16 (over y, z_hi, core), gy: 32 (over z_lo, x).
Axes of the slice: x: 4, y: 4, z: 16 (z_hi: 2, z_lo: 8; z = z_hi * 8 + z_lo), core: 2. Of those that a mesh axis runs over, the one named last changes fastest.
Arguments:
- permeability: float32 [3, 8, 128, 4096], P(None, None, 'gx', 'gy'), may hold values from 0.01 to 10
- layer_map: int32 [8], replicated, may hold values from 0 to 3, never falling along the last dimension, each value on 1 to 3 neighbouring positions
Outputs:
- coarse_perm: float32 [3, 4, 16, 512], P(None, None, 'gx', 'gy')
- coarse_trans: float32 [3, 4, 16, 512], P(None, None, 'gx', 'gy')
The draws below stay inside these ranges and needn't reach their ends.
Inputs may be any that keep to these rules, and one draw needn't show every extreme that they name: layer_map never falls along the fine layers and every one of the 4 coarse layers holds one or more fine layers.
All inputs are finite; a program needn't handle non-finite values.
Results may differ from the reference program's by a relative error of at most 0.0003.
Values sent between devices are 32-bit elements; how exact they have to be, the bound alone decides.
A program may use at most 64 MiB of HBM per device.

```python
import math
import jax
import jax.numpy as jnp
import numpy as np
from jax import lax

NZ = 8
NCL = 4
BXY = 8
SWEEPS = 4
NX = 128
NY = 4096
N_GX = 16
N_GY = 32


def steps_of(key, shape, shards, least, high):
    gain = 1.0
    for axis_at, parts in shards:
        steps = jax.random.uniform(jax.random.fold_in(jax.random.fold_in(key, 6), axis_at), (parts,), jnp.float32, least / len(shards), high / len(shards))
        gain = gain * jnp.repeat(jnp.exp(steps), shape[axis_at] // parts).reshape((-1,) + (1,) * (len(shape) - 1 - axis_at))
    return gain


def profile(number_of, total, most, lean):
    loads = [(1 << 20) // math.isqrt(rank ** lean) + 1 for rank in range(2, number_of + 1)]
    spare, given = total - most - (number_of - 1), [1] * (number_of - 1)
    while spare > 0:
        candidates = [i for i in range(number_of - 1) if given[i] < most]
        whole, budget = sum([loads[i] for i in candidates]), spare
        for i in candidates:
            more = min(most - given[i], max(1, budget * loads[i] // whole), spare)
            given[i] = given[i] + more
            spare = spare - more
    return np.array([most] + given)


def ragged_sizes(rng, number_of, total, reach, skew):
    if number_of == 2:
        one = jax.random.randint(rng, (), max(1, total - reach), min(reach, total - 1) + 1)
        return jnp.stack([one, total - one])
    tallies = jnp.asarray(profile(number_of, total, reach, skew), jnp.int32)
    pairs = (number_of - 1) // 2
    giver, receiver = tallies[1:1 + 2 * pairs:2], tallies[2:2 + 2 * pairs:2]
    room = jnp.minimum(giver - 1, reach - receiver)
    passed = jax.random.randint(jax.random.fold_in(rng, 1), (pairs,), 0, 1 << 20) % (room + 1)
    tallies = tallies.at[1:1 + 2 * pairs:2].set(giver - passed).at[2:2 + 2 * pairs:2].set(receiver + passed)
    return tallies[jax.random.permutation(jax.random.fold_in(rng, 2), number_of)]


def setup_inputs(seed: int = 0) -> dict:
    seeds = jax.random.split(jax.random.key(seed), 3)
    permeability = jnp.clip(jnp.exp(math.log(10.0) - 6.9077553 * jax.random.uniform(seeds[0], (3, NZ, NX, NY), jnp.float32) ** steps_of(seeds[0], (3, NZ, NX, NY), ((2, 16), (3, 32)), -0.2, 0.2)), 0.01, 10.0)
    layer_map = jnp.searchsorted(jnp.cumsum(ragged_sizes(seeds[1], NCL, NZ, NZ // NCL + NZ // (2 * NCL), 0)), jnp.arange(NZ), side="right").astype(jnp.int32)
    return dict(permeability=permeability, layer_map=layer_map)


KMIN = 0.01
EPS = 1e-6


def sweep_weights(count):
    return [1.0 / (1.05 + 0.95 * math.cos(math.pi * (2 * s + 1) / (2 * count))) for s in range(count)]


def harmonic(left, right):
    return 2.0 * left * right / (left + right)


def linear_field(depth, width, height):
    zc = (jnp.arange(depth + 2, dtype=jnp.float32) - 0.5 - depth / 2.0) / depth
    xc = (jnp.arange(width + 2, dtype=jnp.float32) - 0.5 - width / 2.0) / width
    yc = (jnp.arange(height + 2, dtype=jnp.float32) - 0.5 - height / 2.0) / height
    shape = (depth + 2, width + 2, height + 2)
    return jnp.stack([jnp.broadcast_to(xc[None, :, None], shape), jnp.broadcast_to(yc[None, None, :], shape), jnp.broadcast_to(zc[:, None, None], shape)])


def patch_partials(kext, layer_map):
    depth, width, height = kext.shape[1], kext.shape[2], kext.shape[3]
    perm = kext + KMIN
    tx = jnp.concatenate([perm[0][:, :1], harmonic(perm[0][:, :-1], perm[0][:, 1:]), perm[0][:, -1:]], axis=1)
    ty = jnp.concatenate([perm[1][:, :, :1], harmonic(perm[1][:, :, :-1], perm[1][:, :, 1:]), perm[1][:, :, -1:]], axis=2)
    tz = jnp.concatenate([perm[2][:1], harmonic(perm[2][:-1], perm[2][1:]), perm[2][-1:]], axis=0)
    diag = tx[:, :-1] + tx[:, 1:] + ty[:, :, :-1] + ty[:, :, 1:] + tz[:-1] + tz[1:]
    inverse = 1.0 / diag
    ghost = linear_field(depth, width, height)

    def residual(pressure):
        full = ghost.at[:, 1:-1, 1:-1, 1:-1].set(pressure)
        inflow = tx[:, 1:] * full[:, 1:-1, 2:, 1:-1] + tx[:, :-1] * full[:, 1:-1, :-2, 1:-1]
        inflow = inflow + ty[:, :, 1:] * full[:, 1:-1, 1:-1, 2:] + ty[:, :, :-1] * full[:, 1:-1, 1:-1, :-2]
        inflow = inflow + tz[1:] * full[:, 2:, 1:-1, 1:-1] + tz[:-1] * full[:, :-2, 1:-1, 1:-1]
        return inflow - diag * pressure

    pressure = ghost[:, 1:-1, 1:-1, 1:-1]
    for weight in sweep_weights(SWEEPS):
        pressure = pressure + weight * (residual(pressure) * inverse)
    full = ghost.at[:, 1:-1, 1:-1, 1:-1].set(pressure)
    drop = jnp.stack([full[0, 1:-1, 1:-1, 1:-1] - full[0, 1:-1, 2:, 1:-1], full[1, 1:-1, 1:-1, 1:-1] - full[1, 1:-1, 1:-1, 2:], full[2, 1:-1, 1:-1, 1:-1] - full[2, 2:, 1:-1, 1:-1]])
    faces = jnp.stack([tx[:, 1:], ty[:, :, 1:], tz[1:]])
    square = drop * drop
    energy = faces * square
    onehot = (layer_map[:, None] == jnp.arange(NCL, dtype=jnp.int32)[None, :]).astype(jnp.float32)

    def coarsen(values):
        blocks = values.reshape(3, depth, width // BXY, BXY, height // BXY, BXY).sum(axis=(3, 5))
        return jnp.einsum("dzab,zl->dlab", blocks, onehot, precision=lax.Precision.HIGHEST)

    return coarsen(energy), coarsen(square)


def reference(permeability, layer_map):
    cols_x = permeability.shape[2] // N_GX
    cols_y = permeability.shape[3] // N_GY
    padded = jnp.pad(permeability, ((0, 0), (0, 0), (BXY, BXY), (BXY, BXY)))
    blocks_x = cols_x // BXY
    blocks_y = cols_y // BXY

    def one_row(row):
        def one_patch(col):
            start = (jnp.int32(0), jnp.int32(0), (row * cols_x).astype(jnp.int32), (col * cols_y).astype(jnp.int32))
            kext = lax.dynamic_slice(padded, start, (3, NZ, cols_x + 2 * BXY, cols_y + 2 * BXY))
            return patch_partials(kext, layer_map)
        return jax.vmap(one_patch)(jnp.arange(N_GY, dtype=jnp.int32))

    energy, square = lax.map(one_row, jnp.arange(N_GX, dtype=jnp.int32))
    shape = (3, NCL, N_GX * blocks_x + 2, N_GY * blocks_y + 2)
    size = (3, NCL, blocks_x + 2, blocks_y + 2)

    def accumulate(index, totals):
        row = (index // N_GY).astype(jnp.int32)
        col = (index % N_GY).astype(jnp.int32)
        start = (jnp.int32(0), jnp.int32(0), (row * blocks_x).astype(jnp.int32), (col * blocks_y).astype(jnp.int32))
        total_e, total_s = totals
        total_e = lax.dynamic_update_slice(total_e, lax.dynamic_slice(total_e, start, size) + energy[row, col], start)
        total_s = lax.dynamic_update_slice(total_s, lax.dynamic_slice(total_s, start, size) + square[row, col], start)
        return total_e, total_s

    zeros = jnp.zeros(shape, jnp.float32)
    total_e, total_s = lax.fori_loop(0, N_GX * N_GY, accumulate, (zeros, zeros))
    coarse_perm = total_e[:, :, 1:-1, 1:-1] / (total_s[:, :, 1:-1, 1:-1] + EPS)
    nxt_x = jnp.concatenate([coarse_perm[0][:, 1:], jnp.zeros_like(coarse_perm[0][:, :1])], axis=1)
    nxt_y = jnp.concatenate([coarse_perm[1][:, :, 1:], jnp.zeros_like(coarse_perm[1][:, :, :1])], axis=2)
    trans_x = harmonic(coarse_perm[0], nxt_x)
    trans_y = harmonic(coarse_perm[1], nxt_y)
    trans_z = jnp.concatenate([harmonic(coarse_perm[2][:-1], coarse_perm[2][1:]), jnp.zeros_like(coarse_perm[2][:1])], axis=0)
    return coarse_perm, jnp.stack([trans_x, trans_y, trans_z])
```

```python
import math

import jax
import jax.numpy as jnp
from jax import lax
from jax.experimental import pallas as pl
from jax.experimental.pallas import tpu as pltpu
from jax.sharding import PartitionSpec as P

MESH = pl.DeviceIdType.MESH
NCL = 4
BXY = 8
SWEEPS = 4
KMIN = 0.01
EPS = 1e-06
NZ = 8
LANES = 128
F32 = jnp.float32

DOWN = [(1, r) for r in range(4)] + [(2, r) for r in range(4)] + [(0, r) for r in range(5)]
UP = [(0, r) for r in range(4, 8)] + [(1, r) for r in range(5, 8)] + [(2, r) for r in range(5, 8)]
PLANES = DOWN + UP[1:] + [(1, 4), (2, 4)]
PLANE_AT = {cr: at for at, cr in enumerate(PLANES)}
UP_FROM = PLANE_AT[UP[0]]
SLOT = 9
PACKS = [DOWN, UP + [(1, 4), (2, 4)]]
DIRECTIONS = [(1, 0), (-1, 0), (1, 1), (1, -1), (-1, 1), (-1, -1), (0, 1), (0, -1)]
LEFT_AT = 20
RIGHT_AT = 72
W = [1.0 / (1.05 + 0.95 * math.cos(math.pi * (2 * s + 1) / (2 * SWEEPS))) for s in range(SWEEPS)]


def harmonic(left, right):
    return 2.0 * left * right / (left + right)


def lane_of(shape):
    return lax.broadcasted_iota(jnp.int32, shape, len(shape) - 1)


def between(lane, low, high):
    return (lane >= low) & (lane < high)


def kernel(
    n_gx, n_gy, k_hbm, map_hbm, perm_ref, trans_ref,
    k_own, map_own, planes, packs, from_low, from_high, packs_own, packs_low, packs_high,
    kp, coef, face, q1, q2, q3, q4, u_coef, uq, mess, mess_x, mess_y,
    load_sem, send_sem, recv_sem,
):
    i, j = lax.axis_index("gx"), lax.axis_index("gy")
    load_k = pltpu.make_async_copy(k_hbm, k_own, load_sem.at[0])
    load_map = pltpu.make_async_copy(map_hbm, map_own, load_sem.at[1])
    load_k.start()
    load_map.start()

    def inside(di, dj):
        tests = []
        if di:
            tests.append(i + di < n_gx if di > 0 else i >= -di)
        if dj:
            tests.append(j + dj < n_gy if dj > 0 else j >= -dj)
        return tests[0] if len(tests) == 1 else tests[0] & tests[1]

    def device(di, dj):
        return {"gx": i + di, "gy": j + dj}

    barrier = pltpu.get_barrier_semaphore()
    for di, dj in DIRECTIONS:
        @pl.when(inside(di, dj))
        def _():
            pl.semaphore_signal(barrier, inc=1, device_id=device(di, dj), device_id_type=MESH)

    lane = lane_of((NZ, LANES))
    load_k.wait()
    packed = [jnp.zeros((NZ, LANES), F32), jnp.zeros((NZ, LANES), F32)]
    for at, (c, r) in enumerate(PLANES):
        plane = k_own[pl.ds(c * 64 + r, NZ, stride=8), :]
        planes[at] = plane
        for v, pack in enumerate(PACKS):
            if (c, r) in pack:
                s = SLOT * pack.index((c, r))
                packed[v] = jnp.where(between(lane, s, s + SLOT), pltpu.roll(plane, s + 4, axis=1), packed[v])
    packs[0] = packed[0]
    packs[1] = packed[1]

    rows_near = 1 + (i > 0).astype(jnp.int32) + (i < n_gx - 1).astype(jnp.int32)
    cols_near = 1 + (j > 0).astype(jnp.int32) + (j < n_gy - 1).astype(jnp.int32)
    pl.semaphore_wait(barrier, rows_near * cols_near - 1)

    def copy_of(k, di, dj):
        side = 0 if dj > 0 else 1
        if dj == 0:
            if di > 0:
                source, target = planes.at[pl.ds(UP_FROM, len(UP))], from_low
            else:
                source, target = planes.at[pl.ds(0, len(DOWN))], from_high
        elif di == 0:
            source, target = packs, packs_own.at[side]
        elif di > 0:
            source, target = packs.at[1], packs_low.at[side]
        else:
            source, target = packs.at[0], packs_high.at[side]
        return pltpu.make_async_remote_copy(
            src_ref=source, dst_ref=target, send_sem=send_sem.at[k], recv_sem=recv_sem.at[k],
            device_id=device(di, dj), device_id_type=MESH,
        )

    copies = []
    for k, (di, dj) in enumerate(DIRECTIONS):
        copy = copy_of(k, di, dj)
        copies.append(copy)
        pl.when(inside(di, dj))(copy.start)

    def arrive(k, di, dj):
        copy, target = copies[k], copy_of(k, di, dj).dst_ref
        here = inside(-di, -dj)
        pl.when(here)(copy.wait_recv)

        @pl.when(jnp.logical_not(here))
        def _():
            target[...] = jnp.zeros(target.shape, F32)

    edge = (lane >= LANES - 4) | (lane < 5)
    slot_left = lax.rem(lane, SLOT) < 4

    def assemble(c, r, merged):
        if 0 <= r < 8:
            own = planes[PLANE_AT[c, r]]
            v = 0 if (c, r) in DOWN else 1
            s = SLOT * PACKS[v].index((c, r))
            pack = merged[v]
        elif r < 0:
            at = UP.index((c, r + 8))
            own, s, pack = from_low[at], SLOT * at, merged
        else:
            at = DOWN.index((c, r - 8))
            own, s, pack = from_high[at], SLOT * at, merged
        margin = pltpu.roll(pack, (2 * LANES - s - 4) % LANES, axis=1)
        left = pltpu.roll(jnp.where(lane >= LANES - 4, margin, own), LEFT_AT + 4, axis=1)
        right = pltpu.roll(jnp.where(lane < 5, margin, own), RIGHT_AT + 8, axis=1)
        other = jnp.where(between(lane, LEFT_AT, LEFT_AT + 12), left, 1.0)
        other = jnp.where(between(lane, RIGHT_AT, RIGHT_AT + 13), right, other)
        other = jnp.where(edge, margin, other)
        kp[c, r + 4, :, 0:LANES] = own + KMIN
        kp[c, r + 4, :, LANES : 2 * LANES] = other + KMIN

    lane2 = lane_of((1, NZ, 2 * LANES))
    layer2 = lax.broadcasted_iota(jnp.int32, (1, NZ, 2 * LANES), 1)
    left_end = lane2 == LANES + LEFT_AT + 11
    right_start = lane2 == LANES + RIGHT_AT
    top, bottom = layer2 == NZ - 1, layer2 == 0
    zero = jnp.zeros((1, NZ, 2 * LANES), F32)

    def y_next(v):
        return pltpu.roll(v, 2 * LANES - 1, axis=2)

    def y_last(v):
        return pltpu.roll(v, 1, axis=2)

    def z_next(v):
        return pltpu.roll(v, NZ - 1, axis=1)

    def z_last(v):
        return pltpu.roll(v, 1, axis=1)

    def finish(tx_low, tx_high, ty_low, ty_high, tz_low, tz_high, low_end, high_end):
        inverse = 1.0 / (tx_low + tx_high + ty_low + ty_high + tz_low + tz_high)
        return [
            zero if low_end else tx_low * inverse,
            zero if high_end else tx_high * inverse,
            jnp.where(right_start, 0.0, ty_low * inverse),
            jnp.where(left_end, 0.0, ty_high * inverse),
            jnp.where(bottom, 0.0, tz_low * inverse),
            jnp.where(top, 0.0, tz_high * inverse),
            (tx_high - tx_low) * inverse,
            (ty_high - ty_low) * inverse,
            (tz_high - tz_low) * inverse,
        ]

    def coefficients(r):
        kx_low, kx, kx_high = (kp[0, pl.ds(r + 4 + d, 1)] for d in (-1, 0, 1))
        ky, kz = kp[1, pl.ds(r + 4, 1)], kp[2, pl.ds(r + 4, 1)]
        tx_low, tx_high = harmonic(kx_low, kx), harmonic(kx, kx_high)
        ty = harmonic(ky, y_next(ky))
        ty_low = jnp.where(right_start, ky, y_last(ty))
        ty_high = jnp.where(left_end, ky, ty)
        tz = harmonic(kz, z_next(kz))
        tz_low = jnp.where(bottom, kz, z_last(tz))
        tz_high = jnp.where(top, kz, tz)
        for n, value in enumerate(finish(tx_low, tx_high, ty_low, ty_high, tz_low, tz_high, False, False)):
            coef[n, pl.ds(r + 3, 1)] = value
            if n >= 6:
                q1[n - 6, pl.ds(r + 3, 1)] = W[0] * value
        if 0 <= r < 8:
            for d, value in enumerate((tx_high, ty_high, tz_high)):
                face[d, pl.ds(r, 1)] = value
        if r == 0 or r == 7:
            e = 0 if r == 0 else 1
            low, high = (kx, tx_high) if r == 0 else (tx_low, kx)
            for n, value in enumerate(finish(low, high, ty_low, ty_high, tz_low, tz_high, r == 0, r == 7)):
                u_coef[e, pl.ds(n, 1)] = value
                if n >= 6:
                    uq[e, 0, n - 6, pl.ds(0, 1)] = W[0] * value

    def sweep(w, cs, low, mid, high):
        around = cs[2] * y_last(mid) + cs[3] * y_next(mid) + cs[4] * z_last(mid) + cs[5] * z_next(mid)
        if low is not None:
            around = around + cs[0] * low
        if high is not None:
            around = around + cs[1] * high
        return mid + w * (around + cs[6] - mid)

    def coefs_at(r, d):
        return [coef[n, pl.ds(r + 3, 1)] for n in (0, 1, 2, 3, 4, 5, 6 + d)]

    qs = [(q1, 3), (q2, 2), (q3, 1), (q4, 0)]

    def q_at(s, d, r):
        ref, offset = qs[s]
        return ref[d, pl.ds(r + offset, 1)]

    def e_at(e, s, d, n):
        r = n if e == 0 else 7 - n
        return uq[e, s, d, pl.ds(n, 1)] if n <= s else q_at(s, d, r)

    def main_row(s, r):
        for d in range(3):
            low, mid, high = (q_at(s - 1, d, r + n) for n in (-1, 0, 1))
            ref, offset = qs[s]
            ref[d, pl.ds(r + offset, 1)] = sweep(W[s], coefs_at(r, d), low, mid, high)

    def edge_row(e, s, n):
        r = n if e == 0 else 7 - n
        for d in range(3):
            inner, mid = e_at(e, s - 1, d, n + 1), e_at(e, s - 1, d, n)
            outer = e_at(e, s - 1, d, n - 1) if n else None
            cs = coefs_at(r, d) if n else [u_coef[e, pl.ds(m, 1)] for m in (0, 1, 2, 3, 4, 5, 6 + d)]
            low, high = (outer, inner) if e == 0 else (inner, outer)
            uq[e, s, d, pl.ds(n, 1)] = sweep(W[s], cs, low, mid, high)

    for k in (6, 7):
        arrive(k, *DIRECTIONS[k])
    merged = [jnp.where(slot_left, packs_own[0, v], packs_own[1, v]) for v in range(2)]
    for r in range(8):
        for c in range(3):
            assemble(c, r, merged)
    for r in range(1, 7):
        coefficients(r)

    for k in (2, 3, 0):
        arrive(k, *DIRECTIONS[k])
    merged = jnp.where(slot_left, packs_low[0], packs_low[1])
    for r in range(-4, 0):
        for c in range(3):
            if r > -4 or c == 0:
                assemble(c, r, merged)
    for r in range(-3, 1):
        coefficients(r)
    for k in (4, 5, 1):
        arrive(k, *DIRECTIONS[k])
    merged = jnp.where(slot_left, packs_high[0], packs_high[1])
    for r in range(8, 13):
        for c in range(3):
            if r < 12 or c == 0:
                assemble(c, r, merged)
    for r in range(7, 12):
        coefficients(r)

    for s in range(1, SWEEPS):
        for r in range(s - 4 + 1, 12 - s):
            main_row(s, r)
        for e in range(2):
            for n in range(s + 1):
                edge_row(e, s, n)

    sums = []
    flag_up = (i < n_gx - 1).astype(F32)
    flag_low = (i > 0).astype(F32)
    last = SWEEPS - 1

    def drop(d, here, above):
        if d == 0:
            return here - above - 1.0
        if d == 1:
            return here - jnp.where(left_end, 0.0, y_next(here)) - 1.0
        return here - jnp.where(top, 0.0, z_next(here)) - 1.0

    energies, squares = [], []
    for d in range(3):
        def terms(r, here, above, at_end=False):
            fall = drop(d, here, above)
            square = fall * fall
            t = kp[0, pl.ds(r + 4, 1)] if at_end else face[d, pl.ds(r, 1)]
            return jnp.concatenate([t * square, square], axis=0)

        main = [terms(r, q_at(last, d, r), q_at(last, d, r + 1) if d == 0 else None) for r in range(8)]
        up = [terms(r, e_at(0, last, d, r), e_at(0, last, d, r + 1)) for r in range(4)]
        low = [
            terms(r, e_at(1, last, d, 7 - r), zero if r == 7 else e_at(1, last, d, 6 - r), d == 0 and r == 7)
            for r in range(4, 8)
        ]
        third = terms(3, e_at(1, last, d, 4), e_at(1, last, d, 3)) if d == 0 else main[3]
        main_low = main[0] + main[1] + main[2]
        main_high = main[4] + main[5] + main[6] + main[7]
        total = main_low + main[3] + main_high
        total = total + flag_up * (up[0] + up[1] + up[2] + up[3] + main_high)
        total = total + flag_low * (main_low + third + low[0] + low[1] + low[2] + low[3])
        own, other = total[:, :, 0:LANES], total[:, :, LANES : 2 * LANES]
        lane3 = lane_of(own.shape)
        flag_left = (j > 0).astype(F32)
        flag_right = (j < n_gy - 1).astype(F32)
        left = pltpu.roll(other, LANES - LEFT_AT - 4, axis=2) * flag_left
        right = pltpu.roll(other, LANES - RIGHT_AT - 8, axis=2) * flag_right
        own = own + jnp.where(lane3 < 8, left, 0.0) + jnp.where(lane3 >= LANES - 8, right, 0.0)
        sums.append(own)
    stack = jnp.concatenate(sums, axis=0).reshape(6 * NZ, LANES)
    pick = (lax.broadcasted_iota(jnp.int32, (LANES, LANES), 0) // BXY == lane_of((LANES, LANES))).astype(F32)
    blocks = jnp.dot(stack, pick, precision=lax.Precision.HIGHEST, preferred_element_type=F32)
    blocks = blocks.reshape(3, 2, NZ, LANES)

    load_map.wait()
    layer = lax.broadcasted_iota(jnp.int32, (NZ, LANES), 0)
    layer_map = jnp.zeros((NZ, LANES), jnp.int32)
    for z in range(NZ):
        layer_map = jnp.where(layer == z, map_own[z], layer_map)
    extents = (24, 144, 8)
    perm = [[None] * NCL for _ in range(3)]
    for n in range(NCL):
        for d in range(3):
            held = jnp.where(layer_map == n, blocks[d], 0.0)
            both = jnp.sum(held, axis=1, keepdims=True)
            perm[d][n] = both[0] / (both[1] + EPS * extents[d] * extents[d])
    mess[...] = jnp.concatenate(perm[0] + perm[1], axis=0)

    def tell(k, di, dj, target):
        return pltpu.make_async_remote_copy(
            src_ref=mess, dst_ref=target, send_sem=send_sem.at[k], recv_sem=recv_sem.at[k],
            device_id=device(di, dj), device_id_type=MESH,
        )

    last_copies = [(8, -1, 0, mess_x), (9, 0, -1, mess_y)]
    for k, di, dj, target in last_copies:
        pl.when(inside(di, dj))(tell(k, di, dj, target).start)
    for d in range(3):
        for n in range(NCL):
            perm_ref[d, n] = perm[d][n][:, 0 : LANES // BXY]
    for n in range(NCL):
        value = harmonic(perm[2][n], perm[2][n + 1]) if n < NCL - 1 else jnp.zeros((1, LANES), F32)
        trans_ref[2, n] = value[:, 0 : LANES // BXY]
    for k, (di, dj) in enumerate(DIRECTIONS):
        pl.when(inside(di, dj))(copies[k].wait_send)
    for k, di, dj, target in last_copies:
        copy, here = tell(k, di, dj, target), inside(-di, -dj)
        pl.when(here)(copy.wait_recv)

        @pl.when(jnp.logical_not(here))
        def _():
            target[...] = jnp.zeros(target.shape, F32)

    lane1 = lane_of((1, LANES))
    for n in range(NCL):
        trans_ref[0, n] = harmonic(perm[0][n], mess_x[pl.ds(n, 1)])[:, 0 : LANES // BXY]
        beyond = pltpu.roll(mess_y[pl.ds(NCL + n, 1)], LANES // BXY - 1, axis=1)
        after = jnp.where(lane1 == LANES // BXY - 1, beyond, pltpu.roll(perm[1][n], LANES - 1, axis=1))
        trans_ref[1, n] = harmonic(perm[1][n], after)[:, 0 : LANES // BXY]
    for k, di, dj, target in last_copies:
        pl.when(inside(di, dj))(tell(k, di, dj, target).wait_send)


def solution(mesh):
    n_gx, n_gy = mesh.shape["gx"], mesh.shape["gy"]

    def local(permeability, layer_map):
        k = permeability.reshape(3 * NZ * BXY, LANES)
        out = jax.ShapeDtypeStruct((3, NCL, 1, LANES // BXY), F32)
        vmem = lambda *shape: pltpu.VMEM(shape, F32)
        both = 2 * LANES
        return pl.pallas_call(
            lambda *refs: kernel(n_gx, n_gy, *refs),
            out_shape=(out, out),
            in_specs=[pl.BlockSpec(memory_space=pl.ANY)] * 2,
            out_specs=(pl.BlockSpec(memory_space=pltpu.VMEM),) * 2,
            scratch_shapes=[
                vmem(3 * NZ * BXY, LANES),
                pltpu.SMEM((NZ,), jnp.int32),
                vmem(len(PLANES), NZ, LANES),
                vmem(2, NZ, LANES),
                vmem(len(UP), NZ, LANES),
                vmem(len(DOWN), NZ, LANES),
                vmem(2, 2, NZ, LANES),
                vmem(2, NZ, LANES),
                vmem(2, NZ, LANES),
                vmem(3, 17, NZ, both),
                vmem(9, 15, NZ, both),
                vmem(3, 8, NZ, both),
                vmem(3, 15, NZ, both),
                vmem(3, 13, NZ, both),
                vmem(3, 11, NZ, both),
                vmem(3, 9, NZ, both),
                vmem(2, 9, NZ, both),
                vmem(2, SWEEPS, 3, SWEEPS, NZ, both),
                vmem(NZ, LANES),
                vmem(NZ, LANES),
                vmem(NZ, LANES),
                pltpu.SemaphoreType.DMA((2,)),
                pltpu.SemaphoreType.DMA((10,)),
                pltpu.SemaphoreType.DMA((10,)),
            ],
            compiler_params=pltpu.CompilerParams(collective_id=0, has_side_effects=True),
            name="upscale",
        )(k, layer_map)

    spec = P(None, None, "gx", "gy")
    return jax.shard_map(local, mesh=mesh, in_specs=(spec, P()), out_specs=(spec, spec), check_vma=False)
```

```python
import math

import jax
import jax.numpy as jnp
from jax import lax
from jax.experimental import pallas as pl
from jax.experimental.pallas import tpu as pltpu
from jax.sharding import PartitionSpec as P

MESH = pl.DeviceIdType.MESH
NCL = 4
BXY = 8
SWEEPS = 4
KMIN = 0.01
EPS = 1e-06
NZ = 8
LANES = 128
F32 = jnp.float32

DOWN = [(1, r) for r in range(4)] + [(2, r) for r in range(4)] + [(0, r) for r in range(5)]
UP = [(0, r) for r in range(4, 8)] + [(1, r) for r in range(5, 8)] + [(2, r) for r in range(5, 8)]
PLANES = DOWN + UP[1:] + [(1, 4), (2, 4)]
PLANE_AT = {cr: at for at, cr in enumerate(PLANES)}
UP_FROM = PLANE_AT[UP[0]]
SLOT = 9
PACKS = [DOWN, UP + [(1, 4), (2, 4)]]
DIRECTIONS = [(1, 0), (-1, 0), (1, 1), (1, -1), (-1, 1), (-1, -1), (0, 1), (0, -1)]
MORE = [(-1, 0), (-1, 1), (-1, -1), (-2, 0), (-2, 1), (-2, -1)]
ENDS = [0, 7, 8, 15]
LEFT_AT = 20
RIGHT_AT = 72
W = [1.0 / (1.05 + 0.95 * math.cos(math.pi * (2 * s + 1) / (2 * SWEEPS))) for s in range(SWEEPS)]


def harmonic(left, right):
    return 2.0 * left * right / (left + right)


def lane_of(shape):
    return lax.broadcasted_iota(jnp.int32, shape, len(shape) - 1)


def between(lane, low, high):
    return (lane >= low) & (lane < high)


def kernel(
    n_gx, n_gy, k_hbm, map_hbm, perm_ref, trans_ref,
    k_own, map_own, planes, packs, from_low, from_high, packs_own, packs_low, packs_high,
    more_high, far_high, packs_more, packs_far,
    kp, coef, face, q1, q2, q3, q4, u_coef, uq, mess, mess_x, mess_y,
    load_sem, send_sem, recv_sem,
):
    i, j = lax.axis_index("gx"), lax.axis_index("gy")
    load_k = pltpu.make_async_copy(k_hbm, k_own, load_sem.at[0])
    load_map = pltpu.make_async_copy(map_hbm, map_own, load_sem.at[1])
    load_k.start()
    load_map.start()

    def inside(di, dj):
        tests = []
        if di:
            tests.append(i + di < n_gx if di > 0 else i >= -di)
        if dj:
            tests.append(j + dj < n_gy if dj > 0 else j >= -dj)
        return tests[0] if len(tests) == 1 else tests[0] & tests[1]

    def device(di, dj):
        return {"gx": i + di, "gy": j + dj}

    def reaches(di, dj):
        row, col = i + di, j + dj
        early = jnp.where(col < n_gy // 2, 1, 3)
        return (lax.rem(row + 4, 4) == early) & (row + 1 < n_gx)

    barrier = pltpu.get_barrier_semaphore()
    for di, dj in DIRECTIONS:
        @pl.when(inside(di, dj))
        def _():
            pl.semaphore_signal(barrier, inc=1, device_id=device(di, dj), device_id_type=MESH)

    signals = 0
    for di, dj in MORE[3:]:
        @pl.when(inside(-di, -dj) & reaches(0, 0))
        def _():
            pl.semaphore_signal(barrier, inc=1, device_id=device(-di, -dj), device_id_type=MESH)

        signals = signals + (inside(di, dj) & reaches(di, dj)).astype(jnp.int32)

    lane = lane_of((NZ, LANES))
    load_k.wait()
    packed = [jnp.zeros((NZ, LANES), F32), jnp.zeros((NZ, LANES), F32)]
    for at, (c, r) in enumerate(PLANES):
        plane = k_own[pl.ds(c * 64 + r, NZ, stride=8), :]
        planes[at] = plane
        for v, pack in enumerate(PACKS):
            if (c, r) in pack:
                s = SLOT * pack.index((c, r))
                packed[v] = jnp.where(between(lane, s, s + SLOT), pltpu.roll(plane, s + 4, axis=1), packed[v])
    packs[0] = packed[0]
    packs[1] = packed[1]

    rows_near = 1 + (i > 0).astype(jnp.int32) + (i < n_gx - 1).astype(jnp.int32)
    cols_near = 1 + (j > 0).astype(jnp.int32) + (j < n_gy - 1).astype(jnp.int32)
    pl.semaphore_wait(barrier, rows_near * cols_near - 1 + signals)

    def copy_of(k, di, dj):
        side = 0 if dj > 0 else 1
        if dj == 0:
            if di > 0:
                source, target = planes.at[pl.ds(UP_FROM, len(UP))], from_low
            else:
                source, target = planes.at[pl.ds(0, len(DOWN))], from_high
        elif di == 0:
            source, target = packs, packs_own.at[side]
        elif di > 0:
            source, target = packs.at[1], packs_low.at[side]
        else:
            source, target = packs.at[0], packs_high.at[side]
        return pltpu.make_async_remote_copy(
            src_ref=source, dst_ref=target, send_sem=send_sem.at[k], recv_sem=recv_sem.at[k],
            device_id=device(di, dj), device_id_type=MESH,
        )

    def more_of(k, di, dj):
        side = 0 if dj > 0 else 1
        if dj == 0:
            if di == -1:
                source, target = planes.at[pl.ds(len(DOWN), len(PLANES) - len(DOWN))], more_high
            else:
                source, target = planes.at[pl.ds(0, len(DOWN))], far_high
        elif di == -1:
            source, target = packs.at[1], packs_more.at[side]
        else:
            source, target = packs.at[0], packs_far.at[side]
        return pltpu.make_async_remote_copy(
            src_ref=source, dst_ref=target, send_sem=send_sem.at[k], recv_sem=recv_sem.at[k],
            device_id=device(di, dj), device_id_type=MESH,
        )

    copies = [(copy_of(k, *to), inside(*to), inside(-to[0], -to[1])) for k, to in enumerate(DIRECTIONS)]
    for k, (di, dj) in enumerate(MORE):
        sends = inside(di, dj) & reaches(di, dj)
        copies.append((more_of(len(DIRECTIONS) + k, di, dj), sends, inside(-di, -dj)))
    for copy, sends, _ in copies:
        pl.when(sends)(copy.start)

    def arrive(k):
        copy, _, here = copies[k]
        target = copy.dst_ref
        pl.when(here)(copy.wait_recv)

        @pl.when(jnp.logical_not(here))
        def _():
            target[...] = jnp.zeros(target.shape, F32)

    edge = (lane >= LANES - 4) | (lane < 5)
    slot_left = lax.rem(lane, SLOT) < 4

    def assemble(c, r, merged):
        if 0 <= r < 8:
            own = planes[PLANE_AT[c, r]]
            v = 0 if (c, r) in DOWN else 1
            s = SLOT * PACKS[v].index((c, r))
            pack = merged[v]
        elif r < 0:
            at = UP.index((c, r + 8))
            own, s, pack = from_low[at], SLOT * at, merged
        elif r >= 16 or (c, r - 8) in DOWN:
            at = DOWN.index((c, r % 8))
            own, s, pack = (from_high if r < 16 else far_high)[at], SLOT * at, merged
        else:
            at = PLANE_AT[c, r - 8] - len(DOWN)
            own, s, pack = more_high[at], SLOT * PACKS[1].index((c, r - 8)), merged
        margin = pltpu.roll(pack, (2 * LANES - s - 4) % LANES, axis=1)
        left = pltpu.roll(jnp.where(lane >= LANES - 4, margin, own), LEFT_AT + 4, axis=1)
        right = pltpu.roll(jnp.where(lane < 5, margin, own), RIGHT_AT + 8, axis=1)
        other = jnp.where(between(lane, LEFT_AT, LEFT_AT + 12), left, 1.0)
        other = jnp.where(between(lane, RIGHT_AT, RIGHT_AT + 13), right, other)
        other = jnp.where(edge, margin, other)
        kp[c, r + 4, :, 0:LANES] = own + KMIN
        kp[c, r + 4, :, LANES : 2 * LANES] = other + KMIN

    lane2 = lane_of((1, NZ, 2 * LANES))
    layer2 = lax.broadcasted_iota(jnp.int32, (1, NZ, 2 * LANES), 1)
    left_end = lane2 == LANES + LEFT_AT + 11
    right_start = lane2 == LANES + RIGHT_AT
    top, bottom = layer2 == NZ - 1, layer2 == 0
    zero = jnp.zeros((1, NZ, 2 * LANES), F32)

    def y_next(v):
        return pltpu.roll(v, 2 * LANES - 1, axis=2)

    def y_last(v):
        return pltpu.roll(v, 1, axis=2)

    def z_next(v):
        return pltpu.roll(v, NZ - 1, axis=1)

    def z_last(v):
        return pltpu.roll(v, 1, axis=1)

    def finish(tx_low, tx_high, ty_low, ty_high, tz_low, tz_high, low_end, high_end):
        inverse = 1.0 / (tx_low + tx_high + ty_low + ty_high + tz_low + tz_high)
        return [
            zero if low_end else tx_low * inverse,
            zero if high_end else tx_high * inverse,
            jnp.where(right_start, 0.0, ty_low * inverse),
            jnp.where(left_end, 0.0, ty_high * inverse),
            jnp.where(bottom, 0.0, tz_low * inverse),
            jnp.where(top, 0.0, tz_high * inverse),
            (tx_high - tx_low) * inverse,
            (ty_high - ty_low) * inverse,
            (tz_high - tz_low) * inverse,
        ]

    def coefficients(r):
        kx_low, kx, kx_high = (kp[0, pl.ds(r + 4 + d, 1)] for d in (-1, 0, 1))
        ky, kz = kp[1, pl.ds(r + 4, 1)], kp[2, pl.ds(r + 4, 1)]
        tx_low, tx_high = harmonic(kx_low, kx), harmonic(kx, kx_high)
        ty = harmonic(ky, y_next(ky))
        ty_low = jnp.where(right_start, ky, y_last(ty))
        ty_high = jnp.where(left_end, ky, ty)
        tz = harmonic(kz, z_next(kz))
        tz_low = jnp.where(bottom, kz, z_last(tz))
        tz_high = jnp.where(top, kz, tz)
        for n, value in enumerate(finish(tx_low, tx_high, ty_low, ty_high, tz_low, tz_high, False, False)):
            coef[n, pl.ds(r + 3, 1)] = value
            if n >= 6:
                q1[n - 6, pl.ds(r + 3, 1)] = W[0] * value
        if 0 <= r < 16:
            for d, value in enumerate((tx_high, ty_high, tz_high)):
                if r < 8 or d == 0:
                    face[d, pl.ds(r, 1)] = value
        if r in ENDS:
            e = ENDS.index(r)
            low, high = (tx_low, kx) if e % 2 else (kx, tx_high)
            for n, value in enumerate(finish(low, high, ty_low, ty_high, tz_low, tz_high, not e % 2, e % 2)):
                u_coef[e, pl.ds(n, 1)] = value
                if n >= 6:
                    uq[e, 0, n - 6, pl.ds(0, 1)] = W[0] * value

    def sweep(w, cs, low, mid, high):
        around = cs[2] * y_last(mid) + cs[3] * y_next(mid) + cs[4] * z_last(mid) + cs[5] * z_next(mid)
        if low is not None:
            around = around + cs[0] * low
        if high is not None:
            around = around + cs[1] * high
        return mid + w * (around + cs[6] - mid)

    def coefs_at(r, d):
        return [coef[n, pl.ds(r + 3, 1)] for n in (0, 1, 2, 3, 4, 5, 6 + d)]

    qs = [(q1, 3), (q2, 2), (q3, 1), (q4, 0)]

    def q_at(s, d, r):
        ref, offset = qs[s]
        return ref[d, pl.ds(r + offset, 1)]

    def e_at(e, s, d, n):
        r = ENDS[e] - n if e % 2 else ENDS[e] + n
        return uq[e, s, d, pl.ds(n, 1)] if n <= s else q_at(s, d, r)

    def main_row(s, r, along=range(3)):
        for d in along:
            low, mid, high = (q_at(s - 1, d, r + n) for n in (-1, 0, 1))
            ref, offset = qs[s]
            ref[d, pl.ds(r + offset, 1)] = sweep(W[s], coefs_at(r, d), low, mid, high)

    def edge_row(e, s, n, along=range(3)):
        r = ENDS[e] - n if e % 2 else ENDS[e] + n
        for d in along:
            inner, mid = e_at(e, s - 1, d, n + 1), e_at(e, s - 1, d, n)
            outer = e_at(e, s - 1, d, n - 1) if n else None
            cs = coefs_at(r, d) if n else [u_coef[e, pl.ds(m, 1)] for m in (0, 1, 2, 3, 4, 5, 6 + d)]
            low, high = (inner, outer) if e % 2 else (outer, inner)
            uq[e, s, d, pl.ds(n, 1)] = sweep(W[s], cs, low, mid, high)

    for k in (6, 7):
        arrive(k)
    merged = [jnp.where(slot_left, packs_own[0, v], packs_own[1, v]) for v in range(2)]
    for r in range(8):
        for c in range(3):
            assemble(c, r, merged)
    for r in range(1, 7):
        coefficients(r)

    for k in (2, 3, 0):
        arrive(k)
    merged = jnp.where(slot_left, packs_low[0], packs_low[1])
    for r in range(-4, 0):
        for c in range(3):
            if r > -4 or c == 0:
                assemble(c, r, merged)
    for r in range(-3, 1):
        coefficients(r)
    for k in (4, 5, 1):
        arrive(k)
    merged = jnp.where(slot_left, packs_high[0], packs_high[1])
    for c, r in DOWN:
        assemble(c, r + 8, merged)
    for r in range(7, 12):
        coefficients(r)

    for s in range(1, SWEEPS):
        for r in range(s - 4 + 1, 12 - s):
            main_row(s, r)
        for e in range(2):
            for n in range(s + 1):
                edge_row(e, s, n)

    load_map.wait()
    layer = lax.broadcasted_iota(jnp.int32, (NZ, LANES), 0)
    layer_map = jnp.zeros((NZ, LANES), jnp.int32)
    for z in range(NZ):
        layer_map = jnp.where(layer == z, map_own[z], layer_map)
    last = SWEEPS - 1
    flag_left = (j > 0).astype(F32)
    flag_right = (j < n_gy - 1).astype(F32)
    pick = (lax.broadcasted_iota(jnp.int32, (LANES, LANES), 0) // BXY == lane_of((LANES, LANES))).astype(F32)
    extents = (24, 144, 8)

    def drop(d, here, above):
        if d == 0:
            return here - above - 1.0
        if d == 1:
            return here - jnp.where(left_end, 0.0, y_next(here)) - 1.0
        return here - jnp.where(top, 0.0, z_next(here)) - 1.0

    def coarse(first, along, flag_up, flag_low):
        e_low, e_high = ENDS.index(first), ENDS.index(first + 7)
        sums = []
        for d in along:
            def terms(n, here, above, at_end=False):
                fall = drop(d, here, above)
                square = fall * fall
                t = kp[0, pl.ds(first + n + 4, 1)] if at_end else face[d, pl.ds(first + n, 1)]
                return jnp.concatenate([t * square, square], axis=0)

            def main_at(n):
                return q_at(last, d, first + n)

            main = [terms(n, main_at(n), main_at(n + 1) if d == 0 else None) for n in range(8)]
            up = [terms(n, e_at(e_low, last, d, n), e_at(e_low, last, d, n + 1)) for n in range(4)]
            low = [
                terms(
                    n, e_at(e_high, last, d, 7 - n), zero if n == 7 else e_at(e_high, last, d, 6 - n), d == 0 and n == 7
                )
                for n in range(4, 8)
            ]
            third = terms(3, main_at(3), e_at(e_high, last, d, 3)) if d == 0 else main[3]
            main_low = main[0] + main[1] + main[2]
            main_high = main[4] + main[5] + main[6] + main[7]
            total = main_low + main[3] + main_high
            total = total + flag_up * (up[0] + up[1] + up[2] + up[3] + main_high)
            total = total + flag_low * (main_low + third + low[0] + low[1] + low[2] + low[3])
            own, other = total[:, :, 0:LANES], total[:, :, LANES : 2 * LANES]
            lane3 = lane_of(own.shape)
            left = pltpu.roll(other, LANES - LEFT_AT - 4, axis=2) * flag_left
            right = pltpu.roll(other, LANES - RIGHT_AT - 8, axis=2) * flag_right
            own = own + jnp.where(lane3 < 8, left, 0.0) + jnp.where(lane3 >= LANES - 8, right, 0.0)
            sums.append(own)
        count = len(along)
        stack = jnp.concatenate(sums, axis=0).reshape(2 * count * NZ, LANES)
        blocks = jnp.dot(stack, pick, precision=lax.Precision.HIGHEST, preferred_element_type=F32)
        blocks = blocks.reshape(count, 2, NZ, LANES)
        perm = [[None] * NCL for _ in along]
        for n in range(NCL):
            for at, d in enumerate(along):
                held = jnp.where(layer_map == n, blocks[at], 0.0)
                both = jnp.sum(held, axis=1, keepdims=True)
                perm[at][n] = both[0] / (both[1] + EPS * extents[d] * extents[d])
        return perm

    perm = coarse(0, range(3), (i < n_gx - 1).astype(F32), (i > 0).astype(F32))
    mess[...] = jnp.concatenate(perm[0] + perm[1], axis=0)

    def tell(k, di, dj, target):
        return pltpu.make_async_remote_copy(
            src_ref=mess, dst_ref=target, send_sem=send_sem.at[k], recv_sem=recv_sem.at[k],
            device_id=device(di, dj), device_id_type=MESH,
        )

    first_k = len(copies)
    last_copies = [
        (tell(first_k, -1, 0, mess_x), inside(-1, 0) & jnp.logical_not(reaches(-1, 0)), inside(1, 0)),
        (tell(first_k + 1, 0, -1, mess_y), inside(0, -1), inside(0, 1)),
    ]
    for copy, sends, _ in last_copies:
        pl.when(sends)(copy.start)
    copies.extend(last_copies)
    for d in range(3):
        for n in range(NCL):
            perm_ref[d, n] = perm[d][n][:, 0 : LANES // BXY]
    for n in range(NCL):
        value = harmonic(perm[2][n], perm[2][n + 1]) if n < NCL - 1 else jnp.zeros((1, LANES), F32)
        trans_ref[2, n] = value[:, 0 : LANES // BXY]

    @pl.when(reaches(0, 0))
    def _():
        for k in range(8, 14):
            arrive(k)
        merged = jnp.where(slot_left, packs_more[0], packs_more[1])
        for c, r in PLANES[len(DOWN) :]:
            assemble(c, r + 8, merged)
        merged = jnp.where(slot_left, packs_far[0], packs_far[1])
        for c, r in DOWN:
            assemble(c, r + 16, merged)
        for r in [8] + list(range(12, 20)):
            coefficients(r)
        for s in range(1, SWEEPS):
            for r in range(12 - s, 20 - s):
                main_row(s, r, (0,))
            for e in (2, 3):
                for n in range(s + 1):
                    edge_row(e, s, n, (0,))
        (beyond,) = coarse(8, (0,), (i + 2 < n_gx).astype(F32), 1.0)
        mess_x[pl.ds(0, NCL)] = jnp.concatenate(beyond, axis=0)

    @pl.when(jnp.logical_not(reaches(0, 0)))
    def _():
        arrive(first_k)

    arrive(first_k + 1)
    lane1 = lane_of((1, LANES))
    for n in range(NCL):
        trans_ref[0, n] = harmonic(perm[0][n], mess_x[pl.ds(n, 1)])[:, 0 : LANES // BXY]
        beyond = pltpu.roll(mess_y[pl.ds(NCL + n, 1)], LANES // BXY - 1, axis=1)
        after = jnp.where(lane1 == LANES // BXY - 1, beyond, pltpu.roll(perm[1][n], LANES - 1, axis=1))
        trans_ref[1, n] = harmonic(perm[1][n], after)[:, 0 : LANES // BXY]
    for copy, sends, _ in copies:
        pl.when(sends)(copy.wait_send)


def solution(mesh):
    n_gx, n_gy = mesh.shape["gx"], mesh.shape["gy"]

    def local(permeability, layer_map):
        k = permeability.reshape(3 * NZ * BXY, LANES)
        out = jax.ShapeDtypeStruct((3, NCL, 1, LANES // BXY), F32)
        vmem = lambda *shape: pltpu.VMEM(shape, F32)
        both = 2 * LANES
        return pl.pallas_call(
            lambda *refs: kernel(n_gx, n_gy, *refs),
            out_shape=(out, out),
            in_specs=[pl.BlockSpec(memory_space=pltpu.HBM)] * 2,
            out_specs=(pl.BlockSpec(memory_space=pltpu.VMEM),) * 2,
            scratch_shapes=[
                vmem(3 * NZ * BXY, LANES),
                pltpu.SMEM((NZ,), jnp.int32),
                vmem(len(PLANES), NZ, LANES),
                vmem(2, NZ, LANES),
                vmem(len(UP), NZ, LANES),
                vmem(len(DOWN), NZ, LANES),
                vmem(2, 2, NZ, LANES),
                vmem(2, NZ, LANES),
                vmem(2, NZ, LANES),
                vmem(len(PLANES) - len(DOWN), NZ, LANES),
                vmem(len(DOWN), NZ, LANES),
                vmem(2, NZ, LANES),
                vmem(2, NZ, LANES),
                vmem(3, 25, NZ, both),
                vmem(9, 23, NZ, both),
                vmem(3, 16, NZ, both),
                vmem(3, 23, NZ, both),
                vmem(3, 21, NZ, both),
                vmem(3, 19, NZ, both),
                vmem(3, 17, NZ, both),
                vmem(4, 9, NZ, both),
                vmem(4, SWEEPS, 3, SWEEPS, NZ, both),
                vmem(NZ, LANES),
                vmem(NZ, LANES),
                vmem(NZ, LANES),
                pltpu.SemaphoreType.DMA((2,)),
                pltpu.SemaphoreType.DMA((16,)),
                pltpu.SemaphoreType.DMA((16,)),
            ],
            compiler_params=pltpu.CompilerParams(
                collective_id=0, has_side_effects=True, vmem_limit_bytes=63000000
            ),
            name="upscale",
        )(k, layer_map)

    spec = P(None, None, "gx", "gy")
    return jax.shard_map(local, mesh=mesh, in_specs=(spec, P()), out_specs=(spec, spec), check_vma=False)
```

```python
import math

import jax
import jax.numpy as jnp
from jax import lax
from jax.experimental import pallas as pl
from jax.experimental.pallas import tpu as pltpu
from jax.sharding import PartitionSpec as P

MESH = pl.DeviceIdType.MESH
NCL = 4
BXY = 8
SWEEPS = 4
KMIN = 0.01
EPS = 1e-06
NZ = 8
LANES = 128
F32 = jnp.float32

DOWN = [(1, r) for r in range(4)] + [(2, r) for r in range(4)] + [(0, r) for r in range(5)]
UP = [(0, r) for r in range(4, 8)] + [(1, r) for r in range(5, 8)] + [(2, r) for r in range(5, 8)]
PLANES = DOWN + UP[1:] + [(1, 4), (2, 4)]
PLANE_AT = {cr: at for at, cr in enumerate(PLANES)}
UP_FROM = PLANE_AT[UP[0]]
LAST, FIRST = 4, 13
PER_PACK = LANES // FIRST
UP_SET = UP + [(1, 4), (2, 4)]
PACKS = [DOWN[:PER_PACK], DOWN[PER_PACK:], UP_SET[:PER_PACK], UP_SET[PER_PACK:]]
UP_SLOT = {cr: (at // PER_PACK, at % PER_PACK * FIRST) for at, cr in enumerate(UP_SET)}
SLOT_OF = {cr: (2 + v, s) for cr, (v, s) in UP_SLOT.items()}
SLOT_OF.update({cr: (at // PER_PACK, at % PER_PACK * FIRST) for at, cr in enumerate(DOWN)})
DIRECTIONS = [(1, 0), (-1, 0), (1, 1), (1, -1), (-1, 1), (-1, -1), (0, 1), (0, -1)]
LOW, HIGH, OWN, FAR = range(4)
MORE = [(-1, 0), (-1, -1), (-2, 0), (-2, 1), (-2, -1)]
ENDS = [0, 7, 8, 15]
LEFT_AT = 20
RIGHT_AT = 72
W = [1.0 / (1.05 + 0.95 * math.cos(math.pi * (2 * s + 1) / (2 * SWEEPS))) for s in range(SWEEPS)]


def harmonic(left, right):
    return 2.0 * left * right / (left + right)


def lane_of(shape):
    return lax.broadcasted_iota(jnp.int32, shape, len(shape) - 1)


def between(lane, low, high):
    return (lane >= low) & (lane < high)


def kernel(
    n_gx, n_gy, k_hbm, map_hbm, perm_ref, trans_ref,
    k_own, map_own, planes, lasts, packs, from_low, from_high, from_more, from_far,
    near_lasts, own_packs, low_packs, high_packs, far_packs,
    kp, coef, face, q1, q2, q3, q4, u_coef, uq, mess, mess_x,
    load_sem, send_sem, recv_sem,
):
    i, j = lax.axis_index("gx"), lax.axis_index("gy")
    load_k = pltpu.make_async_copy(k_hbm, k_own, load_sem.at[0])
    load_map = pltpu.make_async_copy(map_hbm, map_own, load_sem.at[1])
    load_k.start()
    load_map.start()

    def inside(di, dj):
        tests = []
        if di:
            tests.append(i + di < n_gx if di > 0 else i >= -di)
        if dj:
            tests.append(j + dj < n_gy if dj > 0 else j >= -dj)
        return tests[0] if len(tests) == 1 else tests[0] & tests[1]

    def device(di, dj):
        return {"gx": i + di, "gy": j + dj}

    def reaches(di):
        row = i + di
        return (lax.rem(row + 4, 4) == 1) & (row + 1 < n_gx)

    barrier = pltpu.get_barrier_semaphore()
    for di, dj in DIRECTIONS:
        @pl.when(inside(di, dj))
        def _():
            pl.semaphore_signal(barrier, inc=1, device_id=device(di, dj), device_id_type=MESH)

    signals = 0
    for di, dj in MORE[2:]:
        @pl.when(inside(-di, -dj) & reaches(0))
        def _():
            pl.semaphore_signal(barrier, inc=1, device_id=device(-di, -dj), device_id_type=MESH)

        signals = signals + (inside(di, dj) & reaches(di)).astype(jnp.int32)

    lane = lane_of((NZ, LANES))
    load_k.wait()
    packed = [jnp.zeros((NZ, LANES), F32)] * len(PACKS)
    last_of = jnp.zeros((NZ, LANES), F32)
    for at, (c, r) in enumerate(PLANES):
        plane = k_own[pl.ds(c * 64 + r, NZ, stride=8), :]
        planes[at] = plane
        last_of = jnp.where(between(lane, LAST * at, LAST * at + LAST), pltpu.roll(plane, LAST * at + LAST, axis=1), last_of)
        for v, pack in enumerate(PACKS):
            if (c, r) in pack:
                s = FIRST * pack.index((c, r))
                first_of = pltpu.roll(plane, s, axis=1) if s else plane
                packed[v] = jnp.where(between(lane, s, s + FIRST), first_of, packed[v])
    lasts[...] = last_of
    for v, value in enumerate(packed):
        packs[v] = value

    rows_near = 1 + (i > 0).astype(jnp.int32) + (i < n_gx - 1).astype(jnp.int32)
    cols_near = 1 + (j > 0).astype(jnp.int32) + (j < n_gy - 1).astype(jnp.int32)
    pl.semaphore_wait(barrier, rows_near * cols_near - 1 + signals)

    low_half, high_half = pl.ds(0, 2), pl.ds(2, 2)

    def remote(k, source, target, di, dj):
        return pltpu.make_async_remote_copy(
            src_ref=source, dst_ref=target, send_sem=send_sem.at[k], recv_sem=recv_sem.at[k],
            device_id=device(di, dj), device_id_type=MESH,
        )

    def copy_of(k, di, dj):
        if dj == 0:
            if di > 0:
                return remote(k, planes.at[pl.ds(UP_FROM, len(UP))], from_low, di, dj)
            return remote(k, planes.at[pl.ds(0, len(DOWN))], from_high, di, dj)
        if dj > 0:
            return remote(k, lasts, near_lasts.at[LOW if di > 0 else HIGH if di < 0 else OWN], di, dj)
        if di == 0:
            return remote(k, packs, own_packs, di, dj)
        if di > 0:
            return remote(k, packs.at[high_half], low_packs, di, dj)
        return remote(k, packs.at[low_half], high_packs.at[low_half], di, dj)

    def more_of(k, di, dj):
        if di == -1:
            if dj == 0:
                return remote(k, planes.at[pl.ds(len(DOWN), len(PLANES) - len(DOWN))], from_more, di, dj)
            return remote(k, packs.at[high_half], high_packs.at[high_half], di, dj)
        if dj == 0:
            return remote(k, planes.at[pl.ds(0, len(DOWN))], from_far, di, dj)
        if dj > 0:
            return remote(k, lasts, near_lasts.at[FAR], di, dj)
        return remote(k, packs.at[low_half], far_packs, di, dj)

    copies = [(copy_of(k, *to), inside(*to), inside(-to[0], -to[1])) for k, to in enumerate(DIRECTIONS)]
    for k, (di, dj) in enumerate(MORE):
        sends = inside(di, dj) & reaches(di)
        copies.append((more_of(len(DIRECTIONS) + k, di, dj), sends, inside(-di, -dj)))
    for copy, sends, _ in copies:
        pl.when(sends)(copy.start)

    def arrive(k):
        copy, _, here = copies[k]
        target = copy.dst_ref
        pl.when(here)(copy.wait_recv)

        @pl.when(jnp.logical_not(here))
        def _():
            target[...] = jnp.zeros(target.shape, F32)

    edge = (lane >= LANES - LAST) | (lane < FIRST)

    def assemble(c, r):
        if 0 <= r < 8:
            at, v, s = PLANE_AT[c, r], *SLOT_OF[c, r]
            own, side, firsts = planes[at], OWN, own_packs[v]
        elif r < 0:
            at, v, s = PLANE_AT[c, r + 8], *UP_SLOT[c, r + 8]
            own, side, firsts = from_low[at - UP_FROM], LOW, low_packs[v]
        elif r >= 16:
            at, v, s = PLANE_AT[c, r - 16], *SLOT_OF[c, r - 16]
            own, side, firsts = from_far[at], FAR, far_packs[v]
        else:
            at, v, s = PLANE_AT[c, r - 8], *SLOT_OF[c, r - 8]
            own = from_high[at] if at < len(DOWN) else from_more[at - len(DOWN)]
            side, firsts = HIGH, high_packs[v]
        before = pltpu.roll(near_lasts[side], LANES - LAST - LAST * at, axis=1)
        after = pltpu.roll(firsts, LANES - s, axis=1) if s else firsts
        margin = jnp.where(lane < FIRST, after, before)
        left = pltpu.roll(jnp.where(lane >= LANES - LAST, margin, own), LEFT_AT + 4, axis=1)
        right = pltpu.roll(jnp.where(lane < BXY, margin, own), RIGHT_AT + 8, axis=1)
        other = jnp.where(between(lane, LEFT_AT, LEFT_AT + 12), left, 1.0)
        other = jnp.where(between(lane, RIGHT_AT, RIGHT_AT + 16), right, other)
        other = jnp.where(edge, margin, other)
        kp[c, r + 4, :, 0:LANES] = own + KMIN
        kp[c, r + 4, :, LANES : 2 * LANES] = other + KMIN

    lane2 = lane_of((1, NZ, 2 * LANES))
    layer2 = lax.broadcasted_iota(jnp.int32, (1, NZ, 2 * LANES), 1)
    left_end = (lane2 == LANES + LEFT_AT + 11) | (lane2 == LANES + RIGHT_AT + 15)
    right_start = lane2 == LANES + RIGHT_AT
    top, bottom = layer2 == NZ - 1, layer2 == 0
    zero = jnp.zeros((1, NZ, 2 * LANES), F32)

    def y_next(v):
        return pltpu.roll(v, 2 * LANES - 1, axis=2)

    def y_last(v):
        return pltpu.roll(v, 1, axis=2)

    def z_next(v):
        return pltpu.roll(v, NZ - 1, axis=1)

    def z_last(v):
        return pltpu.roll(v, 1, axis=1)

    def finish(tx_low, tx_high, ty_low, ty_high, tz_low, tz_high, low_end, high_end):
        inverse = 1.0 / (tx_low + tx_high + ty_low + ty_high + tz_low + tz_high)
        return [
            zero if low_end else tx_low * inverse,
            zero if high_end else tx_high * inverse,
            jnp.where(right_start, 0.0, ty_low * inverse),
            jnp.where(left_end, 0.0, ty_high * inverse),
            jnp.where(bottom, 0.0, tz_low * inverse),
            jnp.where(top, 0.0, tz_high * inverse),
            (tx_high - tx_low) * inverse,
            (ty_high - ty_low) * inverse,
            (tz_high - tz_low) * inverse,
        ]

    def coefficients(r):
        kx_low, kx, kx_high = (kp[0, pl.ds(r + 4 + d, 1)] for d in (-1, 0, 1))
        ky, kz = kp[1, pl.ds(r + 4, 1)], kp[2, pl.ds(r + 4, 1)]
        tx_low, tx_high = harmonic(kx_low, kx), harmonic(kx, kx_high)
        ty = harmonic(ky, y_next(ky))
        ty_low = jnp.where(right_start, ky, y_last(ty))
        ty_high = jnp.where(left_end, ky, ty)
        tz = harmonic(kz, z_next(kz))
        tz_low = jnp.where(bottom, kz, z_last(tz))
        tz_high = jnp.where(top, kz, tz)
        for n, value in enumerate(finish(tx_low, tx_high, ty_low, ty_high, tz_low, tz_high, False, False)):
            coef[n, pl.ds(r + 3, 1)] = value
            if n >= 6:
                q1[n - 6, pl.ds(r + 3, 1)] = W[0] * value
        if 0 <= r < 16:
            for d, value in enumerate((tx_high, ty_high, tz_high)):
                if r < 8 or d == 0:
                    face[d, pl.ds(r, 1)] = value
        if r in ENDS:
            e = ENDS.index(r)
            low, high = (tx_low, kx) if e % 2 else (kx, tx_high)
            for n, value in enumerate(finish(low, high, ty_low, ty_high, tz_low, tz_high, not e % 2, e % 2)):
                u_coef[e, pl.ds(n, 1)] = value
                if n >= 6:
                    uq[e, 0, n - 6, pl.ds(0, 1)] = W[0] * value

    def sweep(w, cs, low, mid, high):
        around = cs[2] * y_last(mid) + cs[3] * y_next(mid) + cs[4] * z_last(mid) + cs[5] * z_next(mid)
        if low is not None:
            around = around + cs[0] * low
        if high is not None:
            around = around + cs[1] * high
        return mid + w * (around + cs[6] - mid)

    def coefs_at(r, d):
        return [coef[n, pl.ds(r + 3, 1)] for n in (0, 1, 2, 3, 4, 5, 6 + d)]

    qs = [(q1, 3), (q2, 2), (q3, 1), (q4, 0)]

    def q_at(s, d, r):
        ref, offset = qs[s]
        return ref[d, pl.ds(r + offset, 1)]

    def e_at(e, s, d, n):
        r = ENDS[e] - n if e % 2 else ENDS[e] + n
        return uq[e, s, d, pl.ds(n, 1)] if n <= s else q_at(s, d, r)

    def main_row(s, r, along=range(3)):
        for d in along:
            low, mid, high = (q_at(s - 1, d, r + n) for n in (-1, 0, 1))
            ref, offset = qs[s]
            ref[d, pl.ds(r + offset, 1)] = sweep(W[s], coefs_at(r, d), low, mid, high)

    def edge_row(e, s, n, along=range(3)):
        r = ENDS[e] - n if e % 2 else ENDS[e] + n
        for d in along:
            inner, mid = e_at(e, s - 1, d, n + 1), e_at(e, s - 1, d, n)
            outer = e_at(e, s - 1, d, n - 1) if n else None
            cs = coefs_at(r, d) if n else [u_coef[e, pl.ds(m, 1)] for m in (0, 1, 2, 3, 4, 5, 6 + d)]
            low, high = (inner, outer) if e % 2 else (outer, inner)
            uq[e, s, d, pl.ds(n, 1)] = sweep(W[s], cs, low, mid, high)

    for k in (6, 7):
        arrive(k)
    for r in range(8):
        for c in range(3):
            assemble(c, r)
    for r in range(1, 7):
        coefficients(r)

    for k in (2, 3, 0):
        arrive(k)
    for c, r in UP:
        assemble(c, r - 8)
    for r in range(-3, 1):
        coefficients(r)
    for k in (4, 5, 1):
        arrive(k)
    for c, r in DOWN:
        assemble(c, r + 8)
    for r in range(7, 12):
        coefficients(r)

    for s in range(1, SWEEPS):
        for r in range(s - 4 + 1, 12 - s):
            main_row(s, r)
        for e in range(2):
            for n in range(s + 1):
                edge_row(e, s, n)

    load_map.wait()
    layer = lax.broadcasted_iota(jnp.int32, (NZ, LANES), 0)
    layer_map = jnp.zeros((NZ, LANES), jnp.int32)
    for z in range(NZ):
        layer_map = jnp.where(layer == z, map_own[z], layer_map)
    last = SWEEPS - 1
    flag_left = (j > 0).astype(F32)
    flag_right = (j < n_gy - 1).astype(F32)
    pick = (lax.broadcasted_iota(jnp.int32, (LANES, LANES), 0) // BXY == lane_of((LANES, LANES))).astype(F32)
    extents = (24, 144, 8)

    def drop(d, here, above):
        if d == 0:
            return here - above - 1.0
        if d == 1:
            return here - jnp.where(left_end, 0.0, y_next(here)) - 1.0
        return here - jnp.where(top, 0.0, z_next(here)) - 1.0

    def coarse(first, along, flag_up, flag_low):
        e_low, e_high = ENDS.index(first), ENDS.index(first + 7)
        sums = []
        for d in along:
            def terms(n, here, above, at_end=False):
                fall = drop(d, here, above)
                square = fall * fall
                t = kp[0, pl.ds(first + n + 4, 1)] if at_end else face[d, pl.ds(first + n, 1)]
                return jnp.concatenate([t * square, square], axis=0)

            def main_at(n):
                return q_at(last, d, first + n)

            main = [terms(n, main_at(n), main_at(n + 1) if d == 0 else None) for n in range(8)]
            up = [terms(n, e_at(e_low, last, d, n), e_at(e_low, last, d, n + 1)) for n in range(4)]
            low = [
                terms(
                    n, e_at(e_high, last, d, 7 - n), zero if n == 7 else e_at(e_high, last, d, 6 - n), d == 0 and n == 7
                )
                for n in range(4, 8)
            ]
            third = terms(3, main_at(3), e_at(e_high, last, d, 3)) if d == 0 else main[3]
            main_low = main[0] + main[1] + main[2]
            main_high = main[4] + main[5] + main[6] + main[7]
            total = main_low + main[3] + main_high
            total = total + flag_up * (up[0] + up[1] + up[2] + up[3] + main_high)
            total = total + flag_low * (main_low + third + low[0] + low[1] + low[2] + low[3])
            own, other = total[:, :, 0:LANES], total[:, :, LANES : 2 * LANES]
            lane3 = lane_of(own.shape)
            left = pltpu.roll(other, LANES - LEFT_AT - 4, axis=2) * flag_left
            right = pltpu.roll(other, LANES - RIGHT_AT - 8, axis=2) * flag_right
            own = own + jnp.where(lane3 < 8, left, 0.0) + jnp.where(lane3 >= LANES - 8, right, 0.0)
            sums.append(own)
            if d == 1:
                after = other + pltpu.roll(other, LANES - RIGHT_AT - 8, axis=2)
        if len(along) == 3:
            sums.append(after)
            along = [*along, 1]
        count = len(along)
        stack = jnp.concatenate(sums, axis=0).reshape(2 * count * NZ, LANES)
        blocks = jnp.dot(stack, pick, precision=lax.Precision.HIGHEST, preferred_element_type=F32)
        blocks = blocks.reshape(count, 2, NZ, LANES)
        perm = [[None] * NCL for _ in along]
        for n in range(NCL):
            for at, d in enumerate(along):
                held = jnp.where(layer_map == n, blocks[at], 0.0)
                both = jnp.sum(held, axis=1, keepdims=True)
                perm[at][n] = both[0] / (both[1] + EPS * extents[d] * extents[d])
        return perm

    perm = coarse(0, range(3), (i < n_gx - 1).astype(F32), (i > 0).astype(F32))
    mess[pl.ds(0, NCL)] = jnp.concatenate(perm[0], axis=0)

    tell_k = len(copies)
    tell = remote(tell_k, mess, mess_x, -1, 0)
    sends = inside(-1, 0) & jnp.logical_not(reaches(-1))
    pl.when(sends)(tell.start)
    copies.append((tell, sends, inside(1, 0)))
    for d in range(3):
        for n in range(NCL):
            perm_ref[d, n] = perm[d][n][:, 0 : LANES // BXY]
    for n in range(NCL):
        value = harmonic(perm[2][n], perm[2][n + 1]) if n < NCL - 1 else jnp.zeros((1, LANES), F32)
        trans_ref[2, n] = value[:, 0 : LANES // BXY]

    exists = (j < n_gy - 1).astype(F32)
    lane1 = lane_of((1, LANES))
    for n in range(NCL):
        beyond = pltpu.roll(perm[3][n], LANES // BXY - 1, axis=1) * exists
        after = jnp.where(lane1 == LANES // BXY - 1, beyond, pltpu.roll(perm[1][n], LANES - 1, axis=1))
        trans_ref[1, n] = harmonic(perm[1][n], after)[:, 0 : LANES // BXY]

    @pl.when(reaches(0))
    def _():
        for k in range(8, 13):
            arrive(k)
        for c, r in PLANES[len(DOWN) :]:
            assemble(c, r + 8)
        for c, r in DOWN:
            assemble(c, r + 16)
        for r in [8] + list(range(12, 20)):
            coefficients(r)
        for s in range(1, SWEEPS):
            for r in range(12 - s, 20 - s):
                main_row(s, r, (0,))
            for e in (2, 3):
                for n in range(s + 1):
                    edge_row(e, s, n, (0,))
        (beyond,) = coarse(8, (0,), (i + 2 < n_gx).astype(F32), 1.0)
        mess_x[pl.ds(0, NCL)] = jnp.concatenate(beyond, axis=0)

    @pl.when(jnp.logical_not(reaches(0)))
    def _():
        arrive(tell_k)

    for n in range(NCL):
        trans_ref[0, n] = harmonic(perm[0][n], mess_x[pl.ds(n, 1)])[:, 0 : LANES // BXY]
    for copy, sends, _ in copies:
        pl.when(sends)(copy.wait_send)


def solution(mesh):
    n_gx, n_gy = mesh.shape["gx"], mesh.shape["gy"]

    def local(permeability, layer_map):
        k = permeability.reshape(3 * NZ * BXY, LANES)
        out = jax.ShapeDtypeStruct((3, NCL, 1, LANES // BXY), F32)
        vmem = lambda *shape: pltpu.VMEM(shape, F32)
        both = 2 * LANES
        return pl.pallas_call(
            lambda *refs: kernel(n_gx, n_gy, *refs),
            out_shape=(out, out),
            in_specs=[pl.BlockSpec(memory_space=pltpu.HBM)] * 2,
            out_specs=(pl.BlockSpec(memory_space=pltpu.VMEM),) * 2,
            scratch_shapes=[
                vmem(3 * NZ * BXY, LANES),
                pltpu.SMEM((NZ,), jnp.int32),
                vmem(len(PLANES), NZ, LANES),
                vmem(NZ, LANES),
                vmem(4, NZ, LANES),
                vmem(len(UP), NZ, LANES),
                vmem(len(DOWN), NZ, LANES),
                vmem(len(PLANES) - len(DOWN), NZ, LANES),
                vmem(len(DOWN), NZ, LANES),
                vmem(4, NZ, LANES),
                vmem(4, NZ, LANES),
                vmem(2, NZ, LANES),
                vmem(4, NZ, LANES),
                vmem(2, NZ, LANES),
                vmem(3, 25, NZ, both),
                vmem(9, 23, NZ, both),
                vmem(3, 16, NZ, both),
                vmem(3, 23, NZ, both),
                vmem(3, 21, NZ, both),
                vmem(3, 19, NZ, both),
                vmem(3, 17, NZ, both),
                vmem(4, 9, NZ, both),
                vmem(4, SWEEPS, 3, SWEEPS, NZ, both),
                vmem(NZ, LANES),
                vmem(NZ, LANES),
                pltpu.SemaphoreType.DMA((2,)),
                pltpu.SemaphoreType.DMA((14,)),
                pltpu.SemaphoreType.DMA((14,)),
            ],
            compiler_params=pltpu.CompilerParams(
                collective_id=0, has_side_effects=True, vmem_limit_bytes=56440000
            ),
            name="upscale",
        )(k, layer_map)

    spec = P(None, None, "gx", "gy")
    return jax.shard_map(local, mesh=mesh, in_specs=(spec, P()), out_specs=(spec, spec), check_vma=False)
```

```python
import math

import jax
import jax.numpy as jnp
from jax import lax
from jax.experimental import pallas as pl
from jax.experimental.pallas import tpu as pltpu
from jax.sharding import PartitionSpec as P

MESH = pl.DeviceIdType.MESH
NCL = 4
BXY = 8
SWEEPS = 4
KMIN = 0.01
EPS = 1e-06
NZ = 8
LANES = 128
F32 = jnp.float32

DOWN = [(1, r) for r in range(4)] + [(2, r) for r in range(4)] + [(0, r) for r in range(5)]
UP = [(0, r) for r in range(4, 8)] + [(1, r) for r in range(5, 8)] + [(2, r) for r in range(5, 8)]
PLANES = DOWN + UP[1:] + [(1, 4), (2, 4)]
PLANE_AT = {cr: at for at, cr in enumerate(PLANES)}
UP_FROM = PLANE_AT[UP[0]]
LAST, FIRST = 4, 13
PER_PACK = LANES // FIRST
UP_SET = UP + [(1, 4), (2, 4)]
PACKS = [DOWN[:PER_PACK], DOWN[PER_PACK:], UP_SET[:PER_PACK], UP_SET[PER_PACK:]]
UP_SLOT = {cr: (at // PER_PACK, at % PER_PACK * FIRST) for at, cr in enumerate(UP_SET)}
SLOT_OF = {cr: (2 + v, s) for cr, (v, s) in UP_SLOT.items()}
SLOT_OF.update({cr: (at // PER_PACK, at % PER_PACK * FIRST) for at, cr in enumerate(DOWN)})
DIRECTIONS = [(1, 0), (-1, 0), (1, 1), (1, -1), (-1, 1), (-1, -1), (0, 1), (0, -1)]
LOW, HIGH, OWN, FAR = range(4)
MORE = [(-1, 0), (-1, -1), (-2, 0), (-2, 1), (-2, -1)]
ENDS = [0, 7, 8, 15]
LEFT_AT = 20
RIGHT_AT = 72
W = [1.0 / (1.05 + 0.95 * math.cos(math.pi * (2 * s + 1) / (2 * SWEEPS))) for s in range(SWEEPS)]


def harmonic(left, right):
    return 2.0 * left * right / (left + right)


def lane_of(shape):
    return lax.broadcasted_iota(jnp.int32, shape, len(shape) - 1)


def between(lane, low, high):
    return (lane >= low) & (lane < high)


def kernel(
    n_gx, n_gy, k_hbm, map_hbm, perm_ref, trans_ref,
    k_own, map_own, planes, lasts, packs, from_low, from_high, from_more, from_far,
    near_lasts, own_packs, low_packs, high_packs, far_packs,
    kp, coef, face, q1, q2, q3, q4, u_coef, uq, mess, mess_x,
    load_sem, send_sem, recv_sem,
):
    i, j = lax.axis_index("gx"), lax.axis_index("gy")
    load_k = pltpu.make_async_copy(k_hbm, k_own, load_sem.at[0])
    load_map = pltpu.make_async_copy(map_hbm, map_own, load_sem.at[1])
    load_k.start()
    load_map.start()

    def inside(di, dj):
        tests = []
        if di:
            tests.append(i + di < n_gx if di > 0 else i >= -di)
        if dj:
            tests.append(j + dj < n_gy if dj > 0 else j >= -dj)
        return tests[0] if len(tests) == 1 else tests[0] & tests[1]

    def device(di, dj):
        return {"gx": i + di, "gy": j + dj}

    def reaches(di):
        row = i + di
        return (lax.rem(row + 2, 2) == 1) & (row + 1 < n_gx)

    barrier = pltpu.get_barrier_semaphore()
    for di, dj in DIRECTIONS:
        @pl.when(inside(di, dj))
        def _():
            pl.semaphore_signal(barrier, inc=1, device_id=device(di, dj), device_id_type=MESH)

    signals = 0
    for di, dj in MORE[2:]:
        @pl.when(inside(-di, -dj) & reaches(0))
        def _():
            pl.semaphore_signal(barrier, inc=1, device_id=device(-di, -dj), device_id_type=MESH)

        signals = signals + (inside(di, dj) & reaches(di)).astype(jnp.int32)

    lane = lane_of((NZ, LANES))
    load_k.wait()
    packed = [jnp.zeros((NZ, LANES), F32)] * len(PACKS)
    last_of = jnp.zeros((NZ, LANES), F32)
    for at, (c, r) in enumerate(PLANES):
        plane = k_own[pl.ds(c * 64 + r, NZ, stride=8), :]
        planes[at] = plane
        last_of = jnp.where(between(lane, LAST * at, LAST * at + LAST), pltpu.roll(plane, LAST * at + LAST, axis=1), last_of)
        for v, pack in enumerate(PACKS):
            if (c, r) in pack:
                s = FIRST * pack.index((c, r))
                first_of = pltpu.roll(plane, s, axis=1) if s else plane
                packed[v] = jnp.where(between(lane, s, s + FIRST), first_of, packed[v])
    lasts[...] = last_of
    for v, value in enumerate(packed):
        packs[v] = value

    rows_near = 1 + (i > 0).astype(jnp.int32) + (i < n_gx - 1).astype(jnp.int32)
    cols_near = 1 + (j > 0).astype(jnp.int32) + (j < n_gy - 1).astype(jnp.int32)
    pl.semaphore_wait(barrier, rows_near * cols_near - 1 + signals)

    low_half, high_half = pl.ds(0, 2), pl.ds(2, 2)

    def remote(k, source, target, di, dj):
        return pltpu.make_async_remote_copy(
            src_ref=source, dst_ref=target, send_sem=send_sem.at[k], recv_sem=recv_sem.at[k],
            device_id=device(di, dj), device_id_type=MESH,
        )

    def copy_of(k, di, dj):
        if dj == 0:
            if di > 0:
                return remote(k, planes.at[pl.ds(UP_FROM, len(UP))], from_low, di, dj)
            return remote(k, planes.at[pl.ds(0, len(DOWN))], from_high, di, dj)
        if dj > 0:
            return remote(k, lasts, near_lasts.at[LOW if di > 0 else HIGH if di < 0 else OWN], di, dj)
        if di == 0:
            return remote(k, packs, own_packs, di, dj)
        if di > 0:
            return remote(k, packs.at[high_half], low_packs, di, dj)
        return remote(k, packs.at[low_half], high_packs.at[low_half], di, dj)

    def more_of(k, di, dj):
        if di == -1:
            if dj == 0:
                return remote(k, planes.at[pl.ds(len(DOWN), len(PLANES) - len(DOWN))], from_more, di, dj)
            return remote(k, packs.at[high_half], high_packs.at[high_half], di, dj)
        if dj == 0:
            return remote(k, planes.at[pl.ds(0, len(DOWN))], from_far, di, dj)
        if dj > 0:
            return remote(k, lasts, near_lasts.at[FAR], di, dj)
        return remote(k, packs.at[low_half], far_packs, di, dj)

    copies = [(copy_of(k, *to), inside(*to), inside(-to[0], -to[1])) for k, to in enumerate(DIRECTIONS)]
    for k, (di, dj) in enumerate(MORE):
        sends = inside(di, dj) & reaches(di)
        copies.append((more_of(len(DIRECTIONS) + k, di, dj), sends, inside(-di, -dj)))
    for copy, sends, _ in copies:
        pl.when(sends)(copy.start)

    def arrive(k):
        copy, _, here = copies[k]
        target = copy.dst_ref
        pl.when(here)(copy.wait_recv)

        @pl.when(jnp.logical_not(here))
        def _():
            target[...] = jnp.zeros(target.shape, F32)

    edge = (lane >= LANES - LAST) | (lane < FIRST)

    def assemble(c, r):
        if 0 <= r < 8:
            at, v, s = PLANE_AT[c, r], *SLOT_OF[c, r]
            own, side, firsts = planes[at], OWN, own_packs[v]
        elif r < 0:
            at, v, s = PLANE_AT[c, r + 8], *UP_SLOT[c, r + 8]
            own, side, firsts = from_low[at - UP_FROM], LOW, low_packs[v]
        elif r >= 16:
            at, v, s = PLANE_AT[c, r - 16], *SLOT_OF[c, r - 16]
            own, side, firsts = from_far[at], FAR, far_packs[v]
        else:
            at, v, s = PLANE_AT[c, r - 8], *SLOT_OF[c, r - 8]
            own = from_high[at] if at < len(DOWN) else from_more[at - len(DOWN)]
            side, firsts = HIGH, high_packs[v]
        before = pltpu.roll(near_lasts[side], LANES - LAST - LAST * at, axis=1)
        after = pltpu.roll(firsts, LANES - s, axis=1) if s else firsts
        margin = jnp.where(lane < FIRST, after, before)
        left = pltpu.roll(jnp.where(lane >= LANES - LAST, margin, own), LEFT_AT + 4, axis=1)
        right = pltpu.roll(jnp.where(lane < BXY, margin, own), RIGHT_AT + 8, axis=1)
        other = jnp.where(between(lane, LEFT_AT, LEFT_AT + 12), left, 1.0)
        other = jnp.where(between(lane, RIGHT_AT, RIGHT_AT + 16), right, other)
        other = jnp.where(edge, margin, other)
        kp[c, r + 4, :, 0:LANES] = own + KMIN
        kp[c, r + 4, :, LANES : 2 * LANES] = other + KMIN

    lane2 = lane_of((1, NZ, 2 * LANES))
    layer2 = lax.broadcasted_iota(jnp.int32, (1, NZ, 2 * LANES), 1)
    left_end = (lane2 == LANES + LEFT_AT + 11) | (lane2 == LANES + RIGHT_AT + 15)
    right_start = lane2 == LANES + RIGHT_AT
    top, bottom = layer2 == NZ - 1, layer2 == 0
    zero = jnp.zeros((1, NZ, 2 * LANES), F32)

    def y_next(v):
        return pltpu.roll(v, 2 * LANES - 1, axis=2)

    def y_last(v):
        return pltpu.roll(v, 1, axis=2)

    def z_next(v):
        return pltpu.roll(v, NZ - 1, axis=1)

    def z_last(v):
        return pltpu.roll(v, 1, axis=1)

    def finish(tx_low, tx_high, ty_low, ty_high, tz_low, tz_high, low_end, high_end):
        inverse = 1.0 / (tx_low + tx_high + ty_low + ty_high + tz_low + tz_high)
        return [
            zero if low_end else tx_low * inverse,
            zero if high_end else tx_high * inverse,
            jnp.where(right_start, 0.0, ty_low * inverse),
            jnp.where(left_end, 0.0, ty_high * inverse),
            jnp.where(bottom, 0.0, tz_low * inverse),
            jnp.where(top, 0.0, tz_high * inverse),
            (tx_high - tx_low) * inverse,
            (ty_high - ty_low) * inverse,
            (tz_high - tz_low) * inverse,
        ]

    def coefficients(r):
        kx_low, kx, kx_high = (kp[0, pl.ds(r + 4 + d, 1)] for d in (-1, 0, 1))
        ky, kz = kp[1, pl.ds(r + 4, 1)], kp[2, pl.ds(r + 4, 1)]
        tx_low, tx_high = harmonic(kx_low, kx), harmonic(kx, kx_high)
        ty = harmonic(ky, y_next(ky))
        ty_low = jnp.where(right_start, ky, y_last(ty))
        ty_high = jnp.where(left_end, ky, ty)
        tz = harmonic(kz, z_next(kz))
        tz_low = jnp.where(bottom, kz, z_last(tz))
        tz_high = jnp.where(top, kz, tz)
        for n, value in enumerate(finish(tx_low, tx_high, ty_low, ty_high, tz_low, tz_high, False, False)):
            coef[n, pl.ds(r + 3, 1)] = value
            if n >= 6:
                q1[n - 6, pl.ds(r + 3, 1)] = W[0] * value
        if 0 <= r < 16:
            for d, value in enumerate((tx_high, ty_high, tz_high)):
                if r < 8 or d == 0:
                    face[d, pl.ds(r, 1)] = value
        if r in ENDS:
            e = ENDS.index(r)
            low, high = (tx_low, kx) if e % 2 else (kx, tx_high)
            for n, value in enumerate(finish(low, high, ty_low, ty_high, tz_low, tz_high, not e % 2, e % 2)):
                u_coef[e, pl.ds(n, 1)] = value
                if n >= 6:
                    uq[e, 0, n - 6, pl.ds(0, 1)] = W[0] * value

    def sweep(w, cs, low, mid, high):
        around = cs[2] * y_last(mid) + cs[3] * y_next(mid) + cs[4] * z_last(mid) + cs[5] * z_next(mid)
        if low is not None:
            around = around + cs[0] * low
        if high is not None:
            around = around + cs[1] * high
        return mid + w * (around + cs[6] - mid)

    def coefs_at(r, d):
        return [coef[n, pl.ds(r + 3, 1)] for n in (0, 1, 2, 3, 4, 5, 6 + d)]

    qs = [(q1, 3), (q2, 2), (q3, 1), (q4, 0)]

    def q_at(s, d, r):
        ref, offset = qs[s]
        return ref[d, pl.ds(r + offset, 1)]

    def e_at(e, s, d, n):
        r = ENDS[e] - n if e % 2 else ENDS[e] + n
        return uq[e, s, d, pl.ds(n, 1)] if n <= s else q_at(s, d, r)

    def main_row(s, r, along=range(3)):
        for d in along:
            low, mid, high = (q_at(s - 1, d, r + n) for n in (-1, 0, 1))
            ref, offset = qs[s]
            ref[d, pl.ds(r + offset, 1)] = sweep(W[s], coefs_at(r, d), low, mid, high)

    def edge_row(e, s, n, along=range(3)):
        r = ENDS[e] - n if e % 2 else ENDS[e] + n
        for d in along:
            inner, mid = e_at(e, s - 1, d, n + 1), e_at(e, s - 1, d, n)
            outer = e_at(e, s - 1, d, n - 1) if n else None
            cs = coefs_at(r, d) if n else [u_coef[e, pl.ds(m, 1)] for m in (0, 1, 2, 3, 4, 5, 6 + d)]
            low, high = (inner, outer) if e % 2 else (outer, inner)
            uq[e, s, d, pl.ds(n, 1)] = sweep(W[s], cs, low, mid, high)

    for k in (6, 7):
        arrive(k)
    for r in range(8):
        for c in range(3):
            assemble(c, r)
    for r in range(1, 7):
        coefficients(r)

    for k in (2, 3, 0):
        arrive(k)
    for c, r in UP:
        assemble(c, r - 8)
    for r in range(-3, 1):
        coefficients(r)
    for k in (4, 5, 1):
        arrive(k)
    for c, r in DOWN:
        assemble(c, r + 8)
    for r in range(7, 12):
        coefficients(r)

    for s in range(1, SWEEPS):
        for r in range(s - 4 + 1, 12 - s):
            main_row(s, r)
        for e in range(2):
            for n in range(s + 1):
                edge_row(e, s, n)

    load_map.wait()
    layer = lax.broadcasted_iota(jnp.int32, (NZ, LANES), 0)
    layer_map = jnp.zeros((NZ, LANES), jnp.int32)
    for z in range(NZ):
        layer_map = jnp.where(layer == z, map_own[z], layer_map)
    last = SWEEPS - 1
    flag_left = (j > 0).astype(F32)
    flag_right = (j < n_gy - 1).astype(F32)
    pick = (lax.broadcasted_iota(jnp.int32, (LANES, LANES), 0) // BXY == lane_of((LANES, LANES))).astype(F32)
    extents = (24, 144, 8)

    def drop(d, here, above):
        if d == 0:
            return here - above - 1.0
        if d == 1:
            return here - jnp.where(left_end, 0.0, y_next(here)) - 1.0
        return here - jnp.where(top, 0.0, z_next(here)) - 1.0

    def coarse(first, along, flag_up, flag_low):
        e_low, e_high = ENDS.index(first), ENDS.index(first + 7)
        sums = []
        for d in along:
            def terms(n, here, above, at_end=False):
                fall = drop(d, here, above)
                square = fall * fall
                t = kp[0, pl.ds(first + n + 4, 1)] if at_end else face[d, pl.ds(first + n, 1)]
                return jnp.concatenate([t * square, square], axis=0)

            def main_at(n):
                return q_at(last, d, first + n)

            main = [terms(n, main_at(n), main_at(n + 1) if d == 0 else None) for n in range(8)]
            up = [terms(n, e_at(e_low, last, d, n), e_at(e_low, last, d, n + 1)) for n in range(4)]
            low = [
                terms(
                    n, e_at(e_high, last, d, 7 - n), zero if n == 7 else e_at(e_high, last, d, 6 - n), d == 0 and n == 7
                )
                for n in range(4, 8)
            ]
            third = terms(3, main_at(3), e_at(e_high, last, d, 3)) if d == 0 else main[3]
            main_low = main[0] + main[1] + main[2]
            main_high = main[4] + main[5] + main[6] + main[7]
            total = main_low + main[3] + main_high
            total = total + flag_up * (up[0] + up[1] + up[2] + up[3] + main_high)
            total = total + flag_low * (main_low + third + low[0] + low[1] + low[2] + low[3])
            own, other = total[:, :, 0:LANES], total[:, :, LANES : 2 * LANES]
            lane3 = lane_of(own.shape)
            left = pltpu.roll(other, LANES - LEFT_AT - 4, axis=2) * flag_left
            right = pltpu.roll(other, LANES - RIGHT_AT - 8, axis=2) * flag_right
            own = own + jnp.where(lane3 < 8, left, 0.0) + jnp.where(lane3 >= LANES - 8, right, 0.0)
            sums.append(own)
            if d == 1:
                after = other + pltpu.roll(other, LANES - RIGHT_AT - 8, axis=2)
        if len(along) == 3:
            sums.append(after)
            along = [*along, 1]
        count = len(along)
        stack = jnp.concatenate(sums, axis=0).reshape(2 * count * NZ, LANES)
        blocks = jnp.dot(stack, pick, precision=lax.Precision.HIGHEST, preferred_element_type=F32)
        blocks = blocks.reshape(count, 2, NZ, LANES)
        perm = [[None] * NCL for _ in along]
        for n in range(NCL):
            for at, d in enumerate(along):
                held = jnp.where(layer_map == n, blocks[at], 0.0)
                both = jnp.sum(held, axis=1, keepdims=True)
                perm[at][n] = both[0] / (both[1] + EPS * extents[d] * extents[d])
        return perm

    perm = coarse(0, range(3), (i < n_gx - 1).astype(F32), (i > 0).astype(F32))
    mess[pl.ds(0, NCL)] = jnp.concatenate(perm[0], axis=0)

    tell_k = len(copies)
    tell = remote(tell_k, mess, mess_x, -1, 0)
    sends = inside(-1, 0) & jnp.logical_not(reaches(-1))
    pl.when(sends)(tell.start)
    copies.append((tell, sends, inside(1, 0)))
    for d in range(3):
        for n in range(NCL):
            perm_ref[d, n] = perm[d][n][:, 0 : LANES // BXY]
    for n in range(NCL):
        value = harmonic(perm[2][n], perm[2][n + 1]) if n < NCL - 1 else jnp.zeros((1, LANES), F32)
        trans_ref[2, n] = value[:, 0 : LANES // BXY]

    exists = (j < n_gy - 1).astype(F32)
    lane1 = lane_of((1, LANES))
    for n in range(NCL):
        beyond = pltpu.roll(perm[3][n], LANES // BXY - 1, axis=1) * exists
        after = jnp.where(lane1 == LANES // BXY - 1, beyond, pltpu.roll(perm[1][n], LANES - 1, axis=1))
        trans_ref[1, n] = harmonic(perm[1][n], after)[:, 0 : LANES // BXY]

    @pl.when(reaches(0))
    def _():
        for k in range(8, 13):
            arrive(k)
        for c, r in PLANES[len(DOWN) :]:
            assemble(c, r + 8)
        for c, r in DOWN:
            assemble(c, r + 16)
        for r in [8] + list(range(12, 20)):
            coefficients(r)
        for s in range(1, SWEEPS):
            for r in range(12 - s, 20 - s):
                main_row(s, r, (0,))
            for e in (2, 3):
                for n in range(s + 1):
                    edge_row(e, s, n, (0,))
        (beyond,) = coarse(8, (0,), (i + 2 < n_gx).astype(F32), 1.0)
        mess_x[pl.ds(0, NCL)] = jnp.concatenate(beyond, axis=0)

    @pl.when(jnp.logical_not(reaches(0)))
    def _():
        arrive(tell_k)

    for n in range(NCL):
        trans_ref[0, n] = harmonic(perm[0][n], mess_x[pl.ds(n, 1)])[:, 0 : LANES // BXY]
    for copy, sends, _ in copies:
        pl.when(sends)(copy.wait_send)


def solution(mesh):
    n_gx, n_gy = mesh.shape["gx"], mesh.shape["gy"]

    def local(permeability, layer_map):
        k = permeability.reshape(3 * NZ * BXY, LANES)
        out = jax.ShapeDtypeStruct((3, NCL, 1, LANES // BXY), F32)
        vmem = lambda *shape: pltpu.VMEM(shape, F32)
        both = 2 * LANES
        return pl.pallas_call(
            lambda *refs: kernel(n_gx, n_gy, *refs),
            out_shape=(out, out),
            in_specs=[pl.BlockSpec(memory_space=pltpu.HBM)] * 2,
            out_specs=(pl.BlockSpec(memory_space=pltpu.VMEM),) * 2,
            scratch_shapes=[
                vmem(3 * NZ * BXY, LANES),
                pltpu.SMEM((NZ,), jnp.int32),
                vmem(len(PLANES), NZ, LANES),
                vmem(NZ, LANES),
                vmem(4, NZ, LANES),
                vmem(len(UP), NZ, LANES),
                vmem(len(DOWN), NZ, LANES),
                vmem(len(PLANES) - len(DOWN), NZ, LANES),
                vmem(len(DOWN), NZ, LANES),
                vmem(4, NZ, LANES),
                vmem(4, NZ, LANES),
                vmem(2, NZ, LANES),
                vmem(4, NZ, LANES),
                vmem(2, NZ, LANES),
                vmem(3, 25, NZ, both),
                vmem(9, 23, NZ, both),
                vmem(3, 16, NZ, both),
                vmem(3, 23, NZ, both),
                vmem(3, 21, NZ, both),
                vmem(3, 19, NZ, both),
                vmem(3, 17, NZ, both),
                vmem(4, 9, NZ, both),
                vmem(4, SWEEPS, 3, SWEEPS, NZ, both),
                vmem(NZ, LANES),
                vmem(NZ, LANES),
                pltpu.SemaphoreType.DMA((2,)),
                pltpu.SemaphoreType.DMA((14,)),
                pltpu.SemaphoreType.DMA((14,)),
            ],
            compiler_params=pltpu.CompilerParams(
                collective_id=0, has_side_effects=True, vmem_limit_bytes=32 * 1024 * 1024
            ),
            name="upscale",
        )(pltpu.with_memory_space_constraint(k, pltpu.HBM), pltpu.with_memory_space_constraint(layer_map, pltpu.HBM))

    spec = P(None, None, "gx", "gy")
    return jax.shard_map(local, mesh=mesh, in_specs=(spec, P()), out_specs=(spec, spec), check_vma=False)
```

```python
import math

import jax
import jax.numpy as jnp
from jax import lax
from jax.experimental import pallas as pl
from jax.experimental.pallas import tpu as pltpu
from jax.sharding import PartitionSpec as P

MESH = pl.DeviceIdType.MESH
NCL = 4
BXY = 8
SWEEPS = 4
KMIN = 0.01
EPS = 1e-06
NZ = 8
LANES = 128
F32 = jnp.float32

DOWN = [(1, r) for r in range(4)] + [(2, r) for r in range(4)] + [(0, r) for r in range(5)]
UP = [(0, r) for r in range(4, 8)] + [(1, r) for r in range(5, 8)] + [(2, r) for r in range(5, 8)]
PLANES = DOWN + UP[1:] + [(1, 4), (2, 4)]
PLANE_AT = {cr: at for at, cr in enumerate(PLANES)}
UP_FROM = PLANE_AT[UP[0]]
LAST, FIRST = 4, 13
PER_PACK = LANES // FIRST
LISTS = [DOWN, UP + [(1, 4), (2, 4)]]
PACKS = [part for planes in LISTS for part in (planes[:PER_PACK], planes[PER_PACK:])]
SLOT_OF = {cr: (v, FIRST * at) for v, pack in reversed(list(enumerate(PACKS))) for at, cr in enumerate(pack)}


def slots(widths):
    at, result = 0, {}
    for cr, width in widths.items():
        result[cr] = (at, width)
        at = at + width
    assert at <= LANES
    return result


UP_SLOTS = slots({cr: 12 for cr in UP})
DOWN_WIDTHS = {0: [11, 11, 10, 9, 3], 1: [12, 11, 10, 4], 2: [11, 10, 9, 3]}
DOWN_SLOTS = slots({(c, r): DOWN_WIDTHS[c][r] for c, r in DOWN})
DIRECTIONS = [(1, 0), (-1, 0), (1, 1), (1, -1), (-1, 1), (-1, -1), (0, 1), (0, -1)]
LOW, HIGH, OWN = range(3)
ENDS = [0, 7, 8]
LEFT_AT = 20
RIGHT_AT = 72
W = [1.0 / (1.05 + 0.95 * math.cos(math.pi * (2 * s + 1) / (2 * SWEEPS))) for s in range(SWEEPS)]


def harmonic(left, right):
    return 2.0 * left * right / (left + right)


def lane_of(shape):
    return lax.broadcasted_iota(jnp.int32, shape, len(shape) - 1)


def between(lane, low, high):
    return (lane >= low) & (lane < high)


def kernel(
    n_gx, n_gy, k_hbm, map_hbm, perm_ref, trans_ref,
    k_own, map_own, planes, lasts, packs, corners, from_low, from_high,
    near_lasts, own_packs, low_pack, high_pack, tale, heard,
    kp, coef, face, q1, q2, q3, q4, u_coef, uq, mess, mess_x,
    load_sem, send_sem, recv_sem,
):
    i, j = lax.axis_index("gx"), lax.axis_index("gy")
    load_k = pltpu.make_async_copy(k_hbm, k_own, load_sem.at[0])
    load_map = pltpu.make_async_copy(map_hbm, map_own, load_sem.at[1])
    load_k.start()
    load_map.start()

    def inside(di, dj):
        tests = []
        if di:
            tests.append(i + di < n_gx if di > 0 else i >= -di)
        if dj:
            tests.append(j + dj < n_gy if dj > 0 else j >= -dj)
        return tests[0] if len(tests) == 1 else tests[0] & tests[1]

    def device(di, dj):
        return {"gx": i + di, "gy": j + dj}

    odd = lax.rem(i, 2) == 1
    even = jnp.logical_not(odd)

    barrier = pltpu.get_barrier_semaphore()
    for di, dj in DIRECTIONS:
        @pl.when(inside(di, dj))
        def _():
            pl.semaphore_signal(barrier, inc=1, device_id=device(di, dj), device_id_type=MESH)

    lane = lane_of((NZ, LANES))
    load_k.wait()
    packed = [jnp.zeros((NZ, LANES), F32)] * len(PACKS)
    corner = [jnp.zeros((NZ, LANES), F32)] * 2
    last_of = jnp.zeros((NZ, LANES), F32)
    for at, (c, r) in enumerate(PLANES):
        plane = k_own[pl.ds(c * 64 + r, NZ, stride=8), :]
        planes[at] = plane
        last_of = jnp.where(between(lane, LAST * at, LAST * at + LAST), pltpu.roll(plane, LAST * at + LAST, axis=1), last_of)
        for v, pack in enumerate(PACKS):
            if (c, r) in pack:
                s = FIRST * pack.index((c, r))
                first_of = pltpu.roll(plane, s, axis=1) if s else plane
                packed[v] = jnp.where(between(lane, s, s + FIRST), first_of, packed[v])
        for v, places in enumerate((DOWN_SLOTS, UP_SLOTS)):
            if (c, r) in places:
                s, width = places[c, r]
                first_of = pltpu.roll(plane, s, axis=1) if s else plane
                corner[v] = jnp.where(between(lane, s, s + width), first_of, corner[v])
    lasts[...] = last_of
    corners[0] = corner[0]
    corners[1] = corner[1]
    for v, value in enumerate(packed):
        packs[v] = value

    rows_near = 1 + (i > 0).astype(jnp.int32) + (i < n_gx - 1).astype(jnp.int32)
    cols_near = 1 + (j > 0).astype(jnp.int32) + (j < n_gy - 1).astype(jnp.int32)
    pl.semaphore_wait(barrier, rows_near * cols_near - 1)

    def remote(k, source, target, di, dj):
        return pltpu.make_async_remote_copy(
            src_ref=source, dst_ref=target, send_sem=send_sem.at[k], recv_sem=recv_sem.at[k],
            device_id=device(di, dj), device_id_type=MESH,
        )

    def copy_of(k, di, dj):
        if dj == 0:
            if di > 0:
                return remote(k, planes.at[pl.ds(UP_FROM, len(UP))], from_low, di, dj)
            return remote(k, planes.at[pl.ds(0, len(DOWN))], from_high, di, dj)
        if dj > 0:
            return remote(k, lasts, near_lasts.at[LOW if di > 0 else HIGH if di < 0 else OWN], di, dj)
        if di == 0:
            return remote(k, packs, own_packs, di, dj)
        if di > 0:
            return remote(k, corners.at[1], low_pack, di, dj)
        return remote(k, corners.at[0], high_pack, di, dj)

    copies = [(copy_of(k, *to), inside(*to), inside(-to[0], -to[1])) for k, to in enumerate(DIRECTIONS)]
    for copy, sends, _ in copies:
        pl.when(sends)(copy.start)

    def arrive(k):
        copy, _, here = copies[k]
        target = copy.dst_ref
        pl.when(here)(copy.wait_recv)

        @pl.when(jnp.logical_not(here))
        def _():
            target[...] = jnp.zeros(target.shape, F32)

    edge = (lane >= LANES - LAST) | (lane < FIRST)

    def assemble(c, r):
        if 0 <= r < 8:
            at, (v, s) = PLANE_AT[c, r], SLOT_OF[c, r]
            own, side, firsts = planes[at], OWN, own_packs[v]
        elif r < 0:
            at, s = PLANE_AT[c, r + 8], UP_SLOTS[c, r + 8][0]
            own, side, firsts = from_low[at - UP_FROM], LOW, low_pack[...]
        else:
            at, s = PLANE_AT[c, r - 8], DOWN_SLOTS[c, r - 8][0]
            own, side, firsts = from_high[at], HIGH, high_pack[...]
        before = pltpu.roll(near_lasts[side], LANES - LAST - LAST * at, axis=1)
        after = pltpu.roll(firsts, LANES - s, axis=1) if s else firsts
        margin = jnp.where(lane < FIRST, after, before)
        left = pltpu.roll(jnp.where(lane >= LANES - LAST, margin, own), LEFT_AT + 4, axis=1)
        right = pltpu.roll(jnp.where(lane < BXY, margin, own), RIGHT_AT + 8, axis=1)
        other = jnp.where(between(lane, LEFT_AT, LEFT_AT + 12), left, 1.0)
        other = jnp.where(between(lane, RIGHT_AT, RIGHT_AT + 16), right, other)
        other = jnp.where(edge, margin, other)
        kp[c, r + 4, :, 0:LANES] = own + KMIN
        kp[c, r + 4, :, LANES : 2 * LANES] = other + KMIN

    lane2 = lane_of((1, NZ, 2 * LANES))
    layer2 = lax.broadcasted_iota(jnp.int32, (1, NZ, 2 * LANES), 1)
    left_end = (lane2 == LANES + LEFT_AT + 11) | (lane2 == LANES + RIGHT_AT + 15)
    right_start = lane2 == LANES + RIGHT_AT
    top, bottom = layer2 == NZ - 1, layer2 == 0
    zero = jnp.zeros((1, NZ, 2 * LANES), F32)

    def y_next(v):
        return pltpu.roll(v, 2 * LANES - 1, axis=2)

    def y_last(v):
        return pltpu.roll(v, 1, axis=2)

    def z_next(v):
        return pltpu.roll(v, NZ - 1, axis=1)

    def z_last(v):
        return pltpu.roll(v, 1, axis=1)

    def finish(tx_low, tx_high, ty_low, ty_high, tz_low, tz_high, low_end, high_end):
        inverse = 1.0 / (tx_low + tx_high + ty_low + ty_high + tz_low + tz_high)
        return [
            zero if low_end else tx_low * inverse,
            zero if high_end else tx_high * inverse,
            jnp.where(right_start, 0.0, ty_low * inverse),
            jnp.where(left_end, 0.0, ty_high * inverse),
            jnp.where(bottom, 0.0, tz_low * inverse),
            jnp.where(top, 0.0, tz_high * inverse),
            (tx_high - tx_low) * inverse,
            (ty_high - ty_low) * inverse,
            (tz_high - tz_low) * inverse,
        ]

    def coefficients(r):
        kx_low, kx, kx_high = (kp[0, pl.ds(r + 4 + d, 1)] for d in (-1, 0, 1))
        ky, kz = kp[1, pl.ds(r + 4, 1)], kp[2, pl.ds(r + 4, 1)]
        tx_low, tx_high = harmonic(kx_low, kx), harmonic(kx, kx_high)
        ty = harmonic(ky, y_next(ky))
        ty_low = jnp.where(right_start, ky, y_last(ty))
        ty_high = jnp.where(left_end, ky, ty)
        tz = harmonic(kz, z_next(kz))
        tz_low = jnp.where(bottom, kz, z_last(tz))
        tz_high = jnp.where(top, kz, tz)
        for n, value in enumerate(finish(tx_low, tx_high, ty_low, ty_high, tz_low, tz_high, False, False)):
            coef[n, pl.ds(r + 3, 1)] = value
            if n >= 6:
                q1[n - 6, pl.ds(r + 3, 1)] = W[0] * value
        if 0 <= r < 12:
            for d, value in enumerate((tx_high, ty_high, tz_high)):
                if r < 8 or d == 0:
                    face[d, pl.ds(r, 1)] = value
        if r in ENDS:
            e = ENDS.index(r)
            low, high = (tx_low, kx) if e % 2 else (kx, tx_high)
            for n, value in enumerate(finish(low, high, ty_low, ty_high, tz_low, tz_high, not e % 2, e % 2)):
                u_coef[e, pl.ds(n, 1)] = value
                if n >= 6:
                    uq[e, 0, n - 6, pl.ds(0, 1)] = W[0] * value

    def sweep(w, cs, low, mid, high):
        around = cs[2] * y_last(mid) + cs[3] * y_next(mid) + cs[4] * z_last(mid) + cs[5] * z_next(mid)
        if low is not None:
            around = around + cs[0] * low
        if high is not None:
            around = around + cs[1] * high
        return mid + w * (around + cs[6] - mid)

    def coefs_at(r, d):
        return [coef[n, pl.ds(r + 3, 1)] for n in (0, 1, 2, 3, 4, 5, 6 + d)]

    qs = [(q1, 3), (q2, 2), (q3, 1), (q4, 0)]

    def q_at(s, d, r):
        if r == 12:
            return jnp.concatenate([heard[pl.ds(s, 1)], heard[pl.ds(SWEEPS + 1 + s, 1)]], axis=2)
        ref, offset = qs[s]
        return ref[d, pl.ds(r + offset, 1)]

    def e_at(e, s, d, n):
        r = ENDS[e] - n if e % 2 else ENDS[e] + n
        return uq[e, s, d, pl.ds(n, 1)] if n <= s else q_at(s, d, r)

    def main_row(s, r, along=range(3)):
        for d in along:
            low, mid, high = (q_at(s - 1, d, r + n) for n in (-1, 0, 1))
            ref, offset = qs[s]
            ref[d, pl.ds(r + offset, 1)] = sweep(W[s], coefs_at(r, d), low, mid, high)

    def edge_row(e, s, n, along=range(3)):
        r = ENDS[e] - n if e % 2 else ENDS[e] + n
        for d in along:
            inner, mid = e_at(e, s - 1, d, n + 1), e_at(e, s - 1, d, n)
            outer = e_at(e, s - 1, d, n - 1) if n else None
            cs = coefs_at(r, d) if n else [u_coef[e, pl.ds(m, 1)] for m in (0, 1, 2, 3, 4, 5, 6 + d)]
            low, high = (inner, outer) if e % 2 else (outer, inner)
            uq[e, s, d, pl.ds(n, 1)] = sweep(W[s], cs, low, mid, high)

    last = SWEEPS - 1
    flag_left = (j > 0).astype(F32)
    flag_right = (j < n_gy - 1).astype(F32)
    flag_up = (i < n_gx - 1).astype(F32)
    flag_low = (i > 0).astype(F32)

    def terms(d, r, here, above, at_end=False):
        if d == 0:
            fall = here - above - 1.0
        elif d == 1:
            fall = here - jnp.where(left_end, 0.0, y_next(here)) - 1.0
        else:
            fall = here - jnp.where(top, 0.0, z_next(here)) - 1.0
        square = fall * fall
        t = kp[0, pl.ds(r + 4, 1)] if at_end else face[d, pl.ds(r, 1)]
        return jnp.concatenate([t * square, square], axis=0)

    def main_terms(d, r):
        return terms(d, r, q_at(last, d, r), q_at(last, d, r + 1) if d == 0 else None)

    def upper_sums(d):
        main = [main_terms(d, r) for r in range(4, 8)]
        main = main[0] + main[1] + main[2] + main[3]
        ends = [
            terms(d, r, e_at(1, last, d, 7 - r), zero if r == 7 else e_at(1, last, d, 6 - r), d == 0 and r == 7)
            for r in range(4, 8)
        ]
        return main + flag_up * main + flag_low * (ends[0] + ends[1] + ends[2] + ends[3])

    def lower_sums(d, first, ended, up, low):
        e = ENDS.index(first)
        main = [main_terms(d, first + n) for n in range(4)]
        ends = [terms(d, first + n, e_at(e, last, d, n), e_at(e, last, d, n + 1)) for n in range(4)]
        third = terms(d, first + 3, q_at(last, d, first + 3), ended) if d == 0 else main[3]
        three = main[0] + main[1] + main[2]
        return three + main[3] + up * (ends[0] + ends[1] + ends[2] + ends[3]) + low * (three + third)

    def columns(total):
        own, other = total[:, :, 0:LANES], total[:, :, LANES : 2 * LANES]
        lane3 = lane_of(own.shape)
        left = pltpu.roll(other, LANES - LEFT_AT - 4, axis=2) * flag_left
        right = pltpu.roll(other, LANES - RIGHT_AT - 8, axis=2)
        own = own + jnp.where(lane3 < 8, left, 0.0) + jnp.where(lane3 >= LANES - 8, right * flag_right, 0.0)
        return own, other + right

    for k in (6, 7):
        arrive(k)
    for r in range(8):
        for c in range(3):
            assemble(c, r)
    for r in range(1, 7):
        coefficients(r)

    def from_below():
        for k in (2, 3, 0):
            arrive(k)
        for c, r in UP:
            assemble(c, r - 8)
        for r in range(-3, 1):
            coefficients(r)

    def from_above():
        for k in (4, 5, 1):
            arrive(k)
        for c, r in DOWN:
            assemble(c, r + 8)
        for r in range(7, 12):
            coefficients(r)

    def sweeps(starts, stops, e):
        for s in range(1, SWEEPS):
            for r in range(starts[s - 1], stops[s - 1]):
                main_row(s, r, range(3) if r < 12 - s - 1 else (0,))
            for n in range(s + 1):
                edge_row(e, s, n)

    told = remote(len(copies), tale, heard, -1, 0)
    tells = even & (i > 0)
    copies.append((told, tells, odd & (i + 1 < n_gx)))

    @pl.when(even)
    def _():
        from_above()
        sweeps((2, 3, 4), (11, 10, 9), 1)
        for s in range(SWEEPS + 1):
            value = q_at(s, 0, 4) if s < SWEEPS else e_at(1, last, 0, 3)
            tale[pl.ds(s, 1)] = value[:, :, 0:LANES]
            tale[pl.ds(SWEEPS + 1 + s, 1)] = value[:, :, LANES : 2 * LANES]
        tale[pl.ds(2 * SWEEPS + 2, 2)] = columns(upper_sums(0))[0]
        pl.when(tells)(told.start)
        from_below()
        sweeps((-2, -1, 0), (2, 3, 4), 0)

    @pl.when(odd)
    def _():
        from_below()
        sweeps((-2, -1, 0), (6, 5, 4), 0)
        from_above()
        sweeps((6, 5, 4), (11, 10, 9), 1)

    load_map.wait()
    layer = lax.broadcasted_iota(jnp.int32, (NZ, LANES), 0)
    layer_map = jnp.zeros((NZ, LANES), jnp.int32)
    for z in range(NZ):
        layer_map = jnp.where(layer == z, map_own[z], layer_map)
    pick = (lax.broadcasted_iota(jnp.int32, (LANES, LANES), 0) // BXY == lane_of((LANES, LANES))).astype(F32)
    extents = (24, 144, 8)

    def coarse(sums, along):
        count = len(along)
        stack = jnp.concatenate(sums, axis=0).reshape(2 * count * NZ, LANES)
        blocks = jnp.dot(stack, pick, precision=lax.Precision.HIGHEST, preferred_element_type=F32)
        blocks = blocks.reshape(count, 2, NZ, LANES)
        perm = [[None] * NCL for _ in along]
        for n in range(NCL):
            for at, d in enumerate(along):
                held = jnp.where(layer_map == n, blocks[at], 0.0)
                both = jnp.sum(held, axis=1, keepdims=True)
                perm[at][n] = both[0] / (both[1] + EPS * extents[d] * extents[d])
        return perm

    sums = [columns(lower_sums(d, 0, e_at(1, last, d, 3), flag_up, flag_low) + upper_sums(d)) for d in range(3)]
    perm = coarse([own for own, _ in sums] + [sums[1][1]], (0, 1, 2, 1))
    mess[pl.ds(0, NCL)] = jnp.concatenate(perm[0], axis=0)

    tell_k = len(copies)
    tell = remote(tell_k, mess, mess_x, -1, 0)
    sends = odd
    pl.when(sends)(tell.start)
    copies.append((tell, sends, even & inside(1, 0)))
    for d in range(3):
        for n in range(NCL):
            perm_ref[d, n] = perm[d][n][:, 0 : LANES // BXY]
    for n in range(NCL):
        value = harmonic(perm[2][n], perm[2][n + 1]) if n < NCL - 1 else jnp.zeros((1, LANES), F32)
        trans_ref[2, n] = value[:, 0 : LANES // BXY]

    exists = (j < n_gy - 1).astype(F32)
    lane1 = lane_of((1, LANES))
    for n in range(NCL):
        beyond = pltpu.roll(perm[3][n], LANES // BXY - 1, axis=1) * exists
        after = jnp.where(lane1 == LANES // BXY - 1, beyond, pltpu.roll(perm[1][n], LANES - 1, axis=1))
        trans_ref[1, n] = harmonic(perm[1][n], after)[:, 0 : LANES // BXY]

    @pl.when(odd)
    def _():
        arrive(tell_k - 1)
        for s in range(1, SWEEPS):
            for r in range(12 - s, 12):
                main_row(s, r, (0,))
            for n in range(s + 1):
                edge_row(2, s, n, (0,))
        ended = jnp.concatenate([heard[pl.ds(SWEEPS, 1)], heard[pl.ds(2 * SWEEPS + 1, 1)]], axis=2)
        own, _ = columns(lower_sums(0, 8, ended, (i + 2 < n_gx).astype(F32), 1.0))
        (beyond,) = coarse([own + heard[pl.ds(2 * SWEEPS + 2, 2)]], (0,))
        here = (i + 1 < n_gx).astype(F32)
        mess_x[pl.ds(0, NCL)] = jnp.concatenate(beyond, axis=0) * here

    @pl.when(even)
    def _():
        arrive(tell_k)

    for n in range(NCL):
        trans_ref[0, n] = harmonic(perm[0][n], mess_x[pl.ds(n, 1)])[:, 0 : LANES // BXY]
    for copy, sends, _ in copies:
        pl.when(sends)(copy.wait_send)


def solution(mesh):
    n_gx, n_gy = mesh.shape["gx"], mesh.shape["gy"]

    def local(permeability, layer_map):
        k = permeability.reshape(3 * NZ * BXY, LANES)
        out = jax.ShapeDtypeStruct((3, NCL, 1, LANES // BXY), F32)
        vmem = lambda *shape: pltpu.VMEM(shape, F32)
        both = 2 * LANES
        return pl.pallas_call(
            lambda *refs: kernel(n_gx, n_gy, *refs),
            out_shape=(out, out),
            in_specs=[pl.BlockSpec(memory_space=pltpu.HBM)] * 2,
            out_specs=(pl.BlockSpec(memory_space=pltpu.VMEM),) * 2,
            scratch_shapes=[
                vmem(3 * NZ * BXY, LANES),
                pltpu.SMEM((NZ,), jnp.int32),
                vmem(len(PLANES), NZ, LANES),
                vmem(NZ, LANES),
                vmem(4, NZ, LANES),
                vmem(2, NZ, LANES),
                vmem(len(UP), NZ, LANES),
                vmem(len(DOWN), NZ, LANES),
                vmem(3, NZ, LANES),
                vmem(4, NZ, LANES),
                vmem(NZ, LANES),
                vmem(NZ, LANES),
                vmem(2 * SWEEPS + 4, NZ, LANES),
                vmem(2 * SWEEPS + 4, NZ, LANES),
                vmem(3, 17, NZ, both),
                vmem(9, 15, NZ, both),
                vmem(3, 12, NZ, both),
                vmem(3, 15, NZ, both),
                vmem(3, 14, NZ, both),
                vmem(3, 13, NZ, both),
                vmem(3, 12, NZ, both),
                vmem(3, 9, NZ, both),
                vmem(3, SWEEPS, 3, SWEEPS, NZ, both),
                vmem(NZ, LANES),
                vmem(NZ, LANES),
                pltpu.SemaphoreType.DMA((2,)),
                pltpu.SemaphoreType.DMA((10,)),
                pltpu.SemaphoreType.DMA((10,)),
            ],
            compiler_params=pltpu.CompilerParams(
                collective_id=0, has_side_effects=True, vmem_limit_bytes=32 * 1024 * 1024
            ),
            name="upscale",
        )(pltpu.with_memory_space_constraint(k, pltpu.HBM), pltpu.with_memory_space_constraint(layer_map, pltpu.HBM))

    spec = P(None, None, "gx", "gy")
    return jax.shard_map(local, mesh=mesh, in_specs=(spec, P()), out_specs=(spec, spec), check_vma=False)
```

```python
import math

import jax
import jax.numpy as jnp
from jax import lax
from jax.experimental import pallas as pl
from jax.experimental.pallas import tpu as pltpu
from jax.sharding import PartitionSpec as P

MESH = pl.DeviceIdType.MESH
NCL = 4
BXY = 8
SWEEPS = 4
KMIN = 0.01
EPS = 1e-06
NZ = 8
LANES = 128
F32 = jnp.float32

DOWN = [(1, r) for r in range(4)] + [(2, r) for r in range(4)] + [(0, r) for r in range(5)]
UP = [(0, r) for r in range(4, 8)] + [(1, r) for r in range(5, 8)] + [(2, r) for r in range(5, 8)]
PLANES = DOWN + UP[1:] + [(1, 4), (2, 4)]
PLANE_AT = {cr: at for at, cr in enumerate(PLANES)}
UP_FROM = PLANE_AT[UP[0]]
LAST, FIRST = 4, 13
PER_PACK = LANES // FIRST
LISTS = [DOWN, UP + [(1, 4), (2, 4)]]
PACKS = [part for planes in LISTS for part in (planes[:PER_PACK], planes[PER_PACK:])]
SLOT_OF = {cr: (v, FIRST * at) for v, pack in reversed(list(enumerate(PACKS))) for at, cr in enumerate(pack)}


def slots(widths):
    at, result = 0, {}
    for cr, width in widths.items():
        result[cr] = (at, width)
        at = at + width
    assert at <= LANES
    return result


UP_SLOTS = slots({cr: 12 for cr in UP})
DOWN_WIDTHS = {0: [11, 11, 10, 9, 3], 1: [12, 11, 10, 4], 2: [11, 10, 9, 3]}
DOWN_SLOTS = slots({(c, r): DOWN_WIDTHS[c][r] for c, r in DOWN})
DIRECTIONS = [(1, 0), (-1, 0), (1, 1), (1, -1), (-1, 1), (-1, -1), (0, 1), (0, -1)]
LOW, HIGH, OWN = range(3)
ENDS = [0, 7, 8]
LEFT_AT = 20
RIGHT_AT = 72
W = [1.0 / (1.05 + 0.95 * math.cos(math.pi * (2 * s + 1) / (2 * SWEEPS))) for s in range(SWEEPS)]


def harmonic(left, right):
    return 2.0 * left * right / (left + right)


def lane_of(shape):
    return lax.broadcasted_iota(jnp.int32, shape, len(shape) - 1)


def between(lane, low, high):
    return (lane >= low) & (lane < high)


def kernel(
    n_gx, n_gy, k_hbm, map_hbm, perm_ref, trans_ref,
    k_own, map_own, planes, lasts, packs, corners, from_low, from_high,
    near_lasts, own_packs, low_pack, high_pack, tale, heard,
    kp, coef, face, q1, q2, q3, q4, u_coef, uq, mess, mess_x,
    load_sem, send_sem, recv_sem,
):
    i, j = lax.axis_index("gx"), lax.axis_index("gy")
    load_k = pltpu.make_async_copy(k_hbm, k_own, load_sem.at[0])
    load_map = pltpu.make_async_copy(map_hbm, map_own, load_sem.at[1])
    load_k.start()
    load_map.start()

    def inside(di, dj):
        tests = []
        if di:
            tests.append(i + di < n_gx if di > 0 else i >= -di)
        if dj:
            tests.append(j + dj < n_gy if dj > 0 else j >= -dj)
        return tests[0] if len(tests) == 1 else tests[0] & tests[1]

    def device(di, dj):
        return {"gx": i + di, "gy": j + dj}

    odd = lax.rem(i, 2) == 1
    even = jnp.logical_not(odd)

    barrier = pltpu.get_barrier_semaphore()
    for di, dj in DIRECTIONS:
        @pl.when(inside(di, dj))
        def _():
            pl.semaphore_signal(barrier, inc=1, device_id=device(di, dj), device_id_type=MESH)

    lane = lane_of((NZ, LANES))
    load_k.wait()
    packed = [jnp.zeros((NZ, LANES), F32)] * len(PACKS)
    corner = [jnp.zeros((NZ, LANES), F32)] * 2
    last_of = jnp.zeros((NZ, LANES), F32)
    for at, (c, r) in enumerate(PLANES):
        plane = k_own[pl.ds(c * 64 + r, NZ, stride=8), :]
        planes[at] = plane
        last_of = jnp.where(between(lane, LAST * at, LAST * at + LAST), pltpu.roll(plane, LAST * at + LAST, axis=1), last_of)
        for v, pack in enumerate(PACKS):
            if (c, r) in pack:
                s = FIRST * pack.index((c, r))
                first_of = pltpu.roll(plane, s, axis=1) if s else plane
                packed[v] = jnp.where(between(lane, s, s + FIRST), first_of, packed[v])
        for v, places in enumerate((DOWN_SLOTS, UP_SLOTS)):
            if (c, r) in places:
                s, width = places[c, r]
                first_of = pltpu.roll(plane, s, axis=1) if s else plane
                corner[v] = jnp.where(between(lane, s, s + width), first_of, corner[v])
    lasts[...] = last_of
    corners[0] = corner[0]
    corners[1] = corner[1]
    for v, value in enumerate(packed):
        packs[v] = value

    rows_near = 1 + (i > 0).astype(jnp.int32) + (i < n_gx - 1).astype(jnp.int32)
    cols_near = 1 + (j > 0).astype(jnp.int32) + (j < n_gy - 1).astype(jnp.int32)
    pl.semaphore_wait(barrier, rows_near * cols_near - 1)

    def remote(k, source, target, di, dj):
        return pltpu.make_async_remote_copy(
            src_ref=source, dst_ref=target, send_sem=send_sem.at[k], recv_sem=recv_sem.at[k],
            device_id=device(di, dj), device_id_type=MESH,
        )

    def copy_of(k, di, dj):
        if dj == 0:
            if di > 0:
                return remote(k, planes.at[pl.ds(UP_FROM, len(UP))], from_low, di, dj)
            return remote(k, planes.at[pl.ds(0, len(DOWN))], from_high, di, dj)
        if dj > 0:
            return remote(k, lasts, near_lasts.at[LOW if di > 0 else HIGH if di < 0 else OWN], di, dj)
        if di == 0:
            return remote(k, packs, own_packs, di, dj)
        if di > 0:
            return remote(k, corners.at[1], low_pack, di, dj)
        return remote(k, corners.at[0], high_pack, di, dj)

    copies = [(copy_of(k, *to), inside(*to), inside(-to[0], -to[1])) for k, to in enumerate(DIRECTIONS)]
    for k in (7, 6, 5, 4, 3, 2, 1, 0):
        copy, sends, _ = copies[k]
        pl.when(sends)(copy.start)

    def arrive(k):
        copy, _, here = copies[k]
        target = copy.dst_ref
        pl.when(here)(copy.wait_recv)

        @pl.when(jnp.logical_not(here))
        def _():
            target[...] = jnp.zeros(target.shape, F32)

    edge = (lane >= LANES - LAST) | (lane < FIRST)

    def assemble(c, r):
        if 0 <= r < 8:
            at, (v, s) = PLANE_AT[c, r], SLOT_OF[c, r]
            own, side, firsts = planes[at], OWN, own_packs[v]
        elif r < 0:
            at, s = PLANE_AT[c, r + 8], UP_SLOTS[c, r + 8][0]
            own, side, firsts = from_low[at - UP_FROM], LOW, low_pack[...]
        else:
            at, s = PLANE_AT[c, r - 8], DOWN_SLOTS[c, r - 8][0]
            own, side, firsts = from_high[at], HIGH, high_pack[...]
        before = pltpu.roll(near_lasts[side], LANES - LAST - LAST * at, axis=1)
        after = pltpu.roll(firsts, LANES - s, axis=1) if s else firsts
        margin = jnp.where(lane < FIRST, after, before)
        left = pltpu.roll(jnp.where(lane >= LANES - LAST, margin, own), LEFT_AT + 4, axis=1)
        right = pltpu.roll(jnp.where(lane < BXY, margin, own), RIGHT_AT + 8, axis=1)
        other = jnp.where(between(lane, LEFT_AT, LEFT_AT + 12), left, 1.0)
        other = jnp.where(between(lane, RIGHT_AT, RIGHT_AT + 16), right, other)
        other = jnp.where(edge, margin, other)
        kp[c, r + 4, :, 0:LANES] = own + KMIN
        kp[c, r + 4, :, LANES : 2 * LANES] = other + KMIN

    lane2 = lane_of((1, NZ, 2 * LANES))
    layer2 = lax.broadcasted_iota(jnp.int32, (1, NZ, 2 * LANES), 1)
    left_end = (lane2 == LANES + LEFT_AT + 11) | (lane2 == LANES + RIGHT_AT + 15)
    right_start = lane2 == LANES + RIGHT_AT
    top, bottom = layer2 == NZ - 1, layer2 == 0
    zero = jnp.zeros((1, NZ, 2 * LANES), F32)

    def y_next(v):
        return pltpu.roll(v, 2 * LANES - 1, axis=2)

    def y_last(v):
        return pltpu.roll(v, 1, axis=2)

    def z_next(v):
        return pltpu.roll(v, NZ - 1, axis=1)

    def z_last(v):
        return pltpu.roll(v, 1, axis=1)

    def finish(tx_low, tx_high, ty_low, ty_high, tz_low, tz_high, low_end, high_end):
        inverse = 1.0 / (tx_low + tx_high + ty_low + ty_high + tz_low + tz_high)
        return [
            zero if low_end else tx_low * inverse,
            zero if high_end else tx_high * inverse,
            jnp.where(right_start, 0.0, ty_low * inverse),
            jnp.where(left_end, 0.0, ty_high * inverse),
            jnp.where(bottom, 0.0, tz_low * inverse),
            jnp.where(top, 0.0, tz_high * inverse),
            (tx_high - tx_low) * inverse,
            (ty_high - ty_low) * inverse,
            (tz_high - tz_low) * inverse,
        ]

    def coefficients(r):
        kx_low, kx, kx_high = (kp[0, pl.ds(r + 4 + d, 1)] for d in (-1, 0, 1))
        ky, kz = kp[1, pl.ds(r + 4, 1)], kp[2, pl.ds(r + 4, 1)]
        tx_low, tx_high = harmonic(kx_low, kx), harmonic(kx, kx_high)
        ty = harmonic(ky, y_next(ky))
        ty_low = jnp.where(right_start, ky, y_last(ty))
        ty_high = jnp.where(left_end, ky, ty)
        tz = harmonic(kz, z_next(kz))
        tz_low = jnp.where(bottom, kz, z_last(tz))
        tz_high = jnp.where(top, kz, tz)
        for n, value in enumerate(finish(tx_low, tx_high, ty_low, ty_high, tz_low, tz_high, False, False)):
            coef[n, pl.ds(r + 3, 1)] = value
            if n >= 6:
                q1[n - 6, pl.ds(r + 3, 1)] = W[0] * value
        if 0 <= r < 12:
            for d, value in enumerate((tx_high, ty_high, tz_high)):
                if r < 8 or d == 0:
                    face[d, pl.ds(r, 1)] = value
        if r in ENDS:
            e = ENDS.index(r)
            low, high = (tx_low, kx) if e % 2 else (kx, tx_high)
            for n, value in enumerate(finish(low, high, ty_low, ty_high, tz_low, tz_high, not e % 2, e % 2)):
                u_coef[e, pl.ds(n, 1)] = value
                if n >= 6:
                    uq[e, 0, n - 6, pl.ds(0, 1)] = W[0] * value

    def sweep(w, cs, low, mid, high):
        around = cs[2] * y_last(mid) + cs[3] * y_next(mid) + cs[4] * z_last(mid) + cs[5] * z_next(mid)
        if low is not None:
            around = around + cs[0] * low
        if high is not None:
            around = around + cs[1] * high
        return mid + w * (around + cs[6] - mid)

    def coefs_at(r, d):
        return [coef[n, pl.ds(r + 3, 1)] for n in (0, 1, 2, 3, 4, 5, 6 + d)]

    qs = [(q1, 3), (q2, 2), (q3, 1), (q4, 0)]

    def q_at(s, d, r):
        if r == 12:
            return jnp.concatenate([heard[pl.ds(s, 1)], heard[pl.ds(SWEEPS + 1 + s, 1)]], axis=2)
        ref, offset = qs[s]
        return ref[d, pl.ds(r + offset, 1)]

    def e_at(e, s, d, n):
        r = ENDS[e] - n if e % 2 else ENDS[e] + n
        return uq[e, s, d, pl.ds(n, 1)] if n <= s else q_at(s, d, r)

    def main_row(s, r, along=range(3)):
        for d in along:
            low, mid, high = (q_at(s - 1, d, r + n) for n in (-1, 0, 1))
            ref, offset = qs[s]
            ref[d, pl.ds(r + offset, 1)] = sweep(W[s], coefs_at(r, d), low, mid, high)

    def edge_row(e, s, n, along=range(3)):
        r = ENDS[e] - n if e % 2 else ENDS[e] + n
        for d in along:
            inner, mid = e_at(e, s - 1, d, n + 1), e_at(e, s - 1, d, n)
            outer = e_at(e, s - 1, d, n - 1) if n else None
            cs = coefs_at(r, d) if n else [u_coef[e, pl.ds(m, 1)] for m in (0, 1, 2, 3, 4, 5, 6 + d)]
            low, high = (inner, outer) if e % 2 else (outer, inner)
            uq[e, s, d, pl.ds(n, 1)] = sweep(W[s], cs, low, mid, high)

    last = SWEEPS - 1
    flag_left = (j > 0).astype(F32)
    flag_right = (j < n_gy - 1).astype(F32)
    flag_up = (i < n_gx - 1).astype(F32)
    flag_low = (i > 0).astype(F32)

    def terms(d, r, here, above, at_end=False):
        if d == 0:
            fall = here - above - 1.0
        elif d == 1:
            fall = here - jnp.where(left_end, 0.0, y_next(here)) - 1.0
        else:
            fall = here - jnp.where(top, 0.0, z_next(here)) - 1.0
        square = fall * fall
        t = kp[0, pl.ds(r + 4, 1)] if at_end else face[d, pl.ds(r, 1)]
        return jnp.concatenate([t * square, square], axis=0)

    def main_terms(d, r):
        return terms(d, r, q_at(last, d, r), q_at(last, d, r + 1) if d == 0 else None)

    def upper_sums(d):
        main = [main_terms(d, r) for r in range(4, 8)]
        main = main[0] + main[1] + main[2] + main[3]
        ends = [
            terms(d, r, e_at(1, last, d, 7 - r), zero if r == 7 else e_at(1, last, d, 6 - r), d == 0 and r == 7)
            for r in range(4, 8)
        ]
        return main + flag_up * main + flag_low * (ends[0] + ends[1] + ends[2] + ends[3])

    def lower_sums(d, first, ended, up, low):
        e = ENDS.index(first)
        main = [main_terms(d, first + n) for n in range(4)]
        ends = [terms(d, first + n, e_at(e, last, d, n), e_at(e, last, d, n + 1)) for n in range(4)]
        third = terms(d, first + 3, q_at(last, d, first + 3), ended) if d == 0 else main[3]
        three = main[0] + main[1] + main[2]
        return three + main[3] + up * (ends[0] + ends[1] + ends[2] + ends[3]) + low * (three + third)

    def columns(total):
        own, other = total[:, :, 0:LANES], total[:, :, LANES : 2 * LANES]
        lane3 = lane_of(own.shape)
        left = pltpu.roll(other, LANES - LEFT_AT - 4, axis=2) * flag_left
        right = pltpu.roll(other, LANES - RIGHT_AT - 8, axis=2)
        own = own + jnp.where(lane3 < 8, left, 0.0) + jnp.where(lane3 >= LANES - 8, right * flag_right, 0.0)
        return own, other + right

    for k in (6, 7):
        arrive(k)
    for r in range(8):
        for c in range(3):
            assemble(c, r)
    for r in range(1, 7):
        coefficients(r)

    def from_below():
        for k in (2, 3, 0):
            arrive(k)
        for c, r in UP:
            assemble(c, r - 8)
        for r in range(-3, 1):
            coefficients(r)

    def from_above():
        for k in (4, 5, 1):
            arrive(k)
        for c, r in DOWN:
            assemble(c, r + 8)
        for r in range(7, 12):
            coefficients(r)

    def sweeps(starts, stops, e, along=range(3)):
        for s in range(1, SWEEPS):
            for r in range(starts[s - 1], stops[s - 1]):
                main_row(s, r, [d for d in along if d == 0 or r < 12 - s - 1])
            for n in range(s + 1):
                edge_row(e, s, n, along)

    told = remote(len(copies), tale, heard, -1, 0)
    tells = even & (i > 0)
    copies.append((told, tells, odd & (i + 1 < n_gx)))

    @pl.when(even)
    def _():
        from_above()
        sweeps((2, 3, 4), (11, 10, 9), 1, (0,))
        for s in range(SWEEPS + 1):
            value = q_at(s, 0, 4) if s < SWEEPS else e_at(1, last, 0, 3)
            tale[pl.ds(s, 1)] = value[:, :, 0:LANES]
            tale[pl.ds(SWEEPS + 1 + s, 1)] = value[:, :, LANES : 2 * LANES]
        tale[pl.ds(2 * SWEEPS + 2, 2)] = columns(upper_sums(0))[0]
        pl.when(tells)(told.start)
        sweeps((2, 3, 4), (11, 10, 9), 1, (1, 2))
        from_below()
        sweeps((-2, -1, 0), (2, 3, 4), 0)

    @pl.when(odd)
    def _():
        from_below()
        sweeps((-2, -1, 0), (6, 5, 4), 0)
        from_above()
        sweeps((6, 5, 4), (11, 10, 9), 1)

    load_map.wait()
    layer = lax.broadcasted_iota(jnp.int32, (NZ, LANES), 0)
    layer_map = jnp.zeros((NZ, LANES), jnp.int32)
    for z in range(NZ):
        layer_map = jnp.where(layer == z, map_own[z], layer_map)
    pick = (lax.broadcasted_iota(jnp.int32, (LANES, LANES), 0) // BXY == lane_of((LANES, LANES))).astype(F32)
    extents = (24, 144, 8)

    def coarse(sums, along):
        count = len(along)
        stack = jnp.concatenate(sums, axis=0).reshape(2 * count * NZ, LANES)
        blocks = jnp.dot(stack, pick, precision=lax.Precision.HIGHEST, preferred_element_type=F32)
        blocks = blocks.reshape(count, 2, NZ, LANES)
        perm = [[None] * NCL for _ in along]
        for n in range(NCL):
            for at, d in enumerate(along):
                held = jnp.where(layer_map == n, blocks[at], 0.0)
                both = jnp.sum(held, axis=1, keepdims=True)
                perm[at][n] = both[0] / (both[1] + EPS * extents[d] * extents[d])
        return perm

    sums = [columns(lower_sums(d, 0, e_at(1, last, d, 3), flag_up, flag_low) + upper_sums(d)) for d in range(3)]
    perm = coarse([own for own, _ in sums] + [sums[1][1]], (0, 1, 2, 1))
    mess[pl.ds(0, NCL)] = jnp.concatenate(perm[0], axis=0)

    tell_k = len(copies)
    tell = remote(tell_k, mess, mess_x, -1, 0)
    sends = odd
    pl.when(sends)(tell.start)
    copies.append((tell, sends, even & inside(1, 0)))
    for d in range(3):
        for n in range(NCL):
            perm_ref[d, n] = perm[d][n][:, 0 : LANES // BXY]
    for n in range(NCL):
        value = harmonic(perm[2][n], perm[2][n + 1]) if n < NCL - 1 else jnp.zeros((1, LANES), F32)
        trans_ref[2, n] = value[:, 0 : LANES // BXY]

    exists = (j < n_gy - 1).astype(F32)
    lane1 = lane_of((1, LANES))
    for n in range(NCL):
        beyond = pltpu.roll(perm[3][n], LANES // BXY - 1, axis=1) * exists
        after = jnp.where(lane1 == LANES // BXY - 1, beyond, pltpu.roll(perm[1][n], LANES - 1, axis=1))
        trans_ref[1, n] = harmonic(perm[1][n], after)[:, 0 : LANES // BXY]

    @pl.when(odd)
    def _():
        arrive(tell_k - 1)
        for s in range(1, SWEEPS):
            for r in range(12 - s, 12):
                main_row(s, r, (0,))
            for n in range(s + 1):
                edge_row(2, s, n, (0,))
        ended = jnp.concatenate([heard[pl.ds(SWEEPS, 1)], heard[pl.ds(2 * SWEEPS + 1, 1)]], axis=2)
        own, _ = columns(lower_sums(0, 8, ended, (i + 2 < n_gx).astype(F32), 1.0))
        (beyond,) = coarse([own + heard[pl.ds(2 * SWEEPS + 2, 2)]], (0,))
        here = (i + 1 < n_gx).astype(F32)
        mess_x[pl.ds(0, NCL)] = jnp.concatenate(beyond, axis=0) * here

    @pl.when(even)
    def _():
        arrive(tell_k)

    for n in range(NCL):
        trans_ref[0, n] = harmonic(perm[0][n], mess_x[pl.ds(n, 1)])[:, 0 : LANES // BXY]
    for copy, sends, _ in copies:
        pl.when(sends)(copy.wait_send)


def solution(mesh):
    n_gx, n_gy = mesh.shape["gx"], mesh.shape["gy"]

    def local(permeability, layer_map):
        k = permeability.reshape(3 * NZ * BXY, LANES)
        out = jax.ShapeDtypeStruct((3, NCL, 1, LANES // BXY), F32)
        vmem = lambda *shape: pltpu.VMEM(shape, F32)
        both = 2 * LANES
        return pl.pallas_call(
            lambda *refs: kernel(n_gx, n_gy, *refs),
            out_shape=(out, out),
            in_specs=[pl.BlockSpec(memory_space=pltpu.HBM)] * 2,
            out_specs=(pl.BlockSpec(memory_space=pltpu.VMEM),) * 2,
            scratch_shapes=[
                vmem(3 * NZ * BXY, LANES),
                pltpu.SMEM((NZ,), jnp.int32),
                vmem(len(PLANES), NZ, LANES),
                vmem(NZ, LANES),
                vmem(4, NZ, LANES),
                vmem(2, NZ, LANES),
                vmem(len(UP), NZ, LANES),
                vmem(len(DOWN), NZ, LANES),
                vmem(3, NZ, LANES),
                vmem(4, NZ, LANES),
                vmem(NZ, LANES),
                vmem(NZ, LANES),
                vmem(2 * SWEEPS + 4, NZ, LANES),
                vmem(2 * SWEEPS + 4, NZ, LANES),
                vmem(3, 17, NZ, both),
                vmem(9, 15, NZ, both),
                vmem(3, 12, NZ, both),
                vmem(3, 15, NZ, both),
                vmem(3, 14, NZ, both),
                vmem(3, 13, NZ, both),
                vmem(3, 12, NZ, both),
                vmem(3, 9, NZ, both),
                vmem(3, SWEEPS, 3, SWEEPS, NZ, both),
                vmem(NZ, LANES),
                vmem(NZ, LANES),
                pltpu.SemaphoreType.DMA((2,)),
                pltpu.SemaphoreType.DMA((10,)),
                pltpu.SemaphoreType.DMA((10,)),
            ],
            compiler_params=pltpu.CompilerParams(
                collective_id=0, has_side_effects=True, vmem_limit_bytes=32 * 1024 * 1024
            ),
            name="upscale",
        )(pltpu.with_memory_space_constraint(k, pltpu.HBM), pltpu.with_memory_space_constraint(layer_map, pltpu.HBM))

    spec = P(None, None, "gx", "gy")
    return jax.shard_map(local, mesh=mesh, in_specs=(spec, P()), out_specs=(spec, spec), check_vma=False)
```

```python
import math

import jax
import jax.numpy as jnp
from jax import lax
from jax.experimental import pallas as pl
from jax.experimental.pallas import tpu as pltpu
from jax.sharding import PartitionSpec as P

MESH = pl.DeviceIdType.MESH
NCL = 4
BXY = 8
SWEEPS = 4
KMIN = 0.01
EPS = 1e-06
NZ = 8
LANES = 128
F32 = jnp.float32

DOWN = [(1, r) for r in range(4)] + [(2, r) for r in range(4)] + [(0, r) for r in range(5)]
UP = [(0, r) for r in range(4, 8)] + [(1, r) for r in range(5, 8)] + [(2, r) for r in range(5, 8)]
PLANES = DOWN + UP[1:] + [(1, 4), (2, 4)]
PLANE_AT = {cr: at for at, cr in enumerate(PLANES)}
UP_FROM = PLANE_AT[UP[0]]
LAST, FIRST = 4, 13
PER_PACK = LANES // FIRST
LISTS = [DOWN, UP + [(1, 4), (2, 4)]]
PACKS = [part for planes in LISTS for part in (planes[:PER_PACK], planes[PER_PACK:])]
SLOT_OF = {cr: (v, FIRST * at) for v, pack in reversed(list(enumerate(PACKS))) for at, cr in enumerate(pack)}


def slots(widths):
    at, result = 0, {}
    for cr, width in widths.items():
        result[cr] = (at, width)
        at = at + width
    assert at <= LANES
    return result


UP_SLOTS = slots({cr: 12 for cr in UP})
DOWN_WIDTHS = {0: [11, 11, 10, 9, 3], 1: [12, 11, 10, 4], 2: [11, 10, 9, 3]}
DOWN_SLOTS = slots({(c, r): DOWN_WIDTHS[c][r] for c, r in DOWN})
DIRECTIONS = [(1, 0), (-1, 0), (1, 1), (1, -1), (-1, 1), (-1, -1), (0, 1), (0, -1)]
LOW, HIGH, OWN = range(3)
ENDS = [0, 7, 8]
LEFT_AT = 20
RIGHT_AT = 72
W = [1.0 / (1.05 + 0.95 * math.cos(math.pi * (2 * s + 1) / (2 * SWEEPS))) for s in range(SWEEPS)]


def harmonic(left, right):
    return 2.0 * left * right / (left + right)


def lane_of(shape):
    return lax.broadcasted_iota(jnp.int32, shape, len(shape) - 1)


def between(lane, low, high):
    return (lane >= low) & (lane < high)


def kernel(
    n_gx, n_gy, k_hbm, map_hbm, out_ref,
    k_own, map_own, planes, lasts, packs, corners, from_low, from_high,
    near_lasts, own_packs, low_pack, high_pack, tale, heard,
    kp, coef, face, q1, q2, q3, q4, u_coef, uq, mess, mess_x,
    load_sem, send_sem, recv_sem,
):
    i, j = lax.axis_index("gx"), lax.axis_index("gy")
    perm_ref, trans_ref = out_ref.at[0], out_ref.at[1]
    load_k = pltpu.make_async_copy(k_hbm, k_own, load_sem.at[0])
    load_map = pltpu.make_async_copy(map_hbm, map_own, load_sem.at[1])
    load_k.start()
    load_map.start()

    def inside(di, dj):
        tests = []
        if di:
            tests.append(i + di < n_gx if di > 0 else i >= -di)
        if dj:
            tests.append(j + dj < n_gy if dj > 0 else j >= -dj)
        return tests[0] if len(tests) == 1 else tests[0] & tests[1]

    def device(di, dj):
        return {"gx": i + di, "gy": j + dj}

    odd = lax.rem(i, 2) == 1
    even = jnp.logical_not(odd)

    barrier = pltpu.get_barrier_semaphore()
    for di, dj in DIRECTIONS:
        @pl.when(inside(di, dj))
        def _():
            pl.semaphore_signal(barrier, inc=1, device_id=device(di, dj), device_id_type=MESH)

    lane = lane_of((NZ, LANES))
    load_k.wait()
    packed = [jnp.zeros((NZ, LANES), F32)] * len(PACKS)
    corner = [jnp.zeros((NZ, LANES), F32)] * 2
    last_of = jnp.zeros((NZ, LANES), F32)
    for at, (c, r) in enumerate(PLANES):
        plane = k_own[pl.ds(c * 64 + r, NZ, stride=8), :]
        planes[at] = plane
        last_of = jnp.where(between(lane, LAST * at, LAST * at + LAST), pltpu.roll(plane, LAST * at + LAST, axis=1), last_of)
        for v, pack in enumerate(PACKS):
            if (c, r) in pack:
                s = FIRST * pack.index((c, r))
                first_of = pltpu.roll(plane, s, axis=1) if s else plane
                packed[v] = jnp.where(between(lane, s, s + FIRST), first_of, packed[v])
        for v, places in enumerate((DOWN_SLOTS, UP_SLOTS)):
            if (c, r) in places:
                s, width = places[c, r]
                first_of = pltpu.roll(plane, s, axis=1) if s else plane
                corner[v] = jnp.where(between(lane, s, s + width), first_of, corner[v])
    lasts[...] = last_of
    corners[0] = corner[0]
    corners[1] = corner[1]
    for v, value in enumerate(packed):
        packs[v] = value

    rows_near = 1 + (i > 0).astype(jnp.int32) + (i < n_gx - 1).astype(jnp.int32)
    cols_near = 1 + (j > 0).astype(jnp.int32) + (j < n_gy - 1).astype(jnp.int32)
    pl.semaphore_wait(barrier, rows_near * cols_near - 1)

    def remote(k, source, target, di, dj):
        return pltpu.make_async_remote_copy(
            src_ref=source, dst_ref=target, send_sem=send_sem.at[k], recv_sem=recv_sem.at[k],
            device_id=device(di, dj), device_id_type=MESH,
        )

    def copy_of(k, di, dj):
        if dj == 0:
            if di > 0:
                return remote(k, planes.at[pl.ds(UP_FROM, len(UP))], from_low, di, dj)
            return remote(k, planes.at[pl.ds(0, len(DOWN))], from_high, di, dj)
        if dj > 0:
            return remote(k, lasts, near_lasts.at[LOW if di > 0 else HIGH if di < 0 else OWN], di, dj)
        if di == 0:
            return remote(k, packs, own_packs, di, dj)
        if di > 0:
            return remote(k, corners.at[1], low_pack, di, dj)
        return remote(k, corners.at[0], high_pack, di, dj)

    copies = [(copy_of(k, *to), inside(*to), inside(-to[0], -to[1])) for k, to in enumerate(DIRECTIONS)]
    for k in (7, 6, 5, 4, 3, 2, 1, 0):
        copy, sends, _ = copies[k]
        pl.when(sends)(copy.start)

    def arrive(k):
        copy, _, here = copies[k]
        target = copy.dst_ref
        pl.when(here)(copy.wait_recv)

        @pl.when(jnp.logical_not(here))
        def _():
            target[...] = jnp.zeros(target.shape, F32)

    edge = (lane >= LANES - LAST) | (lane < FIRST)

    def assemble(c, r):
        if 0 <= r < 8:
            at, (v, s) = PLANE_AT[c, r], SLOT_OF[c, r]
            own, side, firsts = planes[at], OWN, own_packs[v]
        elif r < 0:
            at, s = PLANE_AT[c, r + 8], UP_SLOTS[c, r + 8][0]
            own, side, firsts = from_low[at - UP_FROM], LOW, low_pack[...]
        else:
            at, s = PLANE_AT[c, r - 8], DOWN_SLOTS[c, r - 8][0]
            own, side, firsts = from_high[at], HIGH, high_pack[...]
        before = pltpu.roll(near_lasts[side], LANES - LAST - LAST * at, axis=1)
        after = pltpu.roll(firsts, LANES - s, axis=1) if s else firsts
        margin = jnp.where(lane < FIRST, after, before)
        left = pltpu.roll(jnp.where(lane >= LANES - LAST, margin, own), LEFT_AT + 4, axis=1)
        right = pltpu.roll(jnp.where(lane < BXY, margin, own), RIGHT_AT + 8, axis=1)
        other = jnp.where(between(lane, LEFT_AT, LEFT_AT + 12), left, 1.0)
        other = jnp.where(between(lane, RIGHT_AT, RIGHT_AT + 16), right, other)
        other = jnp.where(edge, margin, other)
        kp[c, r + 4, :, 0:LANES] = own + KMIN
        kp[c, r + 4, :, LANES : 2 * LANES] = other + KMIN

    lane2 = lane_of((1, NZ, 2 * LANES))
    layer2 = lax.broadcasted_iota(jnp.int32, (1, NZ, 2 * LANES), 1)
    left_end = (lane2 == LANES + LEFT_AT + 11) | (lane2 == LANES + RIGHT_AT + 15)
    right_start = lane2 == LANES + RIGHT_AT
    top, bottom = layer2 == NZ - 1, layer2 == 0
    zero = jnp.zeros((1, NZ, 2 * LANES), F32)

    def y_next(v):
        return pltpu.roll(v, 2 * LANES - 1, axis=2)

    def y_last(v):
        return pltpu.roll(v, 1, axis=2)

    def z_next(v):
        return pltpu.roll(v, NZ - 1, axis=1)

    def z_last(v):
        return pltpu.roll(v, 1, axis=1)

    def finish(tx_low, tx_high, ty_low, ty_high, tz_low, tz_high, low_end, high_end):
        inverse = 1.0 / (tx_low + tx_high + ty_low + ty_high + tz_low + tz_high)
        return [
            zero if low_end else tx_low * inverse,
            zero if high_end else tx_high * inverse,
            jnp.where(right_start, 0.0, ty_low * inverse),
            jnp.where(left_end, 0.0, ty_high * inverse),
            jnp.where(bottom, 0.0, tz_low * inverse),
            jnp.where(top, 0.0, tz_high * inverse),
            (tx_high - tx_low) * inverse,
            (ty_high - ty_low) * inverse,
            (tz_high - tz_low) * inverse,
        ]

    def coefficients(r):
        kx_low, kx, kx_high = (kp[0, pl.ds(r + 4 + d, 1)] for d in (-1, 0, 1))
        ky, kz = kp[1, pl.ds(r + 4, 1)], kp[2, pl.ds(r + 4, 1)]
        tx_low, tx_high = harmonic(kx_low, kx), harmonic(kx, kx_high)
        ty = harmonic(ky, y_next(ky))
        ty_low = jnp.where(right_start, ky, y_last(ty))
        ty_high = jnp.where(left_end, ky, ty)
        tz = harmonic(kz, z_next(kz))
        tz_low = jnp.where(bottom, kz, z_last(tz))
        tz_high = jnp.where(top, kz, tz)
        for n, value in enumerate(finish(tx_low, tx_high, ty_low, ty_high, tz_low, tz_high, False, False)):
            coef[n, pl.ds(r + 3, 1)] = value
            if n >= 6:
                q1[n - 6, pl.ds(r + 3, 1)] = W[0] * value
        if 0 <= r < 12:
            for d, value in enumerate((tx_high, ty_high, tz_high)):
                if r < 8 or d == 0:
                    face[d, pl.ds(r, 1)] = value
        if r in ENDS:
            e = ENDS.index(r)
            low, high = (tx_low, kx) if e % 2 else (kx, tx_high)
            for n, value in enumerate(finish(low, high, ty_low, ty_high, tz_low, tz_high, not e % 2, e % 2)):
                u_coef[e, pl.ds(n, 1)] = value
                if n >= 6:
                    uq[e, 0, n - 6, pl.ds(0, 1)] = W[0] * value

    def sweep(w, cs, low, mid, high):
        around = cs[2] * y_last(mid) + cs[3] * y_next(mid) + cs[4] * z_last(mid) + cs[5] * z_next(mid)
        if low is not None:
            around = around + cs[0] * low
        if high is not None:
            around = around + cs[1] * high
        return mid + w * (around + cs[6] - mid)

    def coefs_at(r, d):
        return [coef[n, pl.ds(r + 3, 1)] for n in (0, 1, 2, 3, 4, 5, 6 + d)]

    qs = [(q1, 3), (q2, 2), (q3, 1), (q4, 0)]

    def q_at(s, d, r):
        if r == 12:
            return jnp.concatenate([heard[pl.ds(s, 1)], heard[pl.ds(SWEEPS + 1 + s, 1)]], axis=2)
        ref, offset = qs[s]
        return ref[d, pl.ds(r + offset, 1)]

    def e_at(e, s, d, n):
        r = ENDS[e] - n if e % 2 else ENDS[e] + n
        return uq[e, s, d, pl.ds(n, 1)] if n <= s else q_at(s, d, r)

    def main_row(s, r, along=range(3)):
        for d in along:
            low, mid, high = (q_at(s - 1, d, r + n) for n in (-1, 0, 1))
            ref, offset = qs[s]
            ref[d, pl.ds(r + offset, 1)] = sweep(W[s], coefs_at(r, d), low, mid, high)

    def edge_row(e, s, n, along=range(3)):
        r = ENDS[e] - n if e % 2 else ENDS[e] + n
        for d in along:
            inner, mid = e_at(e, s - 1, d, n + 1), e_at(e, s - 1, d, n)
            outer = e_at(e, s - 1, d, n - 1) if n else None
            cs = coefs_at(r, d) if n else [u_coef[e, pl.ds(m, 1)] for m in (0, 1, 2, 3, 4, 5, 6 + d)]
            low, high = (inner, outer) if e % 2 else (outer, inner)
            uq[e, s, d, pl.ds(n, 1)] = sweep(W[s], cs, low, mid, high)

    last = SWEEPS - 1
    flag_left = (j > 0).astype(F32)
    flag_right = (j < n_gy - 1).astype(F32)
    flag_up = (i < n_gx - 1).astype(F32)
    flag_low = (i > 0).astype(F32)

    def terms(d, r, here, above, at_end=False):
        if d == 0:
            fall = here - above - 1.0
        elif d == 1:
            fall = here - jnp.where(left_end, 0.0, y_next(here)) - 1.0
        else:
            fall = here - jnp.where(top, 0.0, z_next(here)) - 1.0
        square = fall * fall
        t = kp[0, pl.ds(r + 4, 1)] if at_end else face[d, pl.ds(r, 1)]
        return jnp.concatenate([t * square, square], axis=0)

    def main_terms(d, r):
        return terms(d, r, q_at(last, d, r), q_at(last, d, r + 1) if d == 0 else None)

    def upper_sums(d):
        main = [main_terms(d, r) for r in range(4, 8)]
        main = main[0] + main[1] + main[2] + main[3]
        ends = [
            terms(d, r, e_at(1, last, d, 7 - r), zero if r == 7 else e_at(1, last, d, 6 - r), d == 0 and r == 7)
            for r in range(4, 8)
        ]
        return main + flag_up * main + flag_low * (ends[0] + ends[1] + ends[2] + ends[3])

    def lower_sums(d, first, ended, up, low):
        e = ENDS.index(first)
        main = [main_terms(d, first + n) for n in range(4)]
        ends = [terms(d, first + n, e_at(e, last, d, n), e_at(e, last, d, n + 1)) for n in range(4)]
        third = terms(d, first + 3, q_at(last, d, first + 3), ended) if d == 0 else main[3]
        three = main[0] + main[1] + main[2]
        return three + main[3] + up * (ends[0] + ends[1] + ends[2] + ends[3]) + low * (three + third)

    def columns(total):
        own, other = total[:, :, 0:LANES], total[:, :, LANES : 2 * LANES]
        lane3 = lane_of(own.shape)
        left = pltpu.roll(other, LANES - LEFT_AT - 4, axis=2) * flag_left
        right = pltpu.roll(other, LANES - RIGHT_AT - 8, axis=2)
        own = own + jnp.where(lane3 < 8, left, 0.0) + jnp.where(lane3 >= LANES - 8, right * flag_right, 0.0)
        return own, other + right

    for k in (6, 7):
        arrive(k)
    for r in range(8):
        for c in range(3):
            assemble(c, r)
    for r in range(1, 7):
        coefficients(r)

    def from_below():
        for k in (2, 3, 0):
            arrive(k)
        for c, r in UP:
            assemble(c, r - 8)
        for r in range(-3, 1):
            coefficients(r)

    def from_above():
        for k in (4, 5, 1):
            arrive(k)
        for c, r in DOWN:
            assemble(c, r + 8)
        for r in range(7, 12):
            coefficients(r)

    def sweeps(starts, stops, e, along=range(3)):
        for s in range(1, SWEEPS):
            for r in range(starts[s - 1], stops[s - 1]):
                main_row(s, r, [d for d in along if d == 0 or r < 12 - s - 1])
            for n in range(s + 1):
                edge_row(e, s, n, along)

    told = remote(len(copies), tale, heard, -1, 0)
    tells = even & (i > 0)
    copies.append((told, tells, odd & (i + 1 < n_gx)))

    @pl.when(even)
    def _():
        from_above()
        sweeps((2, 3, 4), (11, 10, 9), 1, (0,))
        for s in range(SWEEPS + 1):
            value = q_at(s, 0, 4) if s < SWEEPS else e_at(1, last, 0, 3)
            tale[pl.ds(s, 1)] = value[:, :, 0:LANES]
            tale[pl.ds(SWEEPS + 1 + s, 1)] = value[:, :, LANES : 2 * LANES]
        tale[pl.ds(2 * SWEEPS + 2, 2)] = columns(upper_sums(0))[0]
        pl.when(tells)(told.start)
        sweeps((2, 3, 4), (11, 10, 9), 1, (1, 2))
        from_below()
        sweeps((-2, -1, 0), (2, 3, 4), 0)

    @pl.when(odd)
    def _():
        from_below()
        sweeps((-2, -1, 0), (6, 5, 4), 0)
        from_above()
        sweeps((6, 5, 4), (11, 10, 9), 1)

    load_map.wait()
    layer = lax.broadcasted_iota(jnp.int32, (NZ, LANES), 0)
    layer_map = jnp.zeros((NZ, LANES), jnp.int32)
    for z in range(NZ):
        layer_map = jnp.where(layer == z, map_own[z], layer_map)
    pick = (lax.broadcasted_iota(jnp.int32, (LANES, LANES), 0) // BXY == lane_of((LANES, LANES))).astype(F32)
    extents = (24, 144, 8)

    def coarse(sums, along):
        count = len(along)
        stack = jnp.concatenate(sums, axis=0).reshape(2 * count * NZ, LANES)
        blocks = jnp.dot(stack, pick, precision=lax.Precision.HIGHEST, preferred_element_type=F32)
        blocks = blocks.reshape(count, 2, NZ, LANES)
        perm = [[None] * NCL for _ in along]
        for n in range(NCL):
            for at, d in enumerate(along):
                held = jnp.where(layer_map == n, blocks[at], 0.0)
                both = jnp.sum(held, axis=1, keepdims=True)
                perm[at][n] = both[0] / (both[1] + EPS * extents[d] * extents[d])
        return perm

    sums = [columns(lower_sums(d, 0, e_at(1, last, d, 3), flag_up, flag_low) + upper_sums(d)) for d in range(3)]
    perm = coarse([own for own, _ in sums] + [sums[1][1]], (0, 1, 2, 1))
    mess[pl.ds(0, NCL)] = jnp.concatenate(perm[0], axis=0)

    tell_k = len(copies)
    tell = remote(tell_k, mess, mess_x, -1, 0)
    sends = odd
    pl.when(sends)(tell.start)
    copies.append((tell, sends, even & inside(1, 0)))
    for d in range(3):
        for n in range(NCL):
            perm_ref[d, n] = perm[d][n][:, 0 : LANES // BXY]
    for n in range(NCL):
        value = harmonic(perm[2][n], perm[2][n + 1]) if n < NCL - 1 else jnp.zeros((1, LANES), F32)
        trans_ref[2, n] = value[:, 0 : LANES // BXY]

    exists = (j < n_gy - 1).astype(F32)
    lane1 = lane_of((1, LANES))
    for n in range(NCL):
        beyond = pltpu.roll(perm[3][n], LANES // BXY - 1, axis=1) * exists
        after = jnp.where(lane1 == LANES // BXY - 1, beyond, pltpu.roll(perm[1][n], LANES - 1, axis=1))
        trans_ref[1, n] = harmonic(perm[1][n], after)[:, 0 : LANES // BXY]

    @pl.when(odd)
    def _():
        arrive(tell_k - 1)
        for s in range(1, SWEEPS):
            for r in range(12 - s, 12):
                main_row(s, r, (0,))
            for n in range(s + 1):
                edge_row(2, s, n, (0,))
        ended = jnp.concatenate([heard[pl.ds(SWEEPS, 1)], heard[pl.ds(2 * SWEEPS + 1, 1)]], axis=2)
        own, _ = columns(lower_sums(0, 8, ended, (i + 2 < n_gx).astype(F32), 1.0))
        (beyond,) = coarse([own + heard[pl.ds(2 * SWEEPS + 2, 2)]], (0,))
        here = (i + 1 < n_gx).astype(F32)
        mess_x[pl.ds(0, NCL)] = jnp.concatenate(beyond, axis=0) * here

    @pl.when(even)
    def _():
        arrive(tell_k)

    for n in range(NCL):
        trans_ref[0, n] = harmonic(perm[0][n], mess_x[pl.ds(n, 1)])[:, 0 : LANES // BXY]
    for copy, sends, _ in copies:
        pl.when(sends)(copy.wait_send)


def solution(mesh):
    n_gx, n_gy = mesh.shape["gx"], mesh.shape["gy"]

    def local(permeability, layer_map):
        k = permeability.reshape(3 * NZ * BXY, LANES)
        out = jax.ShapeDtypeStruct((2, 3, NCL, 1, LANES // BXY), F32)
        vmem = lambda *shape: pltpu.VMEM(shape, F32)
        both = 2 * LANES
        both_out = pl.pallas_call(
            lambda *refs: kernel(n_gx, n_gy, *refs),
            out_shape=out,
            in_specs=[pl.BlockSpec(memory_space=pltpu.HBM)] * 2,
            out_specs=pl.BlockSpec(memory_space=pltpu.VMEM),
            scratch_shapes=[
                vmem(3 * NZ * BXY, LANES),
                pltpu.SMEM((NZ,), jnp.int32),
                vmem(len(PLANES), NZ, LANES),
                vmem(NZ, LANES),
                vmem(4, NZ, LANES),
                vmem(2, NZ, LANES),
                vmem(len(UP), NZ, LANES),
                vmem(len(DOWN), NZ, LANES),
                vmem(3, NZ, LANES),
                vmem(4, NZ, LANES),
                vmem(NZ, LANES),
                vmem(NZ, LANES),
                vmem(2 * SWEEPS + 4, NZ, LANES),
                vmem(2 * SWEEPS + 4, NZ, LANES),
                vmem(3, 17, NZ, both),
                vmem(9, 15, NZ, both),
                vmem(3, 12, NZ, both),
                vmem(3, 15, NZ, both),
                vmem(3, 14, NZ, both),
                vmem(3, 13, NZ, both),
                vmem(3, 12, NZ, both),
                vmem(3, 9, NZ, both),
                vmem(3, SWEEPS, 3, SWEEPS, NZ, both),
                vmem(NZ, LANES),
                vmem(NZ, LANES),
                pltpu.SemaphoreType.DMA((2,)),
                pltpu.SemaphoreType.DMA((10,)),
                pltpu.SemaphoreType.DMA((10,)),
            ],
            compiler_params=pltpu.CompilerParams(
                collective_id=0, has_side_effects=True, vmem_limit_bytes=32 * 1024 * 1024
            ),
            name="upscale",
        )(pltpu.with_memory_space_constraint(k, pltpu.HBM), pltpu.with_memory_space_constraint(layer_map, pltpu.HBM))
        return both_out[0], both_out[1]

    spec = P(None, None, "gx", "gy")
    return jax.shard_map(local, mesh=mesh, in_specs=(spec, P()), out_specs=(spec, spec), check_vma=False)
```

```python
import math

import jax
import jax.numpy as jnp
from jax import lax
from jax.experimental import pallas as pl
from jax.experimental.pallas import tpu as pltpu
from jax.sharding import PartitionSpec as P

MESH = pl.DeviceIdType.MESH
NCL = 4
BXY = 8
SWEEPS = 4
KMIN = 0.01
EPS = 1e-06
NZ = 8
LANES = 128
F32 = jnp.float32

DOWN = [(1, r) for r in range(4)] + [(2, r) for r in range(4)] + [(0, r) for r in range(5)]
UP = [(0, r) for r in range(4, 8)] + [(1, r) for r in range(5, 8)] + [(2, r) for r in range(5, 8)]
PLANES = DOWN + UP[1:] + [(1, 4), (2, 4)]
PLANE_AT = {cr: at for at, cr in enumerate(PLANES)}
UP_FROM = PLANE_AT[UP[0]]
LAST, FIRST = 4, 13
PER_PACK = LANES // FIRST
LISTS = [DOWN, UP + [(1, 4), (2, 4)]]
PACKS = [part for planes in LISTS for part in (planes[:PER_PACK], planes[PER_PACK:])]
SLOT_OF = {cr: (v, FIRST * at) for v, pack in reversed(list(enumerate(PACKS))) for at, cr in enumerate(pack)}


def slots(widths):
    at, result = 0, {}
    for cr, width in widths.items():
        result[cr] = (at, width)
        at = at + width
    assert at <= LANES
    return result


UP_SLOTS = slots({cr: 12 for cr in UP})
DOWN_WIDTHS = {0: [11, 11, 10, 9, 3], 1: [12, 11, 10, 4], 2: [11, 10, 9, 3]}
DOWN_SLOTS = slots({(c, r): DOWN_WIDTHS[c][r] for c, r in DOWN})
DIRECTIONS = [(1, 0), (-1, 0), (1, 1), (1, -1), (-1, 1), (-1, -1), (0, 1), (0, -1)]
LOW, HIGH, OWN = range(3)
ENDS = [0, 7, 8]
LEFT_AT = 13
RIGHT_AT = 25
TOLD = SWEEPS + 1
SPAN = 42
TALE = TOLD + -(-TOLD // 3) + 2
W = [1.0 / (1.05 + 0.95 * math.cos(math.pi * (2 * s + 1) / (2 * SWEEPS))) for s in range(SWEEPS)]


def harmonic(left, right):
    return 2.0 * left * right / (left + right)


def lane_of(shape):
    return lax.broadcasted_iota(jnp.int32, shape, len(shape) - 1)


def between(lane, low, high):
    return (lane >= low) & (lane < high)


def kernel(
    n_gx, n_gy, k_hbm, map_hbm, out_ref,
    k_own, map_own, planes, lasts, packs, corners, from_low, from_high,
    near_lasts, own_packs, low_pack, high_pack, tale, heard,
    kp, coef, face, q1, q2, q3, q4, u_coef, uq, mess, mess_x,
    load_sem, send_sem, recv_sem,
):
    i, j = lax.axis_index("gx"), lax.axis_index("gy")
    perm_ref, trans_ref = out_ref.at[0], out_ref.at[1]
    load_k = pltpu.make_async_copy(k_hbm, k_own, load_sem.at[0])
    load_map = pltpu.make_async_copy(map_hbm, map_own, load_sem.at[1])
    load_k.start()
    load_map.start()

    def inside(di, dj):
        tests = []
        if di:
            tests.append(i + di < n_gx if di > 0 else i >= -di)
        if dj:
            tests.append(j + dj < n_gy if dj > 0 else j >= -dj)
        return tests[0] if len(tests) == 1 else tests[0] & tests[1]

    def device(di, dj):
        return {"gx": i + di, "gy": j + dj}

    odd = lax.rem(i, 2) == 1
    even = jnp.logical_not(odd)

    barrier = pltpu.get_barrier_semaphore()
    for di, dj in DIRECTIONS:
        @pl.when(inside(di, dj))
        def _():
            pl.semaphore_signal(barrier, inc=1, device_id=device(di, dj), device_id_type=MESH)

    lane = lane_of((NZ, LANES))
    load_k.wait()
    packed = [jnp.zeros((NZ, LANES), F32)] * len(PACKS)
    corner = [jnp.zeros((NZ, LANES), F32)] * 2
    last_of = jnp.zeros((NZ, LANES), F32)
    for at, (c, r) in enumerate(PLANES):
        plane = k_own[pl.ds(c * 64 + r, NZ, stride=8), :]
        planes[at] = plane
        last_of = jnp.where(between(lane, LAST * at, LAST * at + LAST), pltpu.roll(plane, LAST * at + LAST, axis=1), last_of)
        for v, pack in enumerate(PACKS):
            if (c, r) in pack:
                s = FIRST * pack.index((c, r))
                first_of = pltpu.roll(plane, s, axis=1) if s else plane
                packed[v] = jnp.where(between(lane, s, s + FIRST), first_of, packed[v])
        for v, places in enumerate((DOWN_SLOTS, UP_SLOTS)):
            if (c, r) in places:
                s, width = places[c, r]
                first_of = pltpu.roll(plane, s, axis=1) if s else plane
                corner[v] = jnp.where(between(lane, s, s + width), first_of, corner[v])
    lasts[...] = last_of
    corners[0] = corner[0]
    corners[1] = corner[1]
    for v, value in enumerate(packed):
        packs[v] = value

    rows_near = 1 + (i > 0).astype(jnp.int32) + (i < n_gx - 1).astype(jnp.int32)
    cols_near = 1 + (j > 0).astype(jnp.int32) + (j < n_gy - 1).astype(jnp.int32)
    pl.semaphore_wait(barrier, rows_near * cols_near - 1)

    def remote(k, source, target, di, dj):
        return pltpu.make_async_remote_copy(
            src_ref=source, dst_ref=target, send_sem=send_sem.at[k], recv_sem=recv_sem.at[k],
            device_id=device(di, dj), device_id_type=MESH,
        )

    def copy_of(k, di, dj):
        if dj == 0:
            if di > 0:
                return remote(k, planes.at[pl.ds(UP_FROM, len(UP))], from_low, di, dj)
            return remote(k, planes.at[pl.ds(0, len(DOWN))], from_high, di, dj)
        if dj > 0:
            return remote(k, lasts, near_lasts.at[LOW if di > 0 else HIGH if di < 0 else OWN], di, dj)
        if di == 0:
            return remote(k, packs, own_packs, di, dj)
        if di > 0:
            return remote(k, corners.at[1], low_pack, di, dj)
        return remote(k, corners.at[0], high_pack, di, dj)

    copies = [(copy_of(k, *to), inside(*to), inside(-to[0], -to[1])) for k, to in enumerate(DIRECTIONS)]
    for k in (7, 6, 5, 4, 3, 2, 1, 0):
        copy, sends, _ = copies[k]
        pl.when(sends)(copy.start)

    def arrive(k):
        copy, _, here = copies[k]
        target = copy.dst_ref
        pl.when(here)(copy.wait_recv)

        @pl.when(jnp.logical_not(here))
        def _():
            target[...] = jnp.zeros(target.shape, F32)

    edge = (lane >= LANES - LAST) | (lane < FIRST)

    def assemble(c, r):
        if 0 <= r < 8:
            at, (v, s) = PLANE_AT[c, r], SLOT_OF[c, r]
            own, side, firsts = planes[at], OWN, own_packs[v]
        elif r < 0:
            at, s = PLANE_AT[c, r + 8], UP_SLOTS[c, r + 8][0]
            own, side, firsts = from_low[at - UP_FROM], LOW, low_pack[...]
        else:
            at, s = PLANE_AT[c, r - 8], DOWN_SLOTS[c, r - 8][0]
            own, side, firsts = from_high[at], HIGH, high_pack[...]
        before = pltpu.roll(near_lasts[side], LANES - LAST - LAST * at, axis=1)
        after = pltpu.roll(firsts, LANES - s, axis=1) if s else firsts
        margin = jnp.where(lane < FIRST, after, before)
        left = pltpu.roll(jnp.where(lane >= LANES - LAST, margin, own), LEFT_AT + 4, axis=1)
        right = pltpu.roll(jnp.where(lane < BXY, margin, own), RIGHT_AT + 8, axis=1)
        other = jnp.where(between(lane, LEFT_AT, LEFT_AT + 12), left, 1.0)
        other = jnp.where(between(lane, RIGHT_AT, RIGHT_AT + 16), right, other)
        other = jnp.where(edge, margin, other)
        kp[c, r + 4, :, 0:LANES] = own + KMIN
        kp[c, r + 4, :, LANES : 2 * LANES] = other + KMIN

    lane2 = lane_of((1, NZ, 2 * LANES))
    layer2 = lax.broadcasted_iota(jnp.int32, (1, NZ, 2 * LANES), 1)
    left_end = (lane2 == LANES + LEFT_AT + 11) | (lane2 == LANES + RIGHT_AT + 15)
    right_start = lane2 == LANES + RIGHT_AT
    top, bottom = layer2 == NZ - 1, layer2 == 0
    zero = jnp.zeros((1, NZ, 2 * LANES), F32)

    def y_next(v):
        return pltpu.roll(v, 2 * LANES - 1, axis=2)

    def y_last(v):
        return pltpu.roll(v, 1, axis=2)

    def z_next(v):
        return pltpu.roll(v, NZ - 1, axis=1)

    def z_last(v):
        return pltpu.roll(v, 1, axis=1)

    def finish(tx_low, tx_high, ty_low, ty_high, tz_low, tz_high, low_end, high_end):
        inverse = 1.0 / (tx_low + tx_high + ty_low + ty_high + tz_low + tz_high)
        return [
            zero if low_end else tx_low * inverse,
            zero if high_end else tx_high * inverse,
            jnp.where(right_start, 0.0, ty_low * inverse),
            jnp.where(left_end, 0.0, ty_high * inverse),
            jnp.where(bottom, 0.0, tz_low * inverse),
            jnp.where(top, 0.0, tz_high * inverse),
            (tx_high - tx_low) * inverse,
            (ty_high - ty_low) * inverse,
            (tz_high - tz_low) * inverse,
        ]

    def coefficients(r):
        kx_low, kx, kx_high = (kp[0, pl.ds(r + 4 + d, 1)] for d in (-1, 0, 1))
        ky, kz = kp[1, pl.ds(r + 4, 1)], kp[2, pl.ds(r + 4, 1)]
        tx_low, tx_high = harmonic(kx_low, kx), harmonic(kx, kx_high)
        ty = harmonic(ky, y_next(ky))
        ty_low = jnp.where(right_start, ky, y_last(ty))
        ty_high = jnp.where(left_end, ky, ty)
        tz = harmonic(kz, z_next(kz))
        tz_low = jnp.where(bottom, kz, z_last(tz))
        tz_high = jnp.where(top, kz, tz)
        for n, value in enumerate(finish(tx_low, tx_high, ty_low, ty_high, tz_low, tz_high, False, False)):
            coef[n, pl.ds(r + 3, 1)] = value
            if n >= 6:
                q1[n - 6, pl.ds(r + 3, 1)] = W[0] * value
        if 0 <= r < 12:
            for d, value in enumerate((tx_high, ty_high, tz_high)):
                if r < 8 or d == 0:
                    face[d, pl.ds(r, 1)] = value
        if r in ENDS:
            e = ENDS.index(r)
            low, high = (tx_low, kx) if e % 2 else (kx, tx_high)
            for n, value in enumerate(finish(low, high, ty_low, ty_high, tz_low, tz_high, not e % 2, e % 2)):
                u_coef[e, pl.ds(n, 1)] = value
                if n >= 6:
                    uq[e, 0, n - 6, pl.ds(0, 1)] = W[0] * value

    def sweep(w, cs, low, mid, high):
        around = cs[2] * y_last(mid) + cs[3] * y_next(mid) + cs[4] * z_last(mid) + cs[5] * z_next(mid)
        if low is not None:
            around = around + cs[0] * low
        if high is not None:
            around = around + cs[1] * high
        return mid + w * (around + cs[6] - mid)

    def coefs_at(r, d):
        return [coef[n, pl.ds(r + 3, 1)] for n in (0, 1, 2, 3, 4, 5, 6 + d)]

    qs = [(q1, 3), (q2, 2), (q3, 1), (q4, 0)]

    def told_row(n):
        other = pltpu.roll(heard[pl.ds(TOLD + n // 3, 1)], LANES - 2 - SPAN * (n % 3), axis=2)
        return jnp.concatenate([heard[pl.ds(n, 1)], other], axis=2)

    def q_at(s, d, r):
        if r == 12:
            return told_row(s)
        ref, offset = qs[s]
        return ref[d, pl.ds(r + offset, 1)]

    def e_at(e, s, d, n):
        r = ENDS[e] - n if e % 2 else ENDS[e] + n
        return uq[e, s, d, pl.ds(n, 1)] if n <= s else q_at(s, d, r)

    def main_row(s, r, along=range(3)):
        for d in along:
            low, mid, high = (q_at(s - 1, d, r + n) for n in (-1, 0, 1))
            ref, offset = qs[s]
            ref[d, pl.ds(r + offset, 1)] = sweep(W[s], coefs_at(r, d), low, mid, high)

    def edge_row(e, s, n, along=range(3)):
        r = ENDS[e] - n if e % 2 else ENDS[e] + n
        for d in along:
            inner, mid = e_at(e, s - 1, d, n + 1), e_at(e, s - 1, d, n)
            outer = e_at(e, s - 1, d, n - 1) if n else None
            cs = coefs_at(r, d) if n else [u_coef[e, pl.ds(m, 1)] for m in (0, 1, 2, 3, 4, 5, 6 + d)]
            low, high = (inner, outer) if e % 2 else (outer, inner)
            uq[e, s, d, pl.ds(n, 1)] = sweep(W[s], cs, low, mid, high)

    last = SWEEPS - 1
    flag_left = (j > 0).astype(F32)
    flag_right = (j < n_gy - 1).astype(F32)
    flag_up = (i < n_gx - 1).astype(F32)
    flag_low = (i > 0).astype(F32)

    def terms(d, r, here, above, at_end=False):
        if d == 0:
            fall = here - above - 1.0
        elif d == 1:
            fall = here - jnp.where(left_end, 0.0, y_next(here)) - 1.0
        else:
            fall = here - jnp.where(top, 0.0, z_next(here)) - 1.0
        square = fall * fall
        t = kp[0, pl.ds(r + 4, 1)] if at_end else face[d, pl.ds(r, 1)]
        return jnp.concatenate([t * square, square], axis=0)

    def main_terms(d, r):
        return terms(d, r, q_at(last, d, r), q_at(last, d, r + 1) if d == 0 else None)

    def upper_sums(d):
        main = [main_terms(d, r) for r in range(4, 8)]
        main = main[0] + main[1] + main[2] + main[3]
        ends = [
            terms(d, r, e_at(1, last, d, 7 - r), zero if r == 7 else e_at(1, last, d, 6 - r), d == 0 and r == 7)
            for r in range(4, 8)
        ]
        return main + flag_up * main + flag_low * (ends[0] + ends[1] + ends[2] + ends[3])

    def lower_sums(d, first, ended, up, low):
        e = ENDS.index(first)
        main = [main_terms(d, first + n) for n in range(4)]
        ends = [terms(d, first + n, e_at(e, last, d, n), e_at(e, last, d, n + 1)) for n in range(4)]
        third = terms(d, first + 3, q_at(last, d, first + 3), ended) if d == 0 else main[3]
        three = main[0] + main[1] + main[2]
        return three + main[3] + up * (ends[0] + ends[1] + ends[2] + ends[3]) + low * (three + third)

    def columns(total):
        own, other = total[:, :, 0:LANES], total[:, :, LANES : 2 * LANES]
        lane3 = lane_of(own.shape)
        left = pltpu.roll(other, LANES - LEFT_AT - 4, axis=2) * flag_left
        right = pltpu.roll(other, LANES - RIGHT_AT - 8, axis=2)
        own = own + jnp.where(lane3 < 8, left, 0.0) + jnp.where(lane3 >= LANES - 8, right * flag_right, 0.0)
        return own, other + right

    for k in (6, 7):
        arrive(k)
    for r in range(8):
        for c in range(3):
            assemble(c, r)
    for r in range(1, 7):
        coefficients(r)

    def from_below():
        for k in (2, 3, 0):
            arrive(k)
        for c, r in UP:
            assemble(c, r - 8)
        for r in range(-3, 1):
            coefficients(r)

    def from_above():
        for k in (4, 5, 1):
            arrive(k)
        for c, r in DOWN:
            assemble(c, r + 8)
        for r in range(7, 12):
            coefficients(r)

    def sweeps(starts, stops, e, along=range(3)):
        for s in range(1, SWEEPS):
            for r in range(starts[s - 1], stops[s - 1]):
                main_row(s, r, [d for d in along if d == 0 or r < 12 - s - 1])
            for n in range(s + 1):
                edge_row(e, s, n, along)

    told = remote(len(copies), tale, heard, -1, 0)
    tells = even & (i > 0)
    copies.append((told, tells, odd & (i + 1 < n_gx)))

    @pl.when(even)
    def _():
        from_above()
        sweeps((2, 3, 4), (11, 10, 9), 1, (0,))
        lane3 = lane_of((1, NZ, LANES))
        others = [None, None]
        for n in range(TOLD):
            value = q_at(n, 0, 4) if n < SWEEPS else e_at(1, last, 0, 3)
            tale[pl.ds(n, 1)] = value[:, :, 0:LANES]
            other = pltpu.roll(value[:, :, LANES : 2 * LANES], 2 + SPAN * (n % 3), axis=2)
            others[n // 3] = other if n % 3 == 0 else jnp.where(lane3 >= SPAN * (n % 3), other, others[n // 3])
        for n, other in enumerate(others):
            tale[pl.ds(TOLD + n, 1)] = other
        tale[pl.ds(TALE - 2, 2)] = columns(upper_sums(0))[0]
        pl.when(tells)(told.start)
        sweeps((2, 3, 4), (11, 10, 9), 1, (1, 2))
        from_below()
        sweeps((-2, -1, 0), (2, 3, 4), 0)

    @pl.when(odd)
    def _():
        from_below()
        sweeps((-2, -1, 0), (6, 5, 4), 0)
        from_above()
        sweeps((6, 5, 4), (11, 10, 9), 1)

    load_map.wait()
    layer = lax.broadcasted_iota(jnp.int32, (NZ, LANES), 0)
    layer_map = jnp.zeros((NZ, LANES), jnp.int32)
    for z in range(NZ):
        layer_map = jnp.where(layer == z, map_own[z], layer_map)
    pick = (lax.broadcasted_iota(jnp.int32, (LANES, LANES), 0) // BXY == lane_of((LANES, LANES))).astype(F32)
    extents = (24, 144, 8)

    def coarse(sums, along):
        count = len(along)
        stack = jnp.concatenate(sums, axis=0).reshape(2 * count * NZ, LANES)
        blocks = jnp.dot(stack, pick, precision=lax.Precision.HIGHEST, preferred_element_type=F32)
        blocks = blocks.reshape(count, 2, NZ, LANES)
        perm = [[None] * NCL for _ in along]
        for n in range(NCL):
            for at, d in enumerate(along):
                held = jnp.where(layer_map == n, blocks[at], 0.0)
                both = jnp.sum(held, axis=1, keepdims=True)
                perm[at][n] = both[0] / (both[1] + EPS * extents[d] * extents[d])
        return perm

    sums = [columns(lower_sums(d, 0, e_at(1, last, d, 3), flag_up, flag_low) + upper_sums(d)) for d in range(3)]
    perm = coarse([own for own, _ in sums] + [sums[1][1]], (0, 1, 2, 1))
    mess[pl.ds(0, NCL)] = jnp.concatenate(perm[0], axis=0)

    tell_k = len(copies)
    tell = remote(tell_k, mess, mess_x, -1, 0)
    sends = odd
    pl.when(sends)(tell.start)
    copies.append((tell, sends, even & inside(1, 0)))
    for d in range(3):
        for n in range(NCL):
            perm_ref[d, n] = perm[d][n][:, 0 : LANES // BXY]
    for n in range(NCL):
        value = harmonic(perm[2][n], perm[2][n + 1]) if n < NCL - 1 else jnp.zeros((1, LANES), F32)
        trans_ref[2, n] = value[:, 0 : LANES // BXY]

    exists = (j < n_gy - 1).astype(F32)
    lane1 = lane_of((1, LANES))
    for n in range(NCL):
        beyond = pltpu.roll(perm[3][n], LANES // BXY - 1, axis=1) * exists
        after = jnp.where(lane1 == LANES // BXY - 1, beyond, pltpu.roll(perm[1][n], LANES - 1, axis=1))
        trans_ref[1, n] = harmonic(perm[1][n], after)[:, 0 : LANES // BXY]

    @pl.when(odd)
    def _():
        arrive(tell_k - 1)
        for s in range(1, SWEEPS):
            for r in range(12 - s, 12):
                main_row(s, r, (0,))
            for n in range(s + 1):
                edge_row(2, s, n, (0,))
        ended = told_row(SWEEPS)
        own, _ = columns(lower_sums(0, 8, ended, (i + 2 < n_gx).astype(F32), 1.0))
        (beyond,) = coarse([own + heard[pl.ds(TALE - 2, 2)]], (0,))
        here = (i + 1 < n_gx).astype(F32)
        mess_x[pl.ds(0, NCL)] = jnp.concatenate(beyond, axis=0) * here

    @pl.when(even)
    def _():
        arrive(tell_k)

    for n in range(NCL):
        trans_ref[0, n] = harmonic(perm[0][n], mess_x[pl.ds(n, 1)])[:, 0 : LANES // BXY]
    for copy, sends, _ in copies:
        pl.when(sends)(copy.wait_send)


def solution(mesh):
    n_gx, n_gy = mesh.shape["gx"], mesh.shape["gy"]

    def local(permeability, layer_map):
        k = permeability.reshape(3 * NZ * BXY, LANES)
        out = jax.ShapeDtypeStruct((2, 3, NCL, 1, LANES // BXY), F32)
        vmem = lambda *shape: pltpu.VMEM(shape, F32)
        both = 2 * LANES
        both_out = pl.pallas_call(
            lambda *refs: kernel(n_gx, n_gy, *refs),
            out_shape=out,
            in_specs=[pl.BlockSpec(memory_space=pltpu.HBM)] * 2,
            out_specs=pl.BlockSpec(memory_space=pltpu.VMEM),
            scratch_shapes=[
                vmem(3 * NZ * BXY, LANES),
                pltpu.SMEM((NZ,), jnp.int32),
                vmem(len(PLANES), NZ, LANES),
                vmem(NZ, LANES),
                vmem(4, NZ, LANES),
                vmem(2, NZ, LANES),
                vmem(len(UP), NZ, LANES),
                vmem(len(DOWN), NZ, LANES),
                vmem(3, NZ, LANES),
                vmem(4, NZ, LANES),
                vmem(NZ, LANES),
                vmem(NZ, LANES),
                vmem(TALE, NZ, LANES),
                vmem(TALE, NZ, LANES),
                vmem(3, 17, NZ, both),
                vmem(9, 15, NZ, both),
                vmem(3, 12, NZ, both),
                vmem(3, 15, NZ, both),
                vmem(3, 14, NZ, both),
                vmem(3, 13, NZ, both),
                vmem(3, 12, NZ, both),
                vmem(3, 9, NZ, both),
                vmem(3, SWEEPS, 3, SWEEPS, NZ, both),
                vmem(NZ, LANES),
                vmem(NZ, LANES),
                pltpu.SemaphoreType.DMA((2,)),
                pltpu.SemaphoreType.DMA((10,)),
                pltpu.SemaphoreType.DMA((10,)),
            ],
            compiler_params=pltpu.CompilerParams(
                collective_id=0, has_side_effects=True, vmem_limit_bytes=32 * 1024 * 1024
            ),
            name="upscale",
        )(pltpu.with_memory_space_constraint(k, pltpu.HBM), pltpu.with_memory_space_constraint(layer_map, pltpu.HBM))
        return both_out[0], both_out[1]

    spec = P(None, None, "gx", "gy")
    return jax.shard_map(local, mesh=mesh, in_specs=(spec, P()), out_specs=(spec, spec), check_vma=False)
```

```python
import math

import jax
import jax.numpy as jnp
from jax import lax
from jax.experimental import pallas as pl
from jax.experimental.pallas import tpu as pltpu
from jax.sharding import PartitionSpec as P

MESH = pl.DeviceIdType.MESH
NCL = 4
BXY = 8
SWEEPS = 4
KMIN = 0.01
EPS = 1e-06
NZ = 8
LANES = 128
F32 = jnp.float32

DOWN = [(1, r) for r in range(4)] + [(2, r) for r in range(4)] + [(0, r) for r in range(5)]
UP = [(0, r) for r in range(4, 8)] + [(1, r) for r in range(5, 8)] + [(2, r) for r in range(5, 8)]
PLANES = DOWN + UP[1:] + [(1, 4), (2, 4)]
PLANE_AT = {cr: at for at, cr in enumerate(PLANES)}
UP_FROM = PLANE_AT[UP[0]]
LAST, FIRST = 4, 13
PER_PACK = LANES // FIRST
LISTS = [DOWN, UP + [(1, 4), (2, 4)]]
PACKS = [part for planes in LISTS for part in (planes[:PER_PACK], planes[PER_PACK:])]
SLOT_OF = {cr: (v, FIRST * at) for v, pack in reversed(list(enumerate(PACKS))) for at, cr in enumerate(pack)}


def slots(widths):
    at, result = 0, {}
    for cr, width in widths.items():
        result[cr] = (at, width)
        at = at + width
    assert at <= LANES
    return result


UP_SLOTS = slots({cr: 12 for cr in UP})
DOWN_WIDTHS = {0: [11, 11, 10, 9, 3], 1: [12, 11, 10, 4], 2: [11, 10, 9, 3]}
DOWN_SLOTS = slots({(c, r): DOWN_WIDTHS[c][r] for c, r in DOWN})
DIRECTIONS = [(1, 0), (-1, 0), (1, 1), (1, -1), (-1, 1), (-1, -1), (0, 1), (0, -1)]
LOW, HIGH, OWN = range(3)
ENDS = [0, 7, 8]
LEFT_AT = 13
RIGHT_AT = 25
TOLD = SWEEPS + 1
SPAN = 42
TALE = TOLD + -(-TOLD // 3) + 2
W = [1.0 / (1.05 + 0.95 * math.cos(math.pi * (2 * s + 1) / (2 * SWEEPS))) for s in range(SWEEPS)]


def harmonic(left, right):
    return 2.0 * left * right / (left + right)


def lane_of(shape):
    return lax.broadcasted_iota(jnp.int32, shape, len(shape) - 1)


def between(lane, low, high):
    return (lane >= low) & (lane < high)


def kernel(
    n_gx, n_gy, k_hbm, map_hbm, out_ref,
    k_own, map_own, planes, lasts, packs, corners, from_low, from_high,
    near_lasts, own_packs, low_pack, high_pack, tale, heard,
    kp, coef, face, q1, q2, q3, q4, u_coef, uq, mess, mess_x,
    load_sem, send_sem, recv_sem,
):
    i, j = lax.axis_index("gx"), lax.axis_index("gy")
    perm_ref, trans_ref = out_ref.at[0], out_ref.at[1]
    load_k = pltpu.make_async_copy(k_hbm, k_own, load_sem.at[0])
    load_map = pltpu.make_async_copy(map_hbm, map_own, load_sem.at[1])
    load_k.start()
    load_map.start()

    def inside(di, dj):
        tests = []
        if di:
            tests.append(i + di < n_gx if di > 0 else i >= -di)
        if dj:
            tests.append(j + dj < n_gy if dj > 0 else j >= -dj)
        return tests[0] if len(tests) == 1 else tests[0] & tests[1]

    def device(di, dj):
        return {"gx": i + di, "gy": j + dj}

    odd = lax.rem(i, 2) == 1
    even = jnp.logical_not(odd)

    barrier = pltpu.get_barrier_semaphore()
    for di, dj in DIRECTIONS:
        @pl.when(inside(di, dj))
        def _():
            pl.semaphore_signal(barrier, inc=1, device_id=device(di, dj), device_id_type=MESH)

    lane = lane_of((NZ, LANES))
    load_k.wait()
    packed = [jnp.zeros((NZ, LANES), F32)] * len(PACKS)
    corner = [jnp.zeros((NZ, LANES), F32)] * 2
    last_of = jnp.zeros((NZ, LANES), F32)
    for at, (c, r) in enumerate(PLANES):
        plane = k_own[pl.ds(c * 64 + r, NZ, stride=8), :]
        planes[at] = plane
        last_of = jnp.where(between(lane, LAST * at, LAST * at + LAST), pltpu.roll(plane, LAST * at + LAST, axis=1), last_of)
        for v, pack in enumerate(PACKS):
            if (c, r) in pack:
                s = FIRST * pack.index((c, r))
                first_of = pltpu.roll(plane, s, axis=1) if s else plane
                packed[v] = jnp.where(between(lane, s, s + FIRST), first_of, packed[v])
        for v, places in enumerate((DOWN_SLOTS, UP_SLOTS)):
            if (c, r) in places:
                s, width = places[c, r]
                first_of = pltpu.roll(plane, s, axis=1) if s else plane
                corner[v] = jnp.where(between(lane, s, s + width), first_of, corner[v])
    lasts[...] = last_of
    corners[0] = corner[0]
    corners[1] = corner[1]
    for v, value in enumerate(packed):
        packs[v] = value

    rows_near = 1 + (i > 0).astype(jnp.int32) + (i < n_gx - 1).astype(jnp.int32)
    cols_near = 1 + (j > 0).astype(jnp.int32) + (j < n_gy - 1).astype(jnp.int32)
    pl.semaphore_wait(barrier, rows_near * cols_near - 1)

    def remote(k, source, target, di, dj):
        return pltpu.make_async_remote_copy(
            src_ref=source, dst_ref=target, send_sem=send_sem.at[k], recv_sem=recv_sem.at[k],
            device_id=device(di, dj), device_id_type=MESH,
        )

    def copy_of(k, di, dj):
        if dj == 0:
            if di > 0:
                return remote(k, planes.at[pl.ds(UP_FROM, len(UP))], from_low, di, dj)
            return remote(k, planes.at[pl.ds(0, len(DOWN))], from_high, di, dj)
        if dj > 0:
            return remote(k, lasts, near_lasts.at[LOW if di > 0 else HIGH if di < 0 else OWN], di, dj)
        if di == 0:
            return remote(k, packs, own_packs, di, dj)
        if di > 0:
            return remote(k, corners.at[1], low_pack, di, dj)
        return remote(k, corners.at[0], high_pack, di, dj)

    copies = [(copy_of(k, *to), inside(*to), inside(-to[0], -to[1])) for k, to in enumerate(DIRECTIONS)]
    for k in (7, 6, 5, 4, 3, 2, 1, 0):
        copy, sends, _ = copies[k]
        pl.when(sends & even if k == 0 else sends)(copy.start)

    def arrive(k):
        copy, _, here = copies[k]
        target = copy.dst_ref
        pl.when(here)(copy.wait_recv)

        @pl.when(jnp.logical_not(here))
        def _():
            target[...] = jnp.zeros(target.shape, F32)

    edge = (lane >= LANES - LAST) | (lane < FIRST)

    def assemble(c, r):
        if 0 <= r < 8:
            at, (v, s) = PLANE_AT[c, r], SLOT_OF[c, r]
            own, side, firsts = planes[at], OWN, own_packs[v]
        elif r < 0:
            at, s = PLANE_AT[c, r + 8], UP_SLOTS[c, r + 8][0]
            own, side, firsts = from_low[at - UP_FROM], LOW, low_pack[...]
        else:
            at, s = PLANE_AT[c, r - 8], DOWN_SLOTS[c, r - 8][0]
            own, side, firsts = from_high[at], HIGH, high_pack[...]
        before = pltpu.roll(near_lasts[side], LANES - LAST - LAST * at, axis=1)
        after = pltpu.roll(firsts, LANES - s, axis=1) if s else firsts
        margin = jnp.where(lane < FIRST, after, before)
        left = pltpu.roll(jnp.where(lane >= LANES - LAST, margin, own), LEFT_AT + 4, axis=1)
        right = pltpu.roll(jnp.where(lane < BXY, margin, own), RIGHT_AT + 8, axis=1)
        other = jnp.where(between(lane, LEFT_AT, LEFT_AT + 12), left, 1.0)
        other = jnp.where(between(lane, RIGHT_AT, RIGHT_AT + 16), right, other)
        other = jnp.where(edge, margin, other)
        kp[c, r + 4, :, 0:LANES] = own + KMIN
        kp[c, r + 4, :, LANES : 2 * LANES] = other + KMIN

    lane2 = lane_of((1, NZ, 2 * LANES))
    layer2 = lax.broadcasted_iota(jnp.int32, (1, NZ, 2 * LANES), 1)
    left_end = (lane2 == LANES + LEFT_AT + 11) | (lane2 == LANES + RIGHT_AT + 15)
    right_start = lane2 == LANES + RIGHT_AT
    top, bottom = layer2 == NZ - 1, layer2 == 0
    zero = jnp.zeros((1, NZ, 2 * LANES), F32)

    def y_next(v):
        return pltpu.roll(v, 2 * LANES - 1, axis=2)

    def y_last(v):
        return pltpu.roll(v, 1, axis=2)

    def z_next(v):
        return pltpu.roll(v, NZ - 1, axis=1)

    def z_last(v):
        return pltpu.roll(v, 1, axis=1)

    def finish(tx_low, tx_high, ty_low, ty_high, tz_low, tz_high, low_end, high_end):
        inverse = 1.0 / (tx_low + tx_high + ty_low + ty_high + tz_low + tz_high)
        return [
            zero if low_end else tx_low * inverse,
            zero if high_end else tx_high * inverse,
            jnp.where(right_start, 0.0, ty_low * inverse),
            jnp.where(left_end, 0.0, ty_high * inverse),
            jnp.where(bottom, 0.0, tz_low * inverse),
            jnp.where(top, 0.0, tz_high * inverse),
            (tx_high - tx_low) * inverse,
            (ty_high - ty_low) * inverse,
            (tz_high - tz_low) * inverse,
        ]

    def coefficients(r):
        kx_low, kx, kx_high = (kp[0, pl.ds(r + 4 + d, 1)] for d in (-1, 0, 1))
        ky, kz = kp[1, pl.ds(r + 4, 1)], kp[2, pl.ds(r + 4, 1)]
        tx_low, tx_high = harmonic(kx_low, kx), harmonic(kx, kx_high)
        ty = harmonic(ky, y_next(ky))
        ty_low = jnp.where(right_start, ky, y_last(ty))
        ty_high = jnp.where(left_end, ky, ty)
        tz = harmonic(kz, z_next(kz))
        tz_low = jnp.where(bottom, kz, z_last(tz))
        tz_high = jnp.where(top, kz, tz)
        for n, value in enumerate(finish(tx_low, tx_high, ty_low, ty_high, tz_low, tz_high, False, False)):
            coef[n, pl.ds(r + 3, 1)] = value
            if n >= 6:
                q1[n - 6, pl.ds(r + 3, 1)] = W[0] * value
        if 0 <= r < 12:
            for d, value in enumerate((tx_high, ty_high, tz_high)):
                if r < 8 or d == 0:
                    face[d, pl.ds(r, 1)] = value
        if r in ENDS:
            e = ENDS.index(r)
            low, high = (tx_low, kx) if e % 2 else (kx, tx_high)
            for n, value in enumerate(finish(low, high, ty_low, ty_high, tz_low, tz_high, not e % 2, e % 2)):
                u_coef[e, pl.ds(n, 1)] = value
                if n >= 6:
                    uq[e, 0, n - 6, pl.ds(0, 1)] = W[0] * value

    def sweep(w, cs, low, mid, high):
        around = cs[2] * y_last(mid) + cs[3] * y_next(mid) + cs[4] * z_last(mid) + cs[5] * z_next(mid)
        if low is not None:
            around = around + cs[0] * low
        if high is not None:
            around = around + cs[1] * high
        return mid + w * (around + cs[6] - mid)

    def coefs_at(r, d):
        return [coef[n, pl.ds(r + 3, 1)] for n in (0, 1, 2, 3, 4, 5, 6 + d)]

    qs = [(q1, 3), (q2, 2), (q3, 1), (q4, 0)]

    def told_row(n):
        other = pltpu.roll(heard[pl.ds(TOLD + n // 3, 1)], LANES - 2 - SPAN * (n % 3), axis=2)
        return jnp.concatenate([heard[pl.ds(n, 1)], other], axis=2)

    def q_at(s, d, r):
        if r == 12:
            return told_row(s)
        ref, offset = qs[s]
        return ref[d, pl.ds(r + offset, 1)]

    def e_at(e, s, d, n):
        r = ENDS[e] - n if e % 2 else ENDS[e] + n
        return uq[e, s, d, pl.ds(n, 1)] if n <= s else q_at(s, d, r)

    def main_row(s, r, along=range(3)):
        for d in along:
            low, mid, high = (q_at(s - 1, d, r + n) for n in (-1, 0, 1))
            ref, offset = qs[s]
            ref[d, pl.ds(r + offset, 1)] = sweep(W[s], coefs_at(r, d), low, mid, high)

    def edge_row(e, s, n, along=range(3)):
        r = ENDS[e] - n if e % 2 else ENDS[e] + n
        for d in along:
            inner, mid = e_at(e, s - 1, d, n + 1), e_at(e, s - 1, d, n)
            outer = e_at(e, s - 1, d, n - 1) if n else None
            cs = coefs_at(r, d) if n else [u_coef[e, pl.ds(m, 1)] for m in (0, 1, 2, 3, 4, 5, 6 + d)]
            low, high = (inner, outer) if e % 2 else (outer, inner)
            uq[e, s, d, pl.ds(n, 1)] = sweep(W[s], cs, low, mid, high)

    last = SWEEPS - 1
    flag_left = (j > 0).astype(F32)
    flag_right = (j < n_gy - 1).astype(F32)
    flag_up = (i < n_gx - 1).astype(F32)
    flag_low = (i > 0).astype(F32)

    def terms(d, r, here, above, at_end=False):
        if d == 0:
            fall = here - above - 1.0
        elif d == 1:
            fall = here - jnp.where(left_end, 0.0, y_next(here)) - 1.0
        else:
            fall = here - jnp.where(top, 0.0, z_next(here)) - 1.0
        square = fall * fall
        t = kp[0, pl.ds(r + 4, 1)] if at_end else face[d, pl.ds(r, 1)]
        return jnp.concatenate([t * square, square], axis=0)

    def main_terms(d, r):
        return terms(d, r, q_at(last, d, r), q_at(last, d, r + 1) if d == 0 else None)

    def upper_sums(d):
        main = [main_terms(d, r) for r in range(4, 8)]
        main = main[0] + main[1] + main[2] + main[3]
        ends = [
            terms(d, r, e_at(1, last, d, 7 - r), zero if r == 7 else e_at(1, last, d, 6 - r), d == 0 and r == 7)
            for r in range(4, 8)
        ]
        return main + flag_up * main + flag_low * (ends[0] + ends[1] + ends[2] + ends[3])

    def lower_sums(d, first, ended, up, low):
        e = ENDS.index(first)
        main = [main_terms(d, first + n) for n in range(4)]
        ends = [terms(d, first + n, e_at(e, last, d, n), e_at(e, last, d, n + 1)) for n in range(4)]
        third = terms(d, first + 3, q_at(last, d, first + 3), ended) if d == 0 else main[3]
        three = main[0] + main[1] + main[2]
        return three + main[3] + up * (ends[0] + ends[1] + ends[2] + ends[3]) + low * (three + third)

    def columns(total):
        own, other = total[:, :, 0:LANES], total[:, :, LANES : 2 * LANES]
        lane3 = lane_of(own.shape)
        left = pltpu.roll(other, LANES - LEFT_AT - 4, axis=2) * flag_left
        right = pltpu.roll(other, LANES - RIGHT_AT - 8, axis=2)
        own = own + jnp.where(lane3 < 8, left, 0.0) + jnp.where(lane3 >= LANES - 8, right * flag_right, 0.0)
        return own, other + right

    for k in (6, 7):
        arrive(k)
    for r in range(8):
        for c in range(3):
            assemble(c, r)
    for r in range(1, 7):
        coefficients(r)

    pl.when(odd & copies[0][1])(copies[0][0].start)

    def from_below():
        for k in (2, 3, 0):
            arrive(k)
        for c, r in UP:
            assemble(c, r - 8)
        for r in range(-3, 1):
            coefficients(r)

    def from_above():
        for k in (4, 5, 1):
            arrive(k)
        for c, r in DOWN:
            assemble(c, r + 8)
        for r in range(7, 12):
            coefficients(r)

    def sweeps(starts, stops, e, along=range(3)):
        for s in range(1, SWEEPS):
            for r in range(starts[s - 1], stops[s - 1]):
                main_row(s, r, [d for d in along if d == 0 or r < 12 - s - 1])
            for n in range(s + 1):
                edge_row(e, s, n, along)

    told = remote(len(copies), tale, heard, -1, 0)
    tells = even & (i > 0)
    copies.append((told, tells, odd & (i + 1 < n_gx)))

    @pl.when(even)
    def _():
        from_above()
        sweeps((2, 3, 4), (11, 10, 9), 1, (0,))
        lane3 = lane_of((1, NZ, LANES))
        others = [None, None]
        for n in range(TOLD):
            value = q_at(n, 0, 4) if n < SWEEPS else e_at(1, last, 0, 3)
            tale[pl.ds(n, 1)] = value[:, :, 0:LANES]
            other = pltpu.roll(value[:, :, LANES : 2 * LANES], 2 + SPAN * (n % 3), axis=2)
            others[n // 3] = other if n % 3 == 0 else jnp.where(lane3 >= SPAN * (n % 3), other, others[n // 3])
        for n, other in enumerate(others):
            tale[pl.ds(TOLD + n, 1)] = other
        tale[pl.ds(TALE - 2, 2)] = columns(upper_sums(0))[0]
        pl.when(tells)(told.start)
        sweeps((2, 3, 4), (11, 10, 9), 1, (1, 2))
        from_below()
        sweeps((-2, -1, 0), (2, 3, 4), 0)

    @pl.when(odd)
    def _():
        from_below()
        sweeps((-2, -1, 0), (6, 5, 4), 0)
        from_above()
        sweeps((6, 5, 4), (11, 10, 9), 1)

    load_map.wait()
    layer = lax.broadcasted_iota(jnp.int32, (NZ, LANES), 0)
    layer_map = jnp.zeros((NZ, LANES), jnp.int32)
    for z in range(NZ):
        layer_map = jnp.where(layer == z, map_own[z], layer_map)
    pick = (lax.broadcasted_iota(jnp.int32, (LANES, LANES), 0) // BXY == lane_of((LANES, LANES))).astype(F32)
    extents = (24, 144, 8)

    def coarse(sums, along):
        count = len(along)
        stack = jnp.concatenate(sums, axis=0).reshape(2 * count * NZ, LANES)
        blocks = jnp.dot(stack, pick, precision=lax.Precision.HIGHEST, preferred_element_type=F32)
        blocks = blocks.reshape(count, 2, NZ, LANES)
        perm = [[None] * NCL for _ in along]
        for n in range(NCL):
            for at, d in enumerate(along):
                held = jnp.where(layer_map == n, blocks[at], 0.0)
                both = jnp.sum(held, axis=1, keepdims=True)
                perm[at][n] = both[0] / (both[1] + EPS * extents[d] * extents[d])
        return perm

    sums = [columns(lower_sums(d, 0, e_at(1, last, d, 3), flag_up, flag_low) + upper_sums(d)) for d in range(3)]
    perm = coarse([own for own, _ in sums] + [sums[1][1]], (0, 1, 2, 1))
    mess[pl.ds(0, NCL)] = jnp.concatenate(perm[0], axis=0)

    tell_k = len(copies)
    tell = remote(tell_k, mess, mess_x, -1, 0)
    sends = odd
    pl.when(sends)(tell.start)
    copies.append((tell, sends, even & inside(1, 0)))
    for d in range(3):
        for n in range(NCL):
            perm_ref[d, n] = perm[d][n][:, 0 : LANES // BXY]
    for n in range(NCL):
        value = harmonic(perm[2][n], perm[2][n + 1]) if n < NCL - 1 else jnp.zeros((1, LANES), F32)
        trans_ref[2, n] = value[:, 0 : LANES // BXY]

    exists = (j < n_gy - 1).astype(F32)
    lane1 = lane_of((1, LANES))
    for n in range(NCL):
        beyond = pltpu.roll(perm[3][n], LANES // BXY - 1, axis=1) * exists
        after = jnp.where(lane1 == LANES // BXY - 1, beyond, pltpu.roll(perm[1][n], LANES - 1, axis=1))
        trans_ref[1, n] = harmonic(perm[1][n], after)[:, 0 : LANES // BXY]

    @pl.when(odd)
    def _():
        arrive(tell_k - 1)
        for s in range(1, SWEEPS):
            for r in range(12 - s, 12):
                main_row(s, r, (0,))
            for n in range(s + 1):
                edge_row(2, s, n, (0,))
        ended = told_row(SWEEPS)
        own, _ = columns(lower_sums(0, 8, ended, (i + 2 < n_gx).astype(F32), 1.0))
        (beyond,) = coarse([own + heard[pl.ds(TALE - 2, 2)]], (0,))
        here = (i + 1 < n_gx).astype(F32)
        mess_x[pl.ds(0, NCL)] = jnp.concatenate(beyond, axis=0) * here

    @pl.when(even)
    def _():
        arrive(tell_k)

    for n in range(NCL):
        trans_ref[0, n] = harmonic(perm[0][n], mess_x[pl.ds(n, 1)])[:, 0 : LANES // BXY]
    for copy, sends, _ in copies:
        pl.when(sends)(copy.wait_send)


def solution(mesh):
    n_gx, n_gy = mesh.shape["gx"], mesh.shape["gy"]

    def local(permeability, layer_map):
        k = permeability.reshape(3 * NZ * BXY, LANES)
        out = jax.ShapeDtypeStruct((2, 3, NCL, 1, LANES // BXY), F32)
        vmem = lambda *shape: pltpu.VMEM(shape, F32)
        both = 2 * LANES
        both_out = pl.pallas_call(
            lambda *refs: kernel(n_gx, n_gy, *refs),
            out_shape=out,
            in_specs=[pl.BlockSpec(memory_space=pltpu.HBM)] * 2,
            out_specs=pl.BlockSpec(memory_space=pltpu.VMEM),
            scratch_shapes=[
                vmem(3 * NZ * BXY, LANES),
                pltpu.SMEM((NZ,), jnp.int32),
                vmem(len(PLANES), NZ, LANES),
                vmem(NZ, LANES),
                vmem(4, NZ, LANES),
                vmem(2, NZ, LANES),
                vmem(len(UP), NZ, LANES),
                vmem(len(DOWN), NZ, LANES),
                vmem(3, NZ, LANES),
                vmem(4, NZ, LANES),
                vmem(NZ, LANES),
                vmem(NZ, LANES),
                vmem(TALE, NZ, LANES),
                vmem(TALE, NZ, LANES),
                vmem(3, 17, NZ, both),
                vmem(9, 15, NZ, both),
                vmem(3, 12, NZ, both),
                vmem(3, 15, NZ, both),
                vmem(3, 14, NZ, both),
                vmem(3, 13, NZ, both),
                vmem(3, 12, NZ, both),
                vmem(3, 9, NZ, both),
                vmem(3, SWEEPS, 3, SWEEPS, NZ, both),
                vmem(NZ, LANES),
                vmem(NZ, LANES),
                pltpu.SemaphoreType.DMA((2,)),
                pltpu.SemaphoreType.DMA((10,)),
                pltpu.SemaphoreType.DMA((10,)),
            ],
            compiler_params=pltpu.CompilerParams(
                collective_id=0, has_side_effects=True, vmem_limit_bytes=32 * 1024 * 1024
            ),
            name="upscale",
        )(pltpu.with_memory_space_constraint(k, pltpu.HBM), pltpu.with_memory_space_constraint(layer_map, pltpu.HBM))
        return both_out[0], both_out[1]

    spec = P(None, None, "gx", "gy")
    return jax.shard_map(local, mesh=mesh, in_specs=(spec, P()), out_specs=(spec, spec), check_vma=False)
```

```python
import math

import jax
import jax.numpy as jnp
from jax import lax
from jax.experimental import pallas as pl
from jax.experimental.pallas import tpu as pltpu
from jax.sharding import PartitionSpec as P

MESH = pl.DeviceIdType.MESH
NCL = 4
BXY = 8
SWEEPS = 4
KMIN = 0.01
EPS = 1e-06
NZ = 8
LANES = 128
F32 = jnp.float32

DOWN = [(1, r) for r in range(4)] + [(2, r) for r in range(4)] + [(0, r) for r in range(5)]
UP = [(0, r) for r in range(4, 8)] + [(1, r) for r in range(5, 8)] + [(2, r) for r in range(5, 8)]
PLANES = DOWN + UP[1:] + [(1, 4), (2, 4)]
PLANE_AT = {cr: at for at, cr in enumerate(PLANES)}
UP_FROM = PLANE_AT[UP[0]]
LAST, FIRST = 4, 13
PER_PACK = LANES // FIRST
LISTS = [DOWN, UP + [(1, 4), (2, 4)]]
PACKS = [part for planes in LISTS for part in (planes[:PER_PACK], planes[PER_PACK:])]
SLOT_OF = {cr: (v, FIRST * at) for v, pack in reversed(list(enumerate(PACKS))) for at, cr in enumerate(pack)}


def slots(widths):
    at, result = 0, {}
    for cr, width in widths.items():
        result[cr] = (at, width)
        at = at + width
    assert at <= LANES
    return result


UP_SLOTS = slots({cr: 12 for cr in UP})
DOWN_WIDTHS = {0: [11, 11, 10, 9, 3], 1: [12, 11, 10, 4], 2: [11, 10, 9, 3]}
DOWN_SLOTS = slots({(c, r): DOWN_WIDTHS[c][r] for c, r in DOWN})
DIRECTIONS = [(1, 0), (-1, 0), (1, 1), (1, -1), (-1, 1), (-1, -1), (0, 1), (0, -1)]
LOW, HIGH, OWN = range(3)
ENDS = [0, 7, 8]
LEFT_AT = 13
RIGHT_AT = 25
TOLD = SWEEPS + 1
SPAN = 42
TALE = TOLD + -(-TOLD // 3) + 2
W = [1.0 / (1.05 + 0.95 * math.cos(math.pi * (2 * s + 1) / (2 * SWEEPS))) for s in range(SWEEPS)]


def harmonic(left, right):
    return 2.0 * left * right / (left + right)


def lane_of(shape):
    return lax.broadcasted_iota(jnp.int32, shape, len(shape) - 1)


def between(lane, low, high):
    return (lane >= low) & (lane < high)


def kernel(
    n_gx, n_gy, k_hbm, map_hbm, out_ref,
    k_own, map_own, planes, lasts, packs, corners, from_low, from_high,
    near_lasts, own_packs, low_pack, high_pack, tale, heard,
    kp, coef, face, q1, q2, q3, q4, u_coef, uq, mess, mess_x,
    load_sem, send_sem, recv_sem,
):
    i, j = lax.axis_index("gx"), lax.axis_index("gy")
    perm_ref, trans_ref = out_ref.at[0], out_ref.at[1]
    load_k = pltpu.make_async_copy(k_hbm, k_own, load_sem.at[0])
    load_map = pltpu.make_async_copy(map_hbm, map_own, load_sem.at[1])
    load_k.start()
    load_map.start()

    def inside(di, dj):
        tests = []
        if di:
            tests.append(i + di < n_gx if di > 0 else i >= -di)
        if dj:
            tests.append(j + dj < n_gy if dj > 0 else j >= -dj)
        return tests[0] if len(tests) == 1 else tests[0] & tests[1]

    def device(di, dj):
        return {"gx": i + di, "gy": j + dj}

    odd = lax.rem(i, 2) == 1
    even = jnp.logical_not(odd)

    barrier = pltpu.get_barrier_semaphore()
    for di, dj in DIRECTIONS:
        @pl.when(inside(di, dj))
        def _():
            pl.semaphore_signal(barrier, inc=1, device_id=device(di, dj), device_id_type=MESH)

    lane = lane_of((NZ, LANES))
    load_k.wait()
    packed = [jnp.zeros((NZ, LANES), F32)] * len(PACKS)
    corner = [jnp.zeros((NZ, LANES), F32)] * 2
    last_of = jnp.zeros((NZ, LANES), F32)
    for at, (c, r) in enumerate(PLANES):
        plane = k_own[pl.ds(c * 64 + r, NZ, stride=8), :]
        planes[at] = plane
        last_of = jnp.where(between(lane, LAST * at, LAST * at + LAST), pltpu.roll(plane, LAST * at + LAST, axis=1), last_of)
        for v, pack in enumerate(PACKS):
            if (c, r) in pack:
                s = FIRST * pack.index((c, r))
                first_of = pltpu.roll(plane, s, axis=1) if s else plane
                packed[v] = jnp.where(between(lane, s, s + FIRST), first_of, packed[v])
        for v, places in enumerate((DOWN_SLOTS, UP_SLOTS)):
            if (c, r) in places:
                s, width = places[c, r]
                first_of = pltpu.roll(plane, s, axis=1) if s else plane
                corner[v] = jnp.where(between(lane, s, s + width), first_of, corner[v])
    lasts[...] = last_of
    corners[0] = corner[0]
    corners[1] = corner[1]
    for v, value in enumerate(packed):
        packs[v] = value

    rows_near = 1 + (i > 0).astype(jnp.int32) + (i < n_gx - 1).astype(jnp.int32)
    cols_near = 1 + (j > 0).astype(jnp.int32) + (j < n_gy - 1).astype(jnp.int32)
    pl.semaphore_wait(barrier, rows_near * cols_near - 1)

    def remote(k, source, target, di, dj):
        return pltpu.make_async_remote_copy(
            src_ref=source, dst_ref=target, send_sem=send_sem.at[k], recv_sem=recv_sem.at[k],
            device_id=device(di, dj), device_id_type=MESH,
        )

    def copy_of(k, di, dj):
        if dj == 0:
            if di > 0:
                return remote(k, planes.at[pl.ds(UP_FROM, len(UP))], from_low, di, dj)
            return remote(k, planes.at[pl.ds(0, len(DOWN))], from_high, di, dj)
        if dj > 0:
            return remote(k, lasts, near_lasts.at[LOW if di > 0 else HIGH if di < 0 else OWN], di, dj)
        if di == 0:
            return remote(k, packs, own_packs, di, dj)
        if di > 0:
            return remote(k, corners.at[1], low_pack, di, dj)
        return remote(k, corners.at[0], high_pack, di, dj)

    copies = [(copy_of(k, *to), inside(*to), inside(-to[0], -to[1])) for k, to in enumerate(DIRECTIONS)]
    for k in (7, 6, 5, 4, 3, 2, 1, 0):
        copy, sends, _ = copies[k]
        pl.when(sends & even if k in (0, 2, 3) else sends)(copy.start)

    def arrive(k):
        copy, _, here = copies[k]
        target = copy.dst_ref
        pl.when(here)(copy.wait_recv)

        @pl.when(jnp.logical_not(here))
        def _():
            target[...] = jnp.zeros(target.shape, F32)

    edge = (lane >= LANES - LAST) | (lane < FIRST)

    def assemble(c, r):
        if 0 <= r < 8:
            at, (v, s) = PLANE_AT[c, r], SLOT_OF[c, r]
            own, side, firsts = planes[at], OWN, own_packs[v]
        elif r < 0:
            at, s = PLANE_AT[c, r + 8], UP_SLOTS[c, r + 8][0]
            own, side, firsts = from_low[at - UP_FROM], LOW, low_pack[...]
        else:
            at, s = PLANE_AT[c, r - 8], DOWN_SLOTS[c, r - 8][0]
            own, side, firsts = from_high[at], HIGH, high_pack[...]
        before = pltpu.roll(near_lasts[side], LANES - LAST - LAST * at, axis=1)
        after = pltpu.roll(firsts, LANES - s, axis=1) if s else firsts
        margin = jnp.where(lane < FIRST, after, before)
        left = pltpu.roll(jnp.where(lane >= LANES - LAST, margin, own), LEFT_AT + 4, axis=1)
        right = pltpu.roll(jnp.where(lane < BXY, margin, own), RIGHT_AT + 8, axis=1)
        other = jnp.where(between(lane, LEFT_AT, LEFT_AT + 12), left, 1.0)
        other = jnp.where(between(lane, RIGHT_AT, RIGHT_AT + 16), right, other)
        other = jnp.where(edge, margin, other)
        kp[c, r + 4, :, 0:LANES] = own + KMIN
        kp[c, r + 4, :, LANES : 2 * LANES] = other + KMIN

    lane2 = lane_of((1, NZ, 2 * LANES))
    layer2 = lax.broadcasted_iota(jnp.int32, (1, NZ, 2 * LANES), 1)
    left_end = (lane2 == LANES + LEFT_AT + 11) | (lane2 == LANES + RIGHT_AT + 15)
    right_start = lane2 == LANES + RIGHT_AT
    top, bottom = layer2 == NZ - 1, layer2 == 0
    zero = jnp.zeros((1, NZ, 2 * LANES), F32)

    def y_next(v):
        return pltpu.roll(v, 2 * LANES - 1, axis=2)

    def y_last(v):
        return pltpu.roll(v, 1, axis=2)

    def z_next(v):
        return pltpu.roll(v, NZ - 1, axis=1)

    def z_last(v):
        return pltpu.roll(v, 1, axis=1)

    def finish(tx_low, tx_high, ty_low, ty_high, tz_low, tz_high, low_end, high_end):
        inverse = 1.0 / (tx_low + tx_high + ty_low + ty_high + tz_low + tz_high)
        return [
            zero if low_end else tx_low * inverse,
            zero if high_end else tx_high * inverse,
            jnp.where(right_start, 0.0, ty_low * inverse),
            jnp.where(left_end, 0.0, ty_high * inverse),
            jnp.where(bottom, 0.0, tz_low * inverse),
            jnp.where(top, 0.0, tz_high * inverse),
            (tx_high - tx_low) * inverse,
            (ty_high - ty_low) * inverse,
            (tz_high - tz_low) * inverse,
        ]

    def coefficients(r):
        kx_low, kx, kx_high = (kp[0, pl.ds(r + 4 + d, 1)] for d in (-1, 0, 1))
        ky, kz = kp[1, pl.ds(r + 4, 1)], kp[2, pl.ds(r + 4, 1)]
        tx_low, tx_high = harmonic(kx_low, kx), harmonic(kx, kx_high)
        ty = harmonic(ky, y_next(ky))
        ty_low = jnp.where(right_start, ky, y_last(ty))
        ty_high = jnp.where(left_end, ky, ty)
        tz = harmonic(kz, z_next(kz))
        tz_low = jnp.where(bottom, kz, z_last(tz))
        tz_high = jnp.where(top, kz, tz)
        for n, value in enumerate(finish(tx_low, tx_high, ty_low, ty_high, tz_low, tz_high, False, False)):
            coef[n, pl.ds(r + 3, 1)] = value
            if n >= 6:
                q1[n - 6, pl.ds(r + 3, 1)] = W[0] * value
        if 0 <= r < 12:
            for d, value in enumerate((tx_high, ty_high, tz_high)):
                if r < 8 or d == 0:
                    face[d, pl.ds(r, 1)] = value
        if r in ENDS:
            e = ENDS.index(r)
            low, high = (tx_low, kx) if e % 2 else (kx, tx_high)
            for n, value in enumerate(finish(low, high, ty_low, ty_high, tz_low, tz_high, not e % 2, e % 2)):
                u_coef[e, pl.ds(n, 1)] = value
                if n >= 6:
                    uq[e, 0, n - 6, pl.ds(0, 1)] = W[0] * value

    def sweep(w, cs, low, mid, high):
        around = cs[2] * y_last(mid) + cs[3] * y_next(mid) + cs[4] * z_last(mid) + cs[5] * z_next(mid)
        if low is not None:
            around = around + cs[0] * low
        if high is not None:
            around = around + cs[1] * high
        return mid + w * (around + cs[6] - mid)

    def coefs_at(r, d):
        return [coef[n, pl.ds(r + 3, 1)] for n in (0, 1, 2, 3, 4, 5, 6 + d)]

    qs = [(q1, 3), (q2, 2), (q3, 1), (q4, 0)]

    def told_row(n):
        other = pltpu.roll(heard[pl.ds(TOLD + n // 3, 1)], LANES - 2 - SPAN * (n % 3), axis=2)
        return jnp.concatenate([heard[pl.ds(n, 1)], other], axis=2)

    def q_at(s, d, r):
        if r == 12:
            return told_row(s)
        ref, offset = qs[s]
        return ref[d, pl.ds(r + offset, 1)]

    def e_at(e, s, d, n):
        r = ENDS[e] - n if e % 2 else ENDS[e] + n
        return uq[e, s, d, pl.ds(n, 1)] if n <= s else q_at(s, d, r)

    def main_row(s, r, along=range(3)):
        for d in along:
            low, mid, high = (q_at(s - 1, d, r + n) for n in (-1, 0, 1))
            ref, offset = qs[s]
            ref[d, pl.ds(r + offset, 1)] = sweep(W[s], coefs_at(r, d), low, mid, high)

    def edge_row(e, s, n, along=range(3)):
        r = ENDS[e] - n if e % 2 else ENDS[e] + n
        for d in along:
            inner, mid = e_at(e, s - 1, d, n + 1), e_at(e, s - 1, d, n)
            outer = e_at(e, s - 1, d, n - 1) if n else None
            cs = coefs_at(r, d) if n else [u_coef[e, pl.ds(m, 1)] for m in (0, 1, 2, 3, 4, 5, 6 + d)]
            low, high = (inner, outer) if e % 2 else (outer, inner)
            uq[e, s, d, pl.ds(n, 1)] = sweep(W[s], cs, low, mid, high)

    last = SWEEPS - 1
    flag_left = (j > 0).astype(F32)
    flag_right = (j < n_gy - 1).astype(F32)
    flag_up = (i < n_gx - 1).astype(F32)
    flag_low = (i > 0).astype(F32)

    def terms(d, r, here, above, at_end=False):
        if d == 0:
            fall = here - above - 1.0
        elif d == 1:
            fall = here - jnp.where(left_end, 0.0, y_next(here)) - 1.0
        else:
            fall = here - jnp.where(top, 0.0, z_next(here)) - 1.0
        square = fall * fall
        t = kp[0, pl.ds(r + 4, 1)] if at_end else face[d, pl.ds(r, 1)]
        return jnp.concatenate([t * square, square], axis=0)

    def main_terms(d, r):
        return terms(d, r, q_at(last, d, r), q_at(last, d, r + 1) if d == 0 else None)

    def upper_sums(d):
        main = [main_terms(d, r) for r in range(4, 8)]
        main = main[0] + main[1] + main[2] + main[3]
        ends = [
            terms(d, r, e_at(1, last, d, 7 - r), zero if r == 7 else e_at(1, last, d, 6 - r), d == 0 and r == 7)
            for r in range(4, 8)
        ]
        return main + flag_up * main + flag_low * (ends[0] + ends[1] + ends[2] + ends[3])

    def lower_sums(d, first, ended, up, low):
        e = ENDS.index(first)
        main = [main_terms(d, first + n) for n in range(4)]
        ends = [terms(d, first + n, e_at(e, last, d, n), e_at(e, last, d, n + 1)) for n in range(4)]
        third = terms(d, first + 3, q_at(last, d, first + 3), ended) if d == 0 else main[3]
        three = main[0] + main[1] + main[2]
        return three + main[3] + up * (ends[0] + ends[1] + ends[2] + ends[3]) + low * (three + third)

    def columns(total):
        own, other = total[:, :, 0:LANES], total[:, :, LANES : 2 * LANES]
        lane3 = lane_of(own.shape)
        left = pltpu.roll(other, LANES - LEFT_AT - 4, axis=2) * flag_left
        right = pltpu.roll(other, LANES - RIGHT_AT - 8, axis=2)
        own = own + jnp.where(lane3 < 8, left, 0.0) + jnp.where(lane3 >= LANES - 8, right * flag_right, 0.0)
        return own, other + right

    for k in (6, 7):
        arrive(k)
    for r in range(8):
        for c in range(3):
            assemble(c, r)
    for r in range(1, 7):
        coefficients(r)

    for k in (0, 2, 3):
        pl.when(odd & copies[k][1])(copies[k][0].start)

    def from_below():
        for k in (2, 3, 0):
            arrive(k)
        for c, r in UP:
            assemble(c, r - 8)
        for r in range(-3, 1):
            coefficients(r)

    def from_above():
        for k in (4, 5, 1):
            arrive(k)
        for c, r in DOWN:
            assemble(c, r + 8)
        for r in range(7, 12):
            coefficients(r)

    def sweeps(starts, stops, e, along=range(3)):
        for s in range(1, SWEEPS):
            for r in range(starts[s - 1], stops[s - 1]):
                main_row(s, r, [d for d in along if d == 0 or r < 12 - s - 1])
            for n in range(s + 1):
                edge_row(e, s, n, along)

    told = remote(len(copies), tale, heard, -1, 0)
    tells = even & (i > 0)
    copies.append((told, tells, odd & (i + 1 < n_gx)))

    @pl.when(even)
    def _():
        from_above()
        sweeps((2, 3, 4), (11, 10, 9), 1, (0,))
        lane3 = lane_of((1, NZ, LANES))
        others = [None, None]
        for n in range(TOLD):
            value = q_at(n, 0, 4) if n < SWEEPS else e_at(1, last, 0, 3)
            tale[pl.ds(n, 1)] = value[:, :, 0:LANES]
            other = pltpu.roll(value[:, :, LANES : 2 * LANES], 2 + SPAN * (n % 3), axis=2)
            others[n // 3] = other if n % 3 == 0 else jnp.where(lane3 >= SPAN * (n % 3), other, others[n // 3])
        for n, other in enumerate(others):
            tale[pl.ds(TOLD + n, 1)] = other
        tale[pl.ds(TALE - 2, 2)] = columns(upper_sums(0))[0]
        pl.when(tells)(told.start)
        sweeps((2, 3, 4), (11, 10, 9), 1, (1, 2))
        from_below()
        sweeps((-2, -1, 0), (2, 3, 4), 0)

    @pl.when(odd)
    def _():
        from_below()
        sweeps((-2, -1, 0), (6, 5, 4), 0)
        from_above()
        sweeps((6, 5, 4), (11, 10, 9), 1)

    load_map.wait()
    layer = lax.broadcasted_iota(jnp.int32, (NZ, LANES), 0)
    layer_map = jnp.zeros((NZ, LANES), jnp.int32)
    for z in range(NZ):
        layer_map = jnp.where(layer == z, map_own[z], layer_map)
    pick = (lax.broadcasted_iota(jnp.int32, (LANES, LANES), 0) // BXY == lane_of((LANES, LANES))).astype(F32)
    extents = (24, 144, 8)

    def coarse(sums, along):
        count = len(along)
        stack = jnp.concatenate(sums, axis=0).reshape(2 * count * NZ, LANES)
        blocks = jnp.dot(stack, pick, precision=lax.Precision.HIGHEST, preferred_element_type=F32)
        blocks = blocks.reshape(count, 2, NZ, LANES)
        perm = [[None] * NCL for _ in along]
        for n in range(NCL):
            for at, d in enumerate(along):
                held = jnp.where(layer_map == n, blocks[at], 0.0)
                both = jnp.sum(held, axis=1, keepdims=True)
                perm[at][n] = both[0] / (both[1] + EPS * extents[d] * extents[d])
        return perm

    sums = [columns(lower_sums(d, 0, e_at(1, last, d, 3), flag_up, flag_low) + upper_sums(d)) for d in range(3)]
    perm = coarse([own for own, _ in sums] + [sums[1][1]], (0, 1, 2, 1))
    mess[pl.ds(0, NCL)] = jnp.concatenate(perm[0], axis=0)

    tell_k = len(copies)
    tell = remote(tell_k, mess, mess_x, -1, 0)
    sends = odd
    pl.when(sends)(tell.start)
    copies.append((tell, sends, even & inside(1, 0)))
    for d in range(3):
        for n in range(NCL):
            perm_ref[d, n] = perm[d][n][:, 0 : LANES // BXY]
    for n in range(NCL):
        value = harmonic(perm[2][n], perm[2][n + 1]) if n < NCL - 1 else jnp.zeros((1, LANES), F32)
        trans_ref[2, n] = value[:, 0 : LANES // BXY]

    exists = (j < n_gy - 1).astype(F32)
    lane1 = lane_of((1, LANES))
    for n in range(NCL):
        beyond = pltpu.roll(perm[3][n], LANES // BXY - 1, axis=1) * exists
        after = jnp.where(lane1 == LANES // BXY - 1, beyond, pltpu.roll(perm[1][n], LANES - 1, axis=1))
        trans_ref[1, n] = harmonic(perm[1][n], after)[:, 0 : LANES // BXY]

    @pl.when(odd)
    def _():
        arrive(tell_k - 1)
        for s in range(1, SWEEPS):
            for r in range(12 - s, 12):
                main_row(s, r, (0,))
            for n in range(s + 1):
                edge_row(2, s, n, (0,))
        ended = told_row(SWEEPS)
        own, _ = columns(lower_sums(0, 8, ended, (i + 2 < n_gx).astype(F32), 1.0))
        (beyond,) = coarse([own + heard[pl.ds(TALE - 2, 2)]], (0,))
        here = (i + 1 < n_gx).astype(F32)
        mess_x[pl.ds(0, NCL)] = jnp.concatenate(beyond, axis=0) * here

    @pl.when(even)
    def _():
        arrive(tell_k)

    for n in range(NCL):
        trans_ref[0, n] = harmonic(perm[0][n], mess_x[pl.ds(n, 1)])[:, 0 : LANES // BXY]
    for copy, sends, _ in copies:
        pl.when(sends)(copy.wait_send)


def solution(mesh):
    n_gx, n_gy = mesh.shape["gx"], mesh.shape["gy"]

    def local(permeability, layer_map):
        k = permeability.reshape(3 * NZ * BXY, LANES)
        out = jax.ShapeDtypeStruct((2, 3, NCL, 1, LANES // BXY), F32)
        vmem = lambda *shape: pltpu.VMEM(shape, F32)
        both = 2 * LANES
        both_out = pl.pallas_call(
            lambda *refs: kernel(n_gx, n_gy, *refs),
            out_shape=out,
            in_specs=[pl.BlockSpec(memory_space=pltpu.HBM)] * 2,
            out_specs=pl.BlockSpec(memory_space=pltpu.VMEM),
            scratch_shapes=[
                vmem(3 * NZ * BXY, LANES),
                pltpu.SMEM((NZ,), jnp.int32),
                vmem(len(PLANES), NZ, LANES),
                vmem(NZ, LANES),
                vmem(4, NZ, LANES),
                vmem(2, NZ, LANES),
                vmem(len(UP), NZ, LANES),
                vmem(len(DOWN), NZ, LANES),
                vmem(3, NZ, LANES),
                vmem(4, NZ, LANES),
                vmem(NZ, LANES),
                vmem(NZ, LANES),
                vmem(TALE, NZ, LANES),
                vmem(TALE, NZ, LANES),
                vmem(3, 17, NZ, both),
                vmem(9, 15, NZ, both),
                vmem(3, 12, NZ, both),
                vmem(3, 15, NZ, both),
                vmem(3, 14, NZ, both),
                vmem(3, 13, NZ, both),
                vmem(3, 12, NZ, both),
                vmem(3, 9, NZ, both),
                vmem(3, SWEEPS, 3, SWEEPS, NZ, both),
                vmem(NZ, LANES),
                vmem(NZ, LANES),
                pltpu.SemaphoreType.DMA((2,)),
                pltpu.SemaphoreType.DMA((10,)),
                pltpu.SemaphoreType.DMA((10,)),
            ],
            compiler_params=pltpu.CompilerParams(
                collective_id=0, has_side_effects=True, vmem_limit_bytes=32 * 1024 * 1024
            ),
            name="upscale",
        )(pltpu.with_memory_space_constraint(k, pltpu.HBM), pltpu.with_memory_space_constraint(layer_map, pltpu.HBM))
        return both_out[0], both_out[1]

    spec = P(None, None, "gx", "gy")
    return jax.shard_map(local, mesh=mesh, in_specs=(spec, P()), out_specs=(spec, spec), check_vma=False)
```
